16 devices in a mesh: dp: 2 (over z), tp: 8 (over y, x, core).
Axes of the slice: x: 2, y: 2, z: 2, core: 2. Of those that a mesh axis runs over, the one named last changes fastest.
Arguments:
- x_seq: bfloat16 [3, 256, 5120], P(None, 'dp'), parts along dimension 1
- cache_len: int32 [256], P('dp'), parts along dimension 0
- k_cache: bfloat16 [256, 8, 256, 128], P('dp', 'tp'), parts along dimension 0
- v_cache: bfloat16 [256, 8, 256, 128], P('dp', 'tp'), parts along dimension 0
- w_q: bfloat16 [5120, 5120], P(None, 'tp')
- w_k: bfloat16 [5120, 1024], P(None, 'tp')
- w_v: bfloat16 [5120, 1024], P(None, 'tp')
- w_o: bfloat16 [5120, 5120], P('tp')
- w_gate: bfloat16 [5120, 13824], P(None, 'tp')
- w_up: bfloat16 [5120, 13824], P(None, 'tp')
- w_down: bfloat16 [13824, 5120], P('tp')
- g_q: bfloat16 [5120], P('tp')
- g_k: bfloat16 [1024], P('tp')
- g_attn: bfloat16 [5120], replicated
- g_mlp: bfloat16 [5120], replicated
Outputs:
- output 1: bfloat16 [3, 256, 5120], P(None, 'dp'), parts along dimension 1
- output 2: bfloat16 [256, 8, 256, 128], P('dp', 'tp'), parts along dimension 0
- output 3: bfloat16 [256, 8, 256, 128], P('dp', 'tp'), parts along dimension 0
There are 2 independent parts. The reference program is written for one: setup_inputs(seed, part) draws one part's arguments, and reference() takes and returns one part's arrays. A program takes and returns all parts, laid end to end along the dimension named above; an argument that names none is the same for every part.
All inputs are finite; a program needn't handle non-finite values.
Results may differ from the reference program's by a relative error of at most 0.02.
Values are sent between devices in bfloat16 or wider.
A program may use at most 1 GiB of HBM per device.

```python
import math
import jax
import jax.numpy as jnp
from jax import lax

STEPS = 3
MIN_LEN = 128
D_MODEL = 5120
N_HEADS = 40
N_KV_HEADS = 8
HEAD_DIM = 128
FF_DIM = 13824
BATCH_ROWS = 128
MAX_SEQ = 256
ROPE_THETA = 500000.0
NORM_EPS = 1e-6


def draw_lengths(len_key):
    sub_keys = jax.random.split(len_key, 3)
    lengths = jax.random.randint(sub_keys[0], (BATCH_ROWS,), MIN_LEN, MAX_SEQ - STEPS + 1)
    long_row = jax.random.randint(sub_keys[1], (), 0, BATCH_ROWS)
    short_row = (long_row + 1 + jax.random.randint(sub_keys[2], (), 0, BATCH_ROWS - 1)) % BATCH_ROWS
    lengths = lengths.at[long_row].set(MAX_SEQ - STEPS).at[short_row].set(MIN_LEN)
    return lengths.astype(jnp.int32)


def normal_weight(w_key, rows_in, cols_out):
    return jax.random.normal(w_key, (rows_in, cols_out), jnp.float32) * rows_in ** -0.5


def head_scales(scale_key, n_heads):
    log_scale = jax.random.uniform(scale_key, (n_heads,), jnp.float32, math.log(0.3), math.log(3.0))
    return jnp.repeat(jnp.exp(log_scale), HEAD_DIM)


def setup_inputs(seed: int = 0, part: int = 0) -> dict:
    base_key = jax.random.key(seed)
    part_keys = jax.random.split(jax.random.fold_in(base_key, part), 4)
    w_keys = jax.random.split(jax.random.key(seed + 1), 13)
    q_width = N_HEADS * HEAD_DIM
    kv_width = N_KV_HEADS * HEAD_DIM
    cache_shape = (BATCH_ROWS, N_KV_HEADS, MAX_SEQ, HEAD_DIM)
    x_seq = jax.random.normal(part_keys[0], (STEPS, BATCH_ROWS, D_MODEL), jnp.float32)
    k_cache = jax.random.normal(part_keys[2], cache_shape, jnp.float32)
    v_cache = jax.random.normal(part_keys[3], cache_shape, jnp.float32)
    w_q = normal_weight(w_keys[0], D_MODEL, q_width) * head_scales(w_keys[1], N_HEADS)[None, :]
    w_k = normal_weight(w_keys[2], D_MODEL, kv_width) * head_scales(w_keys[3], N_KV_HEADS)[None, :]
    w_v = normal_weight(w_keys[4], D_MODEL, kv_width)
    w_o = normal_weight(w_keys[5], q_width, D_MODEL)
    w_gate = normal_weight(w_keys[6], D_MODEL, FF_DIM)
    w_up = normal_weight(w_keys[7], D_MODEL, FF_DIM)
    w_down = normal_weight(w_keys[8], FF_DIM, D_MODEL)
    g_q = jax.random.uniform(w_keys[9], (q_width,), jnp.float32, 0.5, 1.5)
    g_k = jax.random.uniform(w_keys[10], (kv_width,), jnp.float32, 0.5, 1.5)
    g_attn = jax.random.uniform(w_keys[11], (D_MODEL,), jnp.float32, 0.5, 1.5)
    g_mlp = jax.random.uniform(w_keys[12], (D_MODEL,), jnp.float32, 0.5, 1.5)
    return {'x_seq': x_seq.astype(jnp.bfloat16), 'cache_len': draw_lengths(part_keys[1]), 'k_cache': k_cache.astype(jnp.bfloat16), 'v_cache': v_cache.astype(jnp.bfloat16), 'w_q': w_q.astype(jnp.bfloat16), 'w_k': w_k.astype(jnp.bfloat16), 'w_v': w_v.astype(jnp.bfloat16), 'w_o': w_o.astype(jnp.bfloat16), 'w_gate': w_gate.astype(jnp.bfloat16), 'w_up': w_up.astype(jnp.bfloat16), 'w_down': w_down.astype(jnp.bfloat16), 'g_q': g_q.astype(jnp.bfloat16), 'g_k': g_k.astype(jnp.bfloat16), 'g_attn': g_attn.astype(jnp.bfloat16), 'g_mlp': g_mlp.astype(jnp.bfloat16)}


def rms_factor(sq_sum, full_width):
    return lax.rsqrt(sq_sum / full_width + NORM_EPS)


def rope_tables(positions):
    half_dim = HEAD_DIM // 2
    inv_freq = ROPE_THETA ** (-(jnp.arange(half_dim, dtype=jnp.float32) * (2.0 / HEAD_DIM)))
    angles = positions.astype(jnp.float32)[:, None] * inv_freq[None, :]
    return jnp.cos(angles), jnp.sin(angles)


def apply_rope(head_vals, cos_tab, sin_tab):
    half_dim = HEAD_DIM // 2
    lead_half = head_vals[..., :half_dim]
    tail_half = head_vals[..., half_dim:]
    cos_rows = cos_tab[:, None, :]
    sin_rows = sin_tab[:, None, :]
    return jnp.concatenate([lead_half * cos_rows - tail_half * sin_rows, tail_half * cos_rows + lead_half * sin_rows], axis=-1)


def reference(x_seq, cache_len, k_cache, v_cache, w_q, w_k, w_v, w_o, w_gate, w_up, w_down, g_q, g_k, g_attn, g_mlp):
    q_width = N_HEADS * HEAD_DIM
    kv_width = N_KV_HEADS * HEAD_DIM
    group_size = N_HEADS // N_KV_HEADS
    row_ids = jnp.arange(BATCH_ROWS)
    seq_ids = jnp.arange(MAX_SEQ)
    gain_q = g_q.astype(jnp.float32)
    gain_k = g_k.astype(jnp.float32)
    gain_a = g_attn.astype(jnp.float32)
    gain_m = g_mlp.astype(jnp.float32)

    def attend_row(row_in):
        q_row, k_row, v_row, last_pos = row_in
        q_grp = q_row.reshape(N_KV_HEADS, group_size, HEAD_DIM).astype(jnp.float32)
        scores = jnp.einsum('kgd,ksd->kgs', q_grp, k_row.astype(jnp.float32)) * HEAD_DIM ** -0.5
        scores = jnp.where(seq_ids <= last_pos, scores, -jnp.inf)
        row_max = jnp.max(scores, axis=-1, keepdims=True)
        exp_scores = jnp.exp(scores - row_max)
        row_sum = jnp.sum(exp_scores, axis=-1, keepdims=True)
        mixed_vals = jnp.einsum('kgs,ksd->kgd', exp_scores.astype(jnp.bfloat16).astype(jnp.float32), v_row.astype(jnp.float32))
        return (mixed_vals / row_sum).astype(jnp.bfloat16).reshape(q_width)

    def one_step(cache_pair, step_in):
        k_all, v_all = cache_pair
        x_tok, step_idx = step_in
        positions = cache_len + step_idx
        q_raw = jnp.dot(x_tok, w_q, preferred_element_type=jnp.float32).astype(jnp.bfloat16).astype(jnp.float32)
        k_raw = jnp.dot(x_tok, w_k, preferred_element_type=jnp.float32).astype(jnp.bfloat16).astype(jnp.float32)
        v_new = jnp.dot(x_tok, w_v, preferred_element_type=jnp.float32).astype(jnp.bfloat16).reshape(BATCH_ROWS, N_KV_HEADS, HEAD_DIM)
        q_normed = q_raw * rms_factor(jnp.sum(q_raw * q_raw, axis=-1, keepdims=True), q_width) * gain_q
        k_normed = k_raw * rms_factor(jnp.sum(k_raw * k_raw, axis=-1, keepdims=True), kv_width) * gain_k
        cos_tab, sin_tab = rope_tables(positions)
        q_rot = apply_rope(q_normed.reshape(BATCH_ROWS, N_HEADS, HEAD_DIM), cos_tab, sin_tab).astype(jnp.bfloat16)
        k_rot = apply_rope(k_normed.reshape(BATCH_ROWS, N_KV_HEADS, HEAD_DIM), cos_tab, sin_tab).astype(jnp.bfloat16)
        k_all = k_all.at[row_ids, :, positions, :].set(k_rot)
        v_all = v_all.at[row_ids, :, positions, :].set(v_new)
        attn_vals = lax.map(attend_row, (q_rot, k_all, v_all, positions))
        attn_sum = jnp.dot(attn_vals, w_o, preferred_element_type=jnp.float32).astype(jnp.bfloat16).astype(jnp.float32)
        hidden = (x_tok.astype(jnp.float32) + attn_sum * rms_factor(jnp.sum(attn_sum * attn_sum, axis=-1, keepdims=True), D_MODEL) * gain_a).astype(jnp.bfloat16)
        gate_pre = jnp.dot(hidden, w_gate, preferred_element_type=jnp.float32)
        up_pre = jnp.dot(hidden, w_up, preferred_element_type=jnp.float32)
        act_vals = (jax.nn.silu(gate_pre) * up_pre).astype(jnp.bfloat16)
        mlp_sum = jnp.dot(act_vals, w_down, preferred_element_type=jnp.float32).astype(jnp.bfloat16).astype(jnp.float32)
        y_tok = (hidden.astype(jnp.float32) + mlp_sum * rms_factor(jnp.sum(mlp_sum * mlp_sum, axis=-1, keepdims=True), D_MODEL) * gain_m).astype(jnp.bfloat16)
        return (k_all, v_all), y_tok

    (k_final, v_final), y_seq = lax.scan(one_step, (k_cache, v_cache), (x_seq, jnp.arange(STEPS, dtype=jnp.int32)))
    return (y_seq, k_final, v_final)
```

```python
import functools

import jax
import jax.numpy as jnp
from jax import lax
from jax.experimental import pallas as pl
from jax.experimental.pallas import tpu as pltpu
from jax.sharding import PartitionSpec as P

ROPE_THETA = 500000.0
NORM_EPS = 1e-6
F32 = jnp.float32
BF16 = jnp.bfloat16


def rms_factor(sq_sum, full_width):
    return lax.rsqrt(sq_sum / full_width + NORM_EPS)


def tail_kernel(dims, o_ref, ga_ref, gm_ref, x_hbm, wo_hbm, w1_hbm, w3_hbm, w2_hbm, y_hbm,
                buf, r0, r1, r2, st, own, act, w1, w3, w2, send_sem, recv_sem, w_sem, o_sem, x_sem, y_sem, free_sem):
    n_chunks, rows, d_model, q_loc, ff_loc = dims
    blk = rows // 8
    half_d = d_model // 2
    tp = lax.axis_index('tp')
    core = lax.rem(tp, 2)
    xb = lax.rem(lax.div(tp, 2), 2)
    yb = lax.div(tp, 4)
    sib = tp + 1 - 2 * core
    x_nb = tp + 2 - 4 * xb
    y_nb = tp + 4 - 8 * yb
    oc, ox, oy = 1 - core, 1 - xb, 1 - yb
    cols_a = pl.ds(0, half_d)
    cols_b = pl.ds(half_d, half_d)

    def block(c_bit, x_bit, y_bit):
        return c_bit * 4 + x_bit * 2 + y_bit

    me = block(core, xb, yb)

    wo_tile = 1024
    n_wo = d_model // wo_tile

    def wo_copy(j):
        cs = pl.ds(j * wo_tile, wo_tile)
        return pltpu.make_async_copy(wo_hbm.at[:, cs], w2.at[pl.ds(0, q_loc), cs], o_sem.at[j])

    def x_copy():
        return pltpu.make_async_copy(x_hbm.at[:, me], own, x_sem)

    n_k = 4
    k_rows = d_model // n_k

    def w13_copy(i, j):
        src, dst = ((w1_hbm, w1), (w3_hbm, w3))[i]
        rs = pl.ds(j * k_rows, k_rows)
        return pltpu.make_async_copy(src.at[rs], dst.at[rs], w_sem.at[i * n_k + j])

    f_rows = ff_loc // 4

    def w2_copy(j):
        rs = pl.ds(j * f_rows, f_rows)
        return pltpu.make_async_copy(w2_hbm.at[rs], w2.at[rs], w_sem.at[2 * n_k + j])

    for j in range(n_wo):
        wo_copy(j).start()
    x_copy().start()
    for j in range(n_k):
        for i in range(2):
            w13_copy(i, j).start()

    barrier = pltpu.get_barrier_semaphore()
    for peer in (sib, x_nb, y_nb):
        pl.semaphore_signal(barrier, inc=1, device_id={'tp': peer}, device_id_type=pl.DeviceIdType.MESH)
    pl.semaphore_wait(barrier, 3)

    def rcopy(k, c, s, src, dst, peer):
        return pltpu.make_async_remote_copy(
            src_ref=src, dst_ref=dst, send_sem=send_sem.at[k, c, s], recv_sem=recv_sem.at[k, c, s],
            device_id={'tp': peer}, device_id_type=pl.DeviceIdType.MESH)

    def xfer(k, c, s):
        b = buf.at[c]
        if s == 0:
            return rcopy(k, c, s, b.at[pl.ds(oc * 4, 4)], r0.at[c], sib)
        if s == 1:
            return rcopy(k, c, s, b.at[pl.ds(block(core, ox, 0), 2), :, cols_a], r1.at[c, :, :, cols_a], x_nb)
        if s in (2, 3):
            xx = s - 2
            return rcopy(k, c, s, b.at[block(core, xx, oy), :, cols_b], r1.at[c, xx, :, cols_b], y_nb)
        if s == 4:
            return rcopy(k, c, s, st.at[c, :, cols_a], r2.at[c, :, cols_a], y_nb)
        if s == 5:
            return rcopy(k, c, s, st.at[c, :, cols_b], r2.at[c, :, cols_b], x_nb)
        if s == 6:
            return rcopy(k, c, s, b.at[me, :, cols_a], b.at[me, :, cols_a], y_nb)
        if s == 7:
            return rcopy(k, c, s, b.at[me, :, cols_b], b.at[me, :, cols_b], x_nb)
        if s == 8:
            part = b.at[pl.ds(block(core, xb, 0), 2), :, cols_a]
            return rcopy(k, c, s, part, part, x_nb)
        if s in (9, 10):
            part = b.at[block(core, s - 9, yb), :, cols_b]
            return rcopy(k, c, s, part, part, y_nb)
        part = b.at[pl.ds(core * 4, 4)]
        return rcopy(k, c, s, part, part, sib)

    def start(k, c, *stages):
        for s in stages:
            xfer(k, c, s).start()

    def wait_recv(k, c, *stages):
        for s in stages:
            xfer(k, c, s).wait_recv()

    def wait_send(k, c, *stages):
        for s in stages:
            xfer(k, c, s).wait_send()

    v_tile = 512

    def add_cols(lo, hi, fn):
        def body(j, carry):
            fn(pl.ds(pl.multiple_of(j * v_tile, v_tile), v_tile))
            return carry
        lax.fori_loop(lo // v_tile, hi // v_tile, body, 0)

    def s0(k, c):
        start(k, c, 0)

    def s1(k, c):
        wait_recv(k, c, 0)
        wait_send(k, c, 0)
        pl.semaphore_signal(free_sem.at[k, c], inc=1, device_id={'tp': sib}, device_id_type=pl.DeviceIdType.MESH)
        mine = pl.ds(core * 4, 4)

        def add(cs):
            buf[c, mine, :, cs] = (buf[c, mine, :, cs].astype(F32) + r0[c, :, :, cs].astype(F32)).astype(BF16)
        add_cols(0, d_model, add)
        start(k, c, 1, 2, 3)

    def s2(k, c):
        wait_recv(k, c, 1, 2, 3)
        wait_send(k, c, 1, 2, 3)

        def pair(kept, sent, j_kept, j_sent, cs):
            st[c, :, cs] = (buf[c, sent, :, cs].astype(F32) + r1[c, j_sent, :, cs].astype(F32)).astype(BF16)
            buf[c, kept, :, cs] = (buf[c, kept, :, cs].astype(F32) + r1[c, j_kept, :, cs].astype(F32)).astype(BF16)

        def add_a(cs):
            pair(me, block(core, xb, oy), yb, oy, cs)

        def add_b(cs):
            pair(me, block(core, ox, yb), xb, ox, cs)
        add_cols(0, half_d, add_a)
        add_cols(half_d, d_model, add_b)
        start(k, c, 4, 5)

    def s3(k, c):
        wait_recv(k, c, 4, 5)
        wait_send(k, c, 4, 5)
        gain = ga_ref if k == 0 else gm_ref

        def total(j):
            cs = pl.ds(pl.multiple_of(j * v_tile, v_tile), v_tile)
            tot = (buf[c, me, :, cs].astype(F32) + r2[c, :, cs].astype(F32)).astype(BF16)
            buf[c, me, :, cs] = tot
            return tot.astype(F32)

        def sq_body(j, acc):
            tot = total(j)
            return acc + jnp.sum(tot * tot, axis=-1, keepdims=True)
        sq = lax.fori_loop(0, d_model // v_tile, sq_body, jnp.zeros((blk, 1), F32))
        scale = rms_factor(sq, d_model)

        def out_body(cs):
            res = (own[c, :, cs].astype(F32) + buf[c, me, :, cs].astype(F32) * scale * gain[:, cs].astype(F32)).astype(BF16)
            buf[c, me, :, cs] = res
            if k == 0:
                own[c, :, cs] = res
        add_cols(0, d_model, out_body)
        start(k, c, 6, 7)

    def g2(k, c):
        wait_recv(k, c, 6, 7)
        start(k, c, 8, 9, 10)

    def g3(k, c):
        wait_recv(k, c, 8, 9, 10)
        pl.semaphore_wait(free_sem.at[k, c], 1)
        start(k, c, 11)

    def done(k, c):
        wait_recv(k, c, 11)
        wait_send(k, c, 6, 7, 8, 9, 10, 11)

    def y_copy(c):
        return pltpu.make_async_copy(buf.at[c], y_hbm.at[c], y_sem.at[c])

    def fin(k, c):
        done(k, c)
        y_copy(c).start()

    def p1(c):
        def body(j, carry):
            cs = pl.ds(pl.multiple_of(j * wo_tile, wo_tile), wo_tile)
            acc = jnp.dot(o_ref[c], w2[0:q_loc, cs], preferred_element_type=F32)
            buf[c, :, :, cs] = acc.astype(BF16).reshape(8, blk, wo_tile)
            return carry
        lax.fori_loop(0, n_wo, body, 0)

    gu_tile = 256
    n_gu = ff_loc // gu_tile
    gu_tail = ff_loc - n_gu * gu_tile
    dn_tile = 512
    n_dn = d_model // dn_tile

    def gate_up(c, cs, width):
        h = buf[c].reshape(rows, d_model)
        gate = jnp.dot(h, w1[:, cs], preferred_element_type=F32)
        up = jnp.dot(h, w3[:, cs], preferred_element_type=F32)
        act[:, cs] = (gate * jax.nn.sigmoid(gate) * up).astype(BF16)

    def p2(services):
        n_steps = n_gu + 1 + n_dn

        def chunk(c, carry):
            def serve(step):
                for (sc, ss), fns in services.items():
                    @pl.when(jnp.logical_and(c == sc, step == ss))
                    def _(fns=fns):
                        for fn in fns:
                            fn()

            def gu_body(j, carry):
                serve(j)
                gate_up(c, pl.ds(pl.multiple_of(j * gu_tile, gu_tile), gu_tile), gu_tile)
                return carry
            lax.fori_loop(0, n_gu, gu_body, 0)
            if gu_tail:
                gate_up(c, slice(n_gu * gu_tile, ff_loc), gu_tail)

            def dn_body(j, carry):
                serve(j + n_gu)
                cs = pl.ds(pl.multiple_of(j * dn_tile, dn_tile), dn_tile)
                acc = jnp.dot(act[...], w2[:, cs], preferred_element_type=F32)
                buf[c, :, :, cs] = acc.astype(BF16).reshape(8, blk, dn_tile)
                return carry
            lax.fori_loop(0, n_dn, dn_body, 0)
            for sc in range(n_chunks):
                @pl.when(c == sc)
                def _(sc=sc):
                    s0(1, sc)
            return carry
        lax.fori_loop(0, n_chunks, chunk, 0)

    for j in range(n_wo):
        wo_copy(j).wait()
    p1(0)
    s0(0, 0)
    p1(1)
    s0(0, 1)
    s1(0, 0)
    p1(2)
    s0(0, 2)
    for j in range(4):
        w2_copy(j).start()
    s1(0, 1)
    s2(0, 0)
    s1(0, 2)
    x_copy().wait()
    s2(0, 1)
    s3(0, 0)
    s2(0, 2)
    s3(0, 1)
    g2(0, 0)
    s3(0, 2)
    g2(0, 1)
    g3(0, 0)
    for j in range(n_k):
        for i in range(2):
            w13_copy(i, j).wait()
    for j in range(4):
        w2_copy(j).wait()
    done(0, 0)

    F = functools.partial
    p2({
        (0, 0): [F(g2, 0, 2), F(g3, 0, 1)],
        (0, 4): [F(g3, 0, 2)],
        (1, 0): [F(done, 0, 1)],
        (1, 1): [F(s1, 1, 0)],
        (1, 3): [F(s2, 1, 0)],
        (1, 6): [F(s3, 1, 0)],
        (1, 10): [F(g2, 1, 0)],
        (1, 13): [F(g3, 1, 0)],
        (2, 0): [F(done, 0, 2)],
        (2, 1): [F(s1, 1, 1)],
        (2, 3): [F(s2, 1, 1)],
        (2, 6): [F(s3, 1, 1)],
        (2, 8): [F(fin, 1, 0)],
        (2, 10): [F(g2, 1, 1)],
        (2, 13): [F(g3, 1, 1)],
    })
    s1(1, 2)
    s2(1, 2)
    s3(1, 2)
    fin(1, 1)
    g2(1, 2)
    g3(1, 2)
    fin(1, 2)
    for c in range(n_chunks):
        y_copy(c).wait()


def tail(o, x_seq, w_o, w1, w3, w2, g_attn, g_mlp):
    n_chunks, rows, d_model = x_seq.shape
    q_loc = o.shape[-1]
    ff_loc = w1.shape[1]
    blk = rows // 8
    dims = (n_chunks, rows, d_model, q_loc, ff_loc)
    vmem = pl.BlockSpec(memory_space=pltpu.VMEM)
    hbm = pl.BlockSpec(memory_space=pl.ANY)
    y = pl.pallas_call(
        functools.partial(tail_kernel, dims),
        name='tail',
        out_shape=jax.ShapeDtypeStruct((n_chunks, 8, blk, d_model), BF16),
        in_specs=[vmem, vmem, vmem, hbm, hbm, hbm, hbm, hbm],
        out_specs=hbm,
        scratch_shapes=[
            pltpu.VMEM((n_chunks, 8, blk, d_model), BF16),
            pltpu.VMEM((n_chunks, 4, blk, d_model), BF16),
            pltpu.VMEM((n_chunks, 2, blk, d_model), BF16),
            pltpu.VMEM((n_chunks, blk, d_model), BF16),
            pltpu.VMEM((n_chunks, blk, d_model), BF16),
            pltpu.VMEM((n_chunks, blk, d_model), BF16),
            pltpu.VMEM((rows, ff_loc), BF16),
            pltpu.VMEM((d_model, ff_loc), BF16),
            pltpu.VMEM((d_model, ff_loc), BF16),
            pltpu.VMEM((ff_loc, d_model), BF16),
            pltpu.SemaphoreType.DMA((2, n_chunks, 12)),
            pltpu.SemaphoreType.DMA((2, n_chunks, 12)),
            pltpu.SemaphoreType.DMA((12,)),
            pltpu.SemaphoreType.DMA((d_model // 1024,)),
            pltpu.SemaphoreType.DMA,
            pltpu.SemaphoreType.DMA((n_chunks,)),
            pltpu.SemaphoreType.REGULAR((2, n_chunks)),
        ],
        compiler_params=pltpu.CompilerParams(collective_id=1, has_side_effects=True, vmem_limit_bytes=67043328),
    )(o, g_attn.reshape(1, -1), g_mlp.reshape(1, -1), x_seq.reshape(n_chunks, 8, blk, d_model), w_o, w1, w3, w2)
    return y.reshape(n_chunks, rows, d_model)


def rope_tables(positions, head_dim):
    half_dim = head_dim // 2
    inv_freq = ROPE_THETA ** (-(jnp.arange(half_dim, dtype=F32) * (2.0 / head_dim)))
    angles = positions.astype(F32)[:, None] * inv_freq[None, :]
    return jnp.cos(angles), jnp.sin(angles)


def apply_rope(head_vals, cos_tab, sin_tab):
    half_dim = head_vals.shape[-1] // 2
    lead = head_vals[..., :half_dim]
    tail_half = head_vals[..., half_dim:]
    cos_rows = cos_tab[:, None, :]
    sin_rows = sin_tab[:, None, :]
    return jnp.concatenate([lead * cos_rows - tail_half * sin_rows, tail_half * cos_rows + lead * sin_rows], axis=-1)


def local_layer(tp_size, x_seq, cache_len, k_cache, v_cache, w_q, w_k, w_v, w_o, w_gate, w_up, w_down, g_q, g_k, g_attn, g_mlp):
    n_steps, n_rows, d_model = x_seq.shape
    seq_max, head_dim = k_cache.shape[2:]
    q_loc = w_q.shape[1]
    heads = q_loc // head_dim
    x_all = x_seq.reshape(n_steps * n_rows, d_model)
    q_raw = jnp.dot(x_all, w_q, preferred_element_type=F32).astype(BF16).astype(F32)
    k_raw = jnp.dot(x_all, w_k, preferred_element_type=F32).astype(BF16).astype(F32)
    v_new = jnp.dot(x_all, w_v, preferred_element_type=F32).astype(BF16)
    sq = jnp.stack([jnp.sum(q_raw * q_raw, axis=-1), jnp.sum(k_raw * k_raw, axis=-1)])
    sq = lax.psum(sq, 'tp')
    pos = (jnp.arange(n_steps, dtype=jnp.int32)[:, None] + cache_len[None, :]).reshape(-1)
    cos_tab, sin_tab = rope_tables(pos, head_dim)
    q_n = (q_raw * rms_factor(sq[0], q_loc * tp_size)[:, None] * g_q.astype(F32)).reshape(-1, heads, head_dim)
    k_n = (k_raw * rms_factor(sq[1], head_dim * tp_size)[:, None] * g_k.astype(F32)).reshape(-1, 1, head_dim)
    q_rot = apply_rope(q_n, cos_tab, sin_tab).astype(BF16).reshape(n_steps, n_rows, heads, head_dim)
    k_rot = apply_rope(k_n, cos_tab, sin_tab).astype(BF16).reshape(n_steps, n_rows, head_dim)
    v_rot = v_new.reshape(n_steps, n_rows, head_dim)
    slot = jnp.arange(seq_max, dtype=jnp.int32)[None, :, None] - cache_len[:, None, None]
    k_out, v_out = k_cache[:, 0], v_cache[:, 0]
    for t in range(n_steps):
        k_out = jnp.where(slot == t, k_rot[t][:, None, :], k_out)
        v_out = jnp.where(slot == t, v_rot[t][:, None, :], v_out)
    q_seq = q_rot.transpose(1, 0, 2, 3).reshape(n_rows, n_steps * heads, head_dim)
    s = jnp.einsum('bqd,bsd->bqs', q_seq, k_out, preferred_element_type=F32) * head_dim ** -0.5
    limit = cache_len[:, None] + jnp.repeat(jnp.arange(n_steps, dtype=jnp.int32), heads)[None, :]
    s = jnp.where(jnp.arange(seq_max)[None, None, :] <= limit[:, :, None], s, -jnp.inf)
    e = jnp.exp(s - jnp.max(s, axis=-1, keepdims=True))
    l = jnp.sum(e, axis=-1, keepdims=True)
    o = jnp.einsum('bqs,bsd->bqd', e.astype(BF16), v_out, preferred_element_type=F32)
    o = (o / l).astype(BF16).reshape(n_rows, n_steps, q_loc).transpose(1, 0, 2)
    y = tail(o, x_seq, w_o, w_gate, w_up, w_down, g_attn, g_mlp)
    return y, k_out[:, None], v_out[:, None]


def solution(mesh):
    tp_size = mesh.shape['tp']
    data_spec = P(None, 'dp', None)
    cache_spec = P('dp', 'tp', None, None)
    col_spec = P(None, 'tp')
    row_spec = P('tp', None)
    arg_specs = (data_spec, P('dp'), cache_spec, cache_spec, col_spec, col_spec, col_spec, row_spec, col_spec, col_spec, row_spec, P('tp'), P('tp'), P(None), P(None))
    out_specs = (data_spec, cache_spec, cache_spec)
    return jax.shard_map(functools.partial(local_layer, tp_size), mesh=mesh, in_specs=arg_specs, out_specs=out_specs, check_vma=False)
```

```python
import functools

import jax
import jax.numpy as jnp
from jax import lax
from jax.experimental import pallas as pl
from jax.experimental.pallas import tpu as pltpu
from jax.sharding import PartitionSpec as P

ROPE_THETA = 500000.0
NORM_EPS = 1e-6
F32 = jnp.float32
BF16 = jnp.bfloat16


def rms_factor(sq_sum, full_width):
    return lax.rsqrt(sq_sum / full_width + NORM_EPS)


def tail_kernel(dims, o_ref, ga_ref, gm_ref, x_hbm, wo_hbm, w1_hbm, w3_hbm, w2_hbm, y_hbm,
                buf, r0, r1, r2, st, own, act, w1, w3, w2, send_sem, recv_sem, w_sem, o_sem, x_sem, y_sem, free_sem):
    n_chunks, rows, d_model, q_loc, ff_loc = dims
    blk = rows // 8
    half_d = d_model // 2
    tp = lax.axis_index('tp')
    core = lax.rem(tp, 2)
    xb = lax.rem(lax.div(tp, 2), 2)
    yb = lax.div(tp, 4)
    sib = tp + 1 - 2 * core
    x_nb = tp + 2 - 4 * xb
    y_nb = tp + 4 - 8 * yb
    oc, ox, oy = 1 - core, 1 - xb, 1 - yb
    cols_a = pl.ds(0, half_d)
    cols_b = pl.ds(half_d, half_d)

    def block(c_bit, x_bit, y_bit):
        return c_bit * 4 + x_bit * 2 + y_bit

    me = block(core, xb, yb)

    wo_tile = 1024
    n_wo = d_model // wo_tile

    def wo_copy(j):
        cs = pl.ds(j * wo_tile, wo_tile)
        return pltpu.make_async_copy(wo_hbm.at[:, cs], w2.at[pl.ds(0, q_loc), cs], o_sem.at[j])

    def x_copy():
        return pltpu.make_async_copy(x_hbm.at[:, me], own, x_sem)

    n_k = 4
    k_rows = ff_loc // n_k

    def w13_copy(i, j):
        src, dst = ((w1_hbm, w1), (w3_hbm, w3))[i]
        rs = pl.ds(j * k_rows, k_rows)
        return pltpu.make_async_copy(src.at[rs], dst.at[rs], w_sem.at[i * n_k + j])

    f_rows = ff_loc // 4

    def w2_copy(j):
        rs = pl.ds(j * f_rows, f_rows)
        return pltpu.make_async_copy(w2_hbm.at[rs], w2.at[rs], w_sem.at[2 * n_k + j])

    for j in range(n_wo):
        wo_copy(j).start()
    x_copy().start()
    for j in range(n_k):
        for i in range(2):
            w13_copy(i, j).start()

    barrier = pltpu.get_barrier_semaphore()
    for peer in (sib, x_nb, y_nb):
        pl.semaphore_signal(barrier, inc=1, device_id={'tp': peer}, device_id_type=pl.DeviceIdType.MESH)
    pl.semaphore_wait(barrier, 3)

    def rcopy(k, c, s, src, dst, peer):
        return pltpu.make_async_remote_copy(
            src_ref=src, dst_ref=dst, send_sem=send_sem.at[k, c, s], recv_sem=recv_sem.at[k, c, s],
            device_id={'tp': peer}, device_id_type=pl.DeviceIdType.MESH)

    def xfer(k, c, s):
        b = buf.at[c]
        if s == 0:
            return rcopy(k, c, s, b.at[pl.ds(oc * 4, 4)], r0.at[c], sib)
        if s == 1:
            return rcopy(k, c, s, b.at[pl.ds(block(core, ox, 0), 2), :, cols_a], r1.at[c, :, :, cols_a], x_nb)
        if s in (2, 3):
            xx = s - 2
            return rcopy(k, c, s, b.at[block(core, xx, oy), :, cols_b], r1.at[c, xx, :, cols_b], y_nb)
        if s == 4:
            return rcopy(k, c, s, st.at[c, :, cols_a], r2.at[c, :, cols_a], y_nb)
        if s == 5:
            return rcopy(k, c, s, st.at[c, :, cols_b], r2.at[c, :, cols_b], x_nb)
        if s == 6:
            return rcopy(k, c, s, b.at[me, :, cols_a], b.at[me, :, cols_a], y_nb)
        if s == 7:
            return rcopy(k, c, s, b.at[me, :, cols_b], b.at[me, :, cols_b], x_nb)
        if s == 8:
            part = b.at[pl.ds(block(core, xb, 0), 2), :, cols_a]
            return rcopy(k, c, s, part, part, x_nb)
        if s in (9, 10):
            part = b.at[block(core, s - 9, yb), :, cols_b]
            return rcopy(k, c, s, part, part, y_nb)
        part = b.at[pl.ds(core * 4, 4)]
        return rcopy(k, c, s, part, part, sib)

    def start(k, c, *stages):
        for s in stages:
            xfer(k, c, s).start()

    def wait_recv(k, c, *stages):
        for s in stages:
            xfer(k, c, s).wait_recv()

    def wait_send(k, c, *stages):
        for s in stages:
            xfer(k, c, s).wait_send()

    v_tile = 512

    def add_cols(lo, hi, fn):
        def body(j, carry):
            fn(pl.ds(pl.multiple_of(j * v_tile, v_tile), v_tile))
            return carry
        lax.fori_loop(lo // v_tile, hi // v_tile, body, 0)

    def s0(k, c):
        start(k, c, 0)

    def s1(k, c):
        wait_recv(k, c, 0)
        wait_send(k, c, 0)
        pl.semaphore_signal(free_sem.at[k, c], inc=1, device_id={'tp': sib}, device_id_type=pl.DeviceIdType.MESH)
        mine = pl.ds(core * 4, 4)

        def add(cs):
            buf[c, mine, :, cs] = (buf[c, mine, :, cs].astype(F32) + r0[c, :, :, cs].astype(F32)).astype(BF16)
        add_cols(0, d_model, add)
        start(k, c, 1, 2, 3)

    def s2(k, c):
        wait_recv(k, c, 1, 2, 3)
        wait_send(k, c, 1, 2, 3)

        def pair(kept, sent, j_kept, j_sent, cs):
            st[c, :, cs] = (buf[c, sent, :, cs].astype(F32) + r1[c, j_sent, :, cs].astype(F32)).astype(BF16)
            buf[c, kept, :, cs] = (buf[c, kept, :, cs].astype(F32) + r1[c, j_kept, :, cs].astype(F32)).astype(BF16)

        def add_a(cs):
            pair(me, block(core, xb, oy), yb, oy, cs)

        def add_b(cs):
            pair(me, block(core, ox, yb), xb, ox, cs)
        add_cols(0, half_d, add_a)
        add_cols(half_d, d_model, add_b)
        start(k, c, 4, 5)

    def s3(k, c):
        wait_recv(k, c, 4, 5)
        wait_send(k, c, 4, 5)
        gain = ga_ref if k == 0 else gm_ref

        def total(j):
            cs = pl.ds(pl.multiple_of(j * v_tile, v_tile), v_tile)
            tot = (buf[c, me, :, cs].astype(F32) + r2[c, :, cs].astype(F32)).astype(BF16)
            buf[c, me, :, cs] = tot
            return tot.astype(F32)

        def sq_body(j, acc):
            tot = total(j)
            return acc + jnp.sum(tot * tot, axis=-1, keepdims=True)
        sq = lax.fori_loop(0, d_model // v_tile, sq_body, jnp.zeros((blk, 1), F32))
        scale = rms_factor(sq, d_model)

        def out_body(cs):
            res = (own[c, :, cs].astype(F32) + buf[c, me, :, cs].astype(F32) * scale * gain[:, cs].astype(F32)).astype(BF16)
            buf[c, me, :, cs] = res
            if k == 0:
                own[c, :, cs] = res
        add_cols(0, d_model, out_body)
        start(k, c, 6, 7)

    def g2(k, c):
        wait_recv(k, c, 6, 7)
        start(k, c, 8, 9, 10)

    def g3(k, c):
        wait_recv(k, c, 8, 9, 10)
        pl.semaphore_wait(free_sem.at[k, c], 1)
        start(k, c, 11)

    def done(k, c):
        wait_recv(k, c, 11)
        wait_send(k, c, 6, 7, 8, 9, 10, 11)

    def y_copy(c):
        return pltpu.make_async_copy(buf.at[c], y_hbm.at[c], y_sem.at[c])

    def fin(k, c):
        done(k, c)
        y_copy(c).start()

    def p1(c):
        def body(j, carry):
            cs = pl.ds(pl.multiple_of(j * wo_tile, wo_tile), wo_tile)
            acc = jnp.dot(o_ref[c], w2[0:q_loc, cs], preferred_element_type=F32)
            buf[c, :, :, cs] = acc.astype(BF16).reshape(8, blk, wo_tile)
            return carry
        lax.fori_loop(0, n_wo, body, 0)

    gu_tile = 256
    n_gu = ff_loc // gu_tile
    gu_tail = ff_loc - n_gu * gu_tile
    dn_tile = 512
    n_dn = d_model // dn_tile

    def dot_t(lhs, rhs):
        return lax.dot_general(lhs, rhs, (((1,), (1,)), ((), ())), preferred_element_type=F32)

    def gate_up(c, cs, width):
        h = buf[c].reshape(rows, d_model)
        gate = dot_t(h, w1[cs, :])
        up = dot_t(h, w3[cs, :])
        act[:, cs] = (gate * jax.nn.sigmoid(gate) * up).astype(BF16)

    def p2(services):
        n_steps = n_gu + 1 + n_dn

        def chunk(c, carry):
            def serve(step):
                for (sc, ss), fns in services.items():
                    @pl.when(jnp.logical_and(c == sc, step == ss))
                    def _(fns=fns):
                        for fn in fns:
                            fn()

            def gu_body(j, carry):
                serve(j)
                gate_up(c, pl.ds(pl.multiple_of(j * gu_tile, gu_tile), gu_tile), gu_tile)
                return carry
            lax.fori_loop(0, n_gu, gu_body, 0)
            if gu_tail:
                gate_up(c, slice(n_gu * gu_tile, ff_loc), gu_tail)

            def dn_body(j, carry):
                serve(j + n_gu)
                cs = pl.ds(pl.multiple_of(j * dn_tile, dn_tile), dn_tile)
                acc = jnp.dot(act[...], w2[:, cs], preferred_element_type=F32)
                buf[c, :, :, cs] = acc.astype(BF16).reshape(8, blk, dn_tile)
                return carry
            lax.fori_loop(0, n_dn, dn_body, 0)
            for sc in range(n_chunks):
                @pl.when(c == sc)
                def _(sc=sc):
                    s0(1, sc)
            return carry
        lax.fori_loop(0, n_chunks, chunk, 0)

    for j in range(n_wo):
        wo_copy(j).wait()
    p1(0)
    s0(0, 0)
    p1(1)
    s0(0, 1)
    s1(0, 0)
    p1(2)
    s0(0, 2)
    for j in range(4):
        w2_copy(j).start()
    s1(0, 1)
    s2(0, 0)
    s1(0, 2)
    x_copy().wait()
    s2(0, 1)
    s3(0, 0)
    s2(0, 2)
    s3(0, 1)
    g2(0, 0)
    s3(0, 2)
    g2(0, 1)
    g3(0, 0)
    for j in range(n_k):
        for i in range(2):
            w13_copy(i, j).wait()
    for j in range(4):
        w2_copy(j).wait()
    done(0, 0)

    F = functools.partial
    p2({
        (0, 0): [F(g2, 0, 2), F(g3, 0, 1)],
        (0, 4): [F(g3, 0, 2)],
        (1, 0): [F(done, 0, 1)],
        (1, 1): [F(s1, 1, 0)],
        (1, 3): [F(s2, 1, 0)],
        (1, 6): [F(s3, 1, 0)],
        (1, 10): [F(g2, 1, 0)],
        (1, 13): [F(g3, 1, 0)],
        (2, 0): [F(done, 0, 2)],
        (2, 1): [F(s1, 1, 1)],
        (2, 3): [F(s2, 1, 1)],
        (2, 6): [F(s3, 1, 1)],
        (2, 8): [F(fin, 1, 0)],
        (2, 10): [F(g2, 1, 1)],
        (2, 13): [F(g3, 1, 1)],
    })
    s1(1, 2)
    s2(1, 2)
    s3(1, 2)
    fin(1, 1)
    g2(1, 2)
    g3(1, 2)
    fin(1, 2)
    for c in range(n_chunks):
        y_copy(c).wait()


def tail(o, x_seq, w_o, w1, w3, w2, g_attn, g_mlp):
    n_chunks, rows, d_model = x_seq.shape
    q_loc = o.shape[-1]
    ff_loc = w2.shape[0]
    blk = rows // 8
    dims = (n_chunks, rows, d_model, q_loc, ff_loc)
    vmem = pl.BlockSpec(memory_space=pltpu.VMEM)
    hbm = pl.BlockSpec(memory_space=pl.ANY)
    y = pl.pallas_call(
        functools.partial(tail_kernel, dims),
        name='tail',
        out_shape=jax.ShapeDtypeStruct((n_chunks, 8, blk, d_model), BF16),
        in_specs=[vmem, vmem, vmem, hbm, hbm, hbm, hbm, hbm],
        out_specs=hbm,
        scratch_shapes=[
            pltpu.VMEM((n_chunks, 8, blk, d_model), BF16),
            pltpu.VMEM((n_chunks, 4, blk, d_model), BF16),
            pltpu.VMEM((n_chunks, 2, blk, d_model), BF16),
            pltpu.VMEM((n_chunks, blk, d_model), BF16),
            pltpu.VMEM((n_chunks, blk, d_model), BF16),
            pltpu.VMEM((n_chunks, blk, d_model), BF16),
            pltpu.VMEM((rows, ff_loc), BF16),
            pltpu.VMEM((ff_loc, d_model), BF16),
            pltpu.VMEM((ff_loc, d_model), BF16),
            pltpu.VMEM((ff_loc, d_model), BF16),
            pltpu.SemaphoreType.DMA((2, n_chunks, 12)),
            pltpu.SemaphoreType.DMA((2, n_chunks, 12)),
            pltpu.SemaphoreType.DMA((12,)),
            pltpu.SemaphoreType.DMA((d_model // 1024,)),
            pltpu.SemaphoreType.DMA,
            pltpu.SemaphoreType.DMA((n_chunks,)),
            pltpu.SemaphoreType.REGULAR((2, n_chunks)),
        ],
        compiler_params=pltpu.CompilerParams(collective_id=1, has_side_effects=True, vmem_limit_bytes=67043328),
    )(o, g_attn.reshape(1, -1), g_mlp.reshape(1, -1), x_seq.reshape(n_chunks, 8, blk, d_model), w_o, w1.T, w3.T, w2)
    return y.reshape(n_chunks, rows, d_model)


def head_kernel(dims, len_ref, gq_ref, gk_ref, freq_ref, x_hbm, wq_hbm, wk_hbm, wv_hbm, q_out, k_out, v_out,
                x, w, raw, cos_t, sin_t, sums, x_sem, w_sem, send_sem, recv_sem):
    n_steps, rows, d_model, q_loc, hd, n_tp = dims
    heads = q_loc // hd
    width = q_loc + 2 * hd
    tp = lax.axis_index('tp')

    def x_copy(t):
        return pltpu.make_async_copy(x_hbm.at[t], x.at[t], x_sem.at[t])

    n_k = 4
    k_rows = d_model // n_k

    def w_copies(j):
        rs = pl.ds(j * k_rows, k_rows)
        return (pltpu.make_async_copy(wq_hbm.at[rs], w.at[rs, pl.ds(0, q_loc)], w_sem.at[0, j]),
                pltpu.make_async_copy(wk_hbm.at[rs], w.at[rs, pl.ds(q_loc, hd)], w_sem.at[1, j]),
                pltpu.make_async_copy(wv_hbm.at[rs], w.at[rs, pl.ds(q_loc + hd, hd)], w_sem.at[2, j]))

    x_copy(0).start()
    for j in range(n_k):
        for cp in w_copies(j):
            cp.start()
    for t in range(1, n_steps):
        x_copy(t).start()

    barrier = pltpu.get_barrier_semaphore()
    peers = [lax.rem(tp + d, n_tp) for d in range(1, n_tp)]
    for p in peers:
        pl.semaphore_signal(barrier, inc=1, device_id={'tp': p}, device_id_type=pl.DeviceIdType.MESH)

    lens = jnp.transpose(jnp.broadcast_to(len_ref[...].astype(F32), (rows, rows)))
    lane = lax.broadcasted_iota(jnp.int32, (rows, hd), 1)
    sign = jnp.where(lane < hd // 2, -1.0, 1.0).astype(F32)
    for t in range(n_steps):
        ang = (lens + float(t)) * freq_ref[...]
        cos_t[t] = jnp.cos(ang)
        sin_t[t] = jnp.sin(ang) * sign

    for j in range(n_k):
        for cp in w_copies(j):
            cp.wait()
    part = jnp.zeros((rows, rows), F32)
    sq_lane = lax.broadcasted_iota(jnp.int32, (rows, rows), 1)
    for t in range(n_steps):
        x_copy(t).wait()
        res = jnp.dot(x[t], w[...], preferred_element_type=F32).astype(BF16)
        raw[t] = res
        q = res[:, :q_loc].astype(F32)
        k = res[:, q_loc:q_loc + hd].astype(F32)
        part = jnp.where(sq_lane == 2 * t, jnp.sum(q * q, axis=-1, keepdims=True), part)
        part = jnp.where(sq_lane == 2 * t + 1, jnp.sum(k * k, axis=-1, keepdims=True), part)
    sums[tp] = jnp.transpose(part)[0:8]
    pl.semaphore_wait(barrier, n_tp - 1)

    def send(d):
        return pltpu.make_async_remote_copy(
            src_ref=sums.at[tp], dst_ref=sums.at[tp], send_sem=send_sem.at[d], recv_sem=recv_sem.at[d],
            device_id={'tp': peers[d]}, device_id_type=pl.DeviceIdType.MESH)

    for d in range(n_tp - 1):
        send(d).start()
    q_out[pl.ds(n_steps * heads, rows, stride=16), :] = jnp.zeros((rows, hd), F32)
    for t in range(n_steps):
        v_out[t] = raw[t, :, q_loc + hd:width].astype(F32)
    for d in range(n_tp - 1):
        send(d).wait()
    tot = sums[0]
    for d in range(1, n_tp):
        tot = tot + sums[d]
    full = jnp.transpose(jnp.concatenate([tot, jnp.zeros((rows - 8, rows), F32)], axis=0))
    for t in range(n_steps):
        q_scale = rms_factor(full[:, 2 * t:2 * t + 1], q_loc * n_tp)
        k_scale = rms_factor(full[:, 2 * t + 1:2 * t + 2], hd * n_tp)

        def rotate(col, scale, gain):
            val = raw[t, :, col:col + hd].astype(F32) * scale * gain.astype(F32)
            return (val * cos_t[t] + pltpu.roll(val, hd // 2, 1) * sin_t[t]).astype(BF16).astype(F32)
        for j in range(heads):
            q_out[pl.ds(t * heads + j, rows, stride=16), :] = rotate(j * hd, q_scale, gq_ref[:, j * hd:(j + 1) * hd])
        k_out[t] = rotate(q_loc, k_scale, gk_ref[...])


def head(x_seq, cache_len, w_q, w_k, w_v, g_q, g_k, n_tp):
    n_steps, rows, d_model = x_seq.shape
    q_loc, hd = w_q.shape[1], w_k.shape[1]
    width = q_loc + 2 * hd
    half = hd // 2
    inv_freq = ROPE_THETA ** (-(jnp.arange(half, dtype=F32) * (2.0 / hd)))
    freq = jnp.concatenate([inv_freq, inv_freq]).reshape(1, hd)
    vmem = pl.BlockSpec(memory_space=pltpu.VMEM)
    hbm = pl.BlockSpec(memory_space=pl.ANY)
    return pl.pallas_call(
        functools.partial(head_kernel, (n_steps, rows, d_model, q_loc, hd, n_tp)),
        name='head',
        out_shape=(jax.ShapeDtypeStruct((rows * 16, hd), F32),
                   jax.ShapeDtypeStruct((n_steps, rows, hd), F32),
                   jax.ShapeDtypeStruct((n_steps, rows, hd), F32)),
        in_specs=[vmem] * 4 + [hbm] * 4,
        out_specs=(vmem,) * 3,
        scratch_shapes=[
            pltpu.VMEM((n_steps, rows, d_model), BF16),
            pltpu.VMEM((d_model, width), BF16),
            pltpu.VMEM((n_steps, rows, width), BF16),
            pltpu.VMEM((n_steps, rows, hd), F32),
            pltpu.VMEM((n_steps, rows, hd), F32),
            pltpu.VMEM((n_tp, 8, rows), F32),
            pltpu.SemaphoreType.DMA((n_steps,)),
            pltpu.SemaphoreType.DMA((3, 4)),
            pltpu.SemaphoreType.DMA((n_tp - 1,)),
            pltpu.SemaphoreType.DMA((n_tp - 1,)),
        ],
        compiler_params=pltpu.CompilerParams(collective_id=0, has_side_effects=True, vmem_limit_bytes=67043328),
    )(cache_len.reshape(1, -1), g_q.reshape(1, -1), g_k.reshape(1, -1), freq, x_seq, w_q, w_k, w_v)


def attn_kernel(dims, len_ref, q_ref, kn_ref, vn_ref, k_ref, v_ref, o_ref, ko_ref, vo_ref, o_scr):
    n_steps, nb, heads, hd, seq_max = dims
    first = pl.program_id(0) * nb
    win = 32
    row_step = lax.broadcasted_iota(jnp.int32, (16, seq_max), 0) // heads
    col = lax.broadcasted_iota(jnp.int32, (16, seq_max), 1)
    ahead = col - row_step
    win_row = lax.broadcasted_iota(jnp.int32, (win, hd), 0)
    for i in range(nb):
        ln = len_ref[first + i]
        base = pl.multiple_of(jnp.minimum((ln // 16) * 16, seq_max - win), 16)
        rel = win_row + (base - ln)
        for src, new, dst in ((k_ref, kn_ref, ko_ref), (v_ref, vn_ref, vo_ref)):
            dst[i] = src[i]
            cut = src[i, pl.ds(base, win), :].astype(F32)
            for t in range(n_steps):
                cut = jnp.where(rel == t, new[t, i:i + 1, :], cut)
            dst[i, pl.ds(base, win), :] = cut.astype(BF16)
        q = q_ref[i].astype(BF16)
        s = lax.dot_general(q, ko_ref[i], (((1,), (1,)), ((), ())), preferred_element_type=F32) * hd ** -0.5
        s = jnp.where(ahead <= ln, s, -jnp.inf)
        e = jnp.exp(s - jnp.max(s, axis=-1, keepdims=True))
        l = jnp.sum(e, axis=-1, keepdims=True)
        o = jnp.dot(e.astype(BF16), vo_ref[i], preferred_element_type=F32) / l
        o_scr[i * 16:(i + 1) * 16, :] = o
    for t in range(n_steps):
        for j in range(heads):
            o_ref[t, :, j * hd:(j + 1) * hd] = o_scr[pl.ds(t * heads + j, nb, stride=16), :].astype(BF16)


def attend(q, kn, vn, k_cache, v_cache, cache_len, heads):
    n_rows, _, seq_max, hd = k_cache.shape
    n_steps = kn.shape[0]
    nb = 16
    cache_spec = pl.BlockSpec((nb, seq_max, hd), lambda i, ln: (i, 0, 0))
    new_spec = pl.BlockSpec((n_steps, nb, hd), lambda i, ln: (0, i, 0))
    cache_shape = jax.ShapeDtypeStruct((n_rows, seq_max, hd), BF16)
    flops = 4 * n_rows * 16 * seq_max * hd
    return pl.pallas_call(
        functools.partial(attn_kernel, (n_steps, nb, heads, hd, seq_max)),
        name='attend',
        grid_spec=pltpu.PrefetchScalarGridSpec(
            num_scalar_prefetch=1,
            grid=(n_rows // nb,),
            in_specs=[pl.BlockSpec((nb, 16, hd), lambda i, ln: (i, 0, 0)), new_spec, new_spec, cache_spec, cache_spec],
            out_specs=(pl.BlockSpec((n_steps, nb, heads * hd), lambda i, ln: (0, i, 0)), cache_spec, cache_spec),
            scratch_shapes=[pltpu.VMEM((nb * 16, hd), F32)],
        ),
        out_shape=(jax.ShapeDtypeStruct((n_steps, n_rows, heads * hd), BF16), cache_shape, cache_shape),
        compiler_params=pltpu.CompilerParams(vmem_limit_bytes=67043328),
        cost_estimate=pl.CostEstimate(flops=flops, bytes_accessed=4 * n_rows * seq_max * hd * 2, transcendentals=n_rows * 16 * seq_max),
    )(cache_len, q.reshape(n_rows, 16, hd), kn, vn, k_cache[:, 0], v_cache[:, 0])


def local_layer(n_tp, x_seq, cache_len, k_cache, v_cache, w_q, w_k, w_v, w_o, w_gate, w_up, w_down, g_q, g_k, g_attn, g_mlp):
    heads = w_q.shape[1] // k_cache.shape[3]
    q, kn, vn = head(x_seq, cache_len, w_q, w_k, w_v, g_q, g_k, n_tp)
    o, k_out, v_out = attend(q, kn, vn, k_cache, v_cache, cache_len, heads)
    y = tail(o, x_seq, w_o, w_gate, w_up, w_down, g_attn, g_mlp)
    return y, k_out[:, None], v_out[:, None]


def solution(mesh):
    tp_size = mesh.shape['tp']
    data_spec = P(None, 'dp', None)
    cache_spec = P('dp', 'tp', None, None)
    col_spec = P(None, 'tp')
    row_spec = P('tp', None)
    arg_specs = (data_spec, P('dp'), cache_spec, cache_spec, col_spec, col_spec, col_spec, row_spec, col_spec, col_spec, row_spec, P('tp'), P('tp'), P(None), P(None))
    out_specs = (data_spec, cache_spec, cache_spec)
    return jax.shard_map(functools.partial(local_layer, tp_size), mesh=mesh, in_specs=arg_specs, out_specs=out_specs, check_vma=False)
```

```python
import functools

import jax
import jax.numpy as jnp
import numpy as np
from jax import lax
from jax.experimental import pallas as pl
from jax.experimental.pallas import tpu as pltpu
from jax.sharding import PartitionSpec as P

ROPE_THETA = 500000.0
NORM_EPS = 1e-6
F32 = jnp.float32
BF16 = jnp.bfloat16


def rms_factor(sq_sum, full_width):
    return lax.rsqrt(sq_sum / full_width + NORM_EPS)


def tail_kernel(dims, o_ref, ga_ref, gm_ref, x_hbm, wo_hbm, w1_hbm, w3_hbm, w2_hbm, y_hbm,
                buf, r0, r1, r2, st, own, act, gains, w1, w3, w2,
                send_sem, recv_sem, w_sem, o_sem, x_sem, y_sem, free_sem):
    n_chunks, rows, d_model, q_loc, ff_loc = dims
    blk = rows // 8
    half_d = d_model // 2
    tp = lax.axis_index('tp')
    core = lax.rem(tp, 2)
    xb = lax.rem(lax.div(tp, 2), 2)
    yb = lax.div(tp, 4)
    sib = tp + 1 - 2 * core
    x_nb = tp + 2 - 4 * xb
    y_nb = tp + 4 - 8 * yb
    oc, ox, oy = 1 - core, 1 - xb, 1 - yb
    cols = (pl.ds(0, half_d), pl.ds(half_d, half_d))
    me = core * 4 + xb * 2 + yb

    n_wo = 4
    wo_tile = d_model // n_wo

    def wo_copy(j):
        cs = pl.ds(j * wo_tile, wo_tile)
        return pltpu.make_async_copy(wo_hbm.at[:, cs], w2.at[pl.ds(0, q_loc), cs], o_sem.at[j])

    def x_copy():
        return pltpu.make_async_copy(x_hbm.at[:, me], own, x_sem)

    n_k = 4
    k_rows = ff_loc // n_k

    def w_copy(i, j):
        src, dst = ((w1_hbm, w1), (w3_hbm, w3), (w2_hbm, w2))[i]
        rs = pl.ds(j * k_rows, k_rows)
        return pltpu.make_async_copy(src.at[rs], dst.at[rs], w_sem.at[i, j])

    for j in range(n_wo):
        wo_copy(j).start()
    x_copy().start()
    for j in range(n_k):
        for i in range(2):
            w_copy(i, j).start()

    barrier = pltpu.get_barrier_semaphore()
    for peer in (sib, x_nb, y_nb):
        pl.semaphore_signal(barrier, inc=1, device_id={'tp': peer}, device_id_type=pl.DeviceIdType.MESH)
    for i, g_ref in enumerate((ga_ref, gm_ref)):
        for j in range(d_model // 128):
            gains[i:i + 1, j * 128:(j + 1) * 128] = g_ref[j:j + 1, :].astype(F32)
    pl.semaphore_wait(barrier, 3)

    def xfer(k, c, s):
        ab = s % 2
        cs = cols[ab]
        b = buf.at[c]
        if s < 2:
            src, dst, peer = b.at[oc, :, :, :, cs], r0.at[c, :, :, :, cs], sib
        elif s == 2:
            src, dst, peer = b.at[core, ox, :, :, cs], r1.at[c, :, :, cs], x_nb
        elif s == 3:
            src, dst, peer = b.at[core, :, oy, :, cs], r1.at[c, :, :, cs], y_nb
        elif s < 6:
            src, dst, peer = st.at[c, :, cs], r2.at[c, :, cs], (y_nb, x_nb)[ab]
        else:
            if s < 8:
                src, peer = b.at[core, xb, yb, :, cs], (y_nb, x_nb)[ab]
            elif s == 8:
                src, peer = b.at[core, xb, :, :, cs], x_nb
            elif s == 9:
                src, peer = b.at[core, :, yb, :, cs], y_nb
            else:
                src, peer = b.at[core, :, :, :, cs], sib
            dst = src
        return pltpu.make_async_remote_copy(
            src_ref=src, dst_ref=dst, send_sem=send_sem.at[k, c, s], recv_sem=recv_sem.at[k, c, s],
            device_id={'tp': peer}, device_id_type=pl.DeviceIdType.MESH)

    def start(k, c, s):
        xfer(k, c, s).start()

    def s0(k, c, ab):
        start(k, c, ab)

    def s1(k, c, ab):
        cs = cols[ab]
        x = xfer(k, c, ab)
        x.wait_recv()
        if ab == 0:
            buf[c, core, ox, :, :, cs] = buf[c, core, ox, :, :, cs] + r0[c, ox, :, :, cs]
            start(k, c, 2)
            buf[c, core, xb, :, :, cs] = buf[c, core, xb, :, :, cs] + r0[c, xb, :, :, cs]
        else:
            for i in range(2):
                buf[c, core, i, oy, :, cs] = buf[c, core, i, oy, :, cs] + r0[c, i, oy, :, cs]
            start(k, c, 3)
            for i in range(2):
                buf[c, core, i, yb, :, cs] = buf[c, core, i, yb, :, cs] + r0[c, i, yb, :, cs]
        x.wait_send()
        if ab == 1:
            pl.semaphore_signal(free_sem.at[k, c], inc=1, device_id={'tp': sib}, device_id_type=pl.DeviceIdType.MESH)

    def s2(k, c, ab):
        cs = cols[ab]
        x = xfer(k, c, 2 + ab)
        x.wait_recv()
        if ab == 0:
            st[c, :, cs] = buf[c, core, xb, oy, :, cs] + r1[c, oy, :, cs]
            start(k, c, 4)
            buf[c, core, xb, yb, :, cs] = buf[c, core, xb, yb, :, cs] + r1[c, yb, :, cs]
        else:
            st[c, :, cs] = buf[c, core, ox, yb, :, cs] + r1[c, ox, :, cs]
            start(k, c, 5)
            buf[c, core, xb, yb, :, cs] = buf[c, core, xb, yb, :, cs] + r1[c, xb, :, cs]
        x.wait_send()

    v_tile = 512

    def s3(k, c):
        xfer(k, c, 4).wait_recv()
        xfer(k, c, 5).wait_recv()
        sq = jnp.zeros((blk, v_tile), F32)
        for j in range(d_model // v_tile):
            cs = pl.ds(j * v_tile, v_tile)
            tot = (buf[c, core, xb, yb, :, cs].astype(F32) + r2[c, :, cs].astype(F32)).astype(BF16)
            buf[c, core, xb, yb, :, cs] = tot
            tot = tot.astype(F32)
            sq = sq + tot * tot
        scale = rms_factor(jnp.sum(sq, axis=-1, keepdims=True), d_model)
        for ab in range(2):
            for j in range(half_d // v_tile):
                cs = pl.ds(ab * half_d + j * v_tile, v_tile)
                res = (own[c, :, cs].astype(F32) + buf[c, core, xb, yb, :, cs].astype(F32) * scale * gains[k:k + 1, cs]).astype(BF16)
                buf[c, core, xb, yb, :, cs] = res
                if k == 0:
                    own[c, :, cs] = res
            start(k, c, 6 + ab)
        xfer(k, c, 4).wait_send()
        xfer(k, c, 5).wait_send()

    def g2(k, c, ab):
        xfer(k, c, 6 + ab).wait_recv()
        start(k, c, 8 + ab)

    def g3(k, c, ab):
        xfer(k, c, 8 + ab).wait_recv()
        if ab == 0:
            pl.semaphore_wait(free_sem.at[k, c], 1)
        start(k, c, 10 + ab)

    def done(k, c):
        for s in (10, 11):
            xfer(k, c, s).wait_recv()
        for s in range(6, 12):
            xfer(k, c, s).wait_send()

    def y_copy(c):
        return pltpu.make_async_copy(buf.at[c], y_hbm.at[c], y_sem.at[c])

    def fin(k, c):
        done(k, c)
        y_copy(c).start()

    def both(fn, k, c):
        fn(k, c, 0)
        fn(k, c, 1)

    def p1(c):
        def body(j, carry):
            cs = pl.ds(pl.multiple_of(j * wo_tile, wo_tile), wo_tile)
            acc = jnp.dot(o_ref[c], w2[0:q_loc, cs], preferred_element_type=F32)
            buf[c, :, :, :, :, cs] = acc.astype(BF16).reshape(2, 2, 2, blk, wo_tile)
            return carry
        for ab in range(2):
            lax.fori_loop(ab * n_wo // 2, (ab + 1) * n_wo // 2, body, 0)
            s0(0, c, ab)

    gu_tile = 256
    gu_tiles = [(f, min(gu_tile, ff_loc - f)) for f in range(0, ff_loc, gu_tile)]

    def dot_t(w_rows, h):
        return lax.dot_general(w_rows, h, (((1,), (1,)), ((), ())), preferred_element_type=F32)

    def p2(services):
        def chunk(c, carry):
            def serve(point):
                for (sc, sp), fns in services.items():
                    if sp == point:
                        @pl.when(c == sc)
                        def _(fns=fns):
                            for fn in fns:
                                fn()

            for j, (f0, fw) in enumerate(gu_tiles):
                serve(j)
                h = buf[c].reshape(rows, d_model)
                g = dot_t(w1[f0:f0 + fw, :], h)
                up = dot_t(w3[f0:f0 + fw, :], h)
                act[:, f0:f0 + fw] = jnp.transpose(g * jax.nn.sigmoid(g) * up).astype(BF16)

            base = len(gu_tiles)

            def down(cs):
                acc = jnp.dot(act[...], w2[:, cs], preferred_element_type=F32)
                buf[c, :, :, :, :, cs] = acc.astype(BF16).reshape(2, 2, 2, blk, half_d)
            for ab in range(2):
                serve(base + ab)
                down(cols[ab])
                s0(1, c, ab)
            return carry
        lax.fori_loop(0, n_chunks, chunk, 0)

    for j in range(n_wo):
        wo_copy(j).wait()
    p1(0)
    p1(1)
    both(s1, 0, 0)
    p1(2)
    for j in range(n_k):
        w_copy(2, j).start()
    both(s1, 0, 1)
    both(s2, 0, 0)
    x_copy().wait()
    s3(0, 0)
    both(s2, 0, 1)
    both(g2, 0, 0)
    s3(0, 1)
    both(s1, 0, 2)
    both(g3, 0, 0)
    for j in range(n_k):
        for i in range(3):
            w_copy(i, j).wait()
    done(0, 0)

    F = functools.partial
    p2({
        (0, 0): [F(both, g2, 0, 1)],
        (0, 2): [F(both, s2, 0, 2)],
        (0, 5): [F(both, g3, 0, 1)],
        (0, 6): [F(s3, 0, 2)],
        (1, 0): [F(done, 0, 1), F(both, g2, 0, 2)],
        (1, 1): [F(both, s1, 1, 0)],
        (1, 4): [F(both, g3, 0, 2)],
        (1, 6): [F(both, s2, 1, 0)],
        (2, 0): [F(done, 0, 2), F(s3, 1, 0)],
        (2, 1): [F(both, s1, 1, 1)],
        (2, 3): [F(both, g2, 1, 0)],
        (2, 5): [F(both, s2, 1, 1)],
        (2, 7): [F(both, g3, 1, 0)],
    })
    s3(1, 1)
    fin(1, 0)
    both(s1, 1, 2)
    both(g2, 1, 1)
    both(s2, 1, 2)
    both(g3, 1, 1)
    s3(1, 2)
    fin(1, 1)
    both(g2, 1, 2)
    both(g3, 1, 2)
    fin(1, 2)
    for c in range(n_chunks):
        y_copy(c).wait()


def tail(o, x_seq, w_o, w1, w3, w2, g_attn, g_mlp):
    n_chunks, rows, d_model = x_seq.shape
    q_loc = o.shape[-1]
    ff_loc = w2.shape[0]
    blk = rows // 8
    dims = (n_chunks, rows, d_model, q_loc, ff_loc)
    vmem = pl.BlockSpec(memory_space=pltpu.VMEM)
    hbm = pl.BlockSpec(memory_space=pl.ANY)
    y = pl.pallas_call(
        functools.partial(tail_kernel, dims),
        name='tail',
        out_shape=jax.ShapeDtypeStruct((n_chunks, 2, 2, 2, blk, d_model), BF16),
        in_specs=[vmem, vmem, vmem, hbm, hbm, hbm, hbm, hbm],
        out_specs=hbm,
        scratch_shapes=[
            pltpu.VMEM((n_chunks, 2, 2, 2, blk, d_model), BF16),
            pltpu.VMEM((n_chunks, 2, 2, blk, d_model), BF16),
            pltpu.VMEM((n_chunks, 2, blk, d_model), BF16),
            pltpu.VMEM((n_chunks, blk, d_model), BF16),
            pltpu.VMEM((n_chunks, blk, d_model), BF16),
            pltpu.VMEM((n_chunks, blk, d_model), BF16),
            pltpu.VMEM((rows, ff_loc), BF16),
            pltpu.VMEM((2, d_model), F32),
            pltpu.VMEM((ff_loc, d_model), BF16),
            pltpu.VMEM((ff_loc, d_model), BF16),
            pltpu.VMEM((ff_loc, d_model), BF16),
            pltpu.SemaphoreType.DMA((2, n_chunks, 12)),
            pltpu.SemaphoreType.DMA((2, n_chunks, 12)),
            pltpu.SemaphoreType.DMA((3, 4)),
            pltpu.SemaphoreType.DMA((4,)),
            pltpu.SemaphoreType.DMA,
            pltpu.SemaphoreType.DMA((n_chunks,)),
            pltpu.SemaphoreType.REGULAR((2, n_chunks)),
        ],
        compiler_params=pltpu.CompilerParams(collective_id=1, has_side_effects=True, vmem_limit_bytes=67043328),
    )(o, g_attn.reshape(-1, 128), g_mlp.reshape(-1, 128), x_seq.reshape(n_chunks, 8, blk, d_model), w_o, w1.T, w3.T, w2)
    return y.reshape(n_chunks, rows, d_model)


def head_kernel(dims, len_ref, gq_ref, gk_ref, freq_ref, x_hbm, wq_hbm, wk_hbm, wv_hbm, q_out, k_out, v_out,
                x, w, raw, cos_t, sin_t, sums, x_sem, w_sem, send_sem, recv_sem):
    n_steps, rows, d_model, q_loc, hd, n_tp = dims
    heads = q_loc // hd
    width = q_loc + 2 * hd
    tp = lax.axis_index('tp')

    def x_copy(t):
        return pltpu.make_async_copy(x_hbm.at[t], x.at[t], x_sem.at[t])

    n_k = 4
    k_rows = d_model // n_k

    def w_copies(j):
        rs = pl.ds(j * k_rows, k_rows)
        return (pltpu.make_async_copy(wq_hbm.at[rs], w.at[rs, pl.ds(0, q_loc)], w_sem.at[0, j]),
                pltpu.make_async_copy(wk_hbm.at[rs], w.at[rs, pl.ds(q_loc, hd)], w_sem.at[1, j]),
                pltpu.make_async_copy(wv_hbm.at[rs], w.at[rs, pl.ds(q_loc + hd, hd)], w_sem.at[2, j]))

    x_copy(0).start()
    for j in range(n_k):
        for cp in w_copies(j):
            cp.start()
    for t in range(1, n_steps):
        x_copy(t).start()

    barrier = pltpu.get_barrier_semaphore()
    peers = [lax.rem(tp + d, n_tp) for d in range(1, n_tp)]
    for p in peers:
        pl.semaphore_signal(barrier, inc=1, device_id={'tp': p}, device_id_type=pl.DeviceIdType.MESH)

    lens = jnp.transpose(jnp.broadcast_to(len_ref[...].astype(F32), (rows, rows)))
    lane = lax.broadcasted_iota(jnp.int32, (rows, hd), 1)
    sign = jnp.where(lane < hd // 2, -1.0, 1.0).astype(F32)
    for t in range(n_steps):
        ang = (lens + float(t)) * freq_ref[...]
        cos_t[t] = jnp.cos(ang)
        sin_t[t] = jnp.sin(ang) * sign

    for j in range(n_k):
        for cp in w_copies(j):
            cp.wait()
    part = jnp.zeros((rows, rows), F32)
    sq_lane = lax.broadcasted_iota(jnp.int32, (rows, rows), 1)
    for t in range(n_steps):
        x_copy(t).wait()
        res = jnp.dot(x[t], w[...], preferred_element_type=F32).astype(BF16)
        raw[t] = res
        q = res[:, :q_loc].astype(F32)
        k = res[:, q_loc:q_loc + hd].astype(F32)
        part = jnp.where(sq_lane == 2 * t, jnp.sum(q * q, axis=-1, keepdims=True), part)
        part = jnp.where(sq_lane == 2 * t + 1, jnp.sum(k * k, axis=-1, keepdims=True), part)
    sums[tp] = jnp.transpose(part)[0:8]
    pl.semaphore_wait(barrier, n_tp - 1)

    def send(d):
        return pltpu.make_async_remote_copy(
            src_ref=sums.at[tp], dst_ref=sums.at[tp], send_sem=send_sem.at[d], recv_sem=recv_sem.at[d],
            device_id={'tp': peers[d]}, device_id_type=pl.DeviceIdType.MESH)

    for d in range(n_tp - 1):
        send(d).start()
    q_out[pl.ds(n_steps * heads, rows, stride=16), :] = jnp.zeros((rows, hd), F32)
    for t in range(n_steps):
        v_out[t] = raw[t, :, q_loc + hd:width].astype(F32)
    for d in range(n_tp - 1):
        send(d).wait()
    tot = sums[0]
    for d in range(1, n_tp):
        tot = tot + sums[d]
    full = jnp.transpose(jnp.concatenate([tot, jnp.zeros((rows - 8, rows), F32)], axis=0))
    for t in range(n_steps):
        q_scale = rms_factor(full[:, 2 * t:2 * t + 1], q_loc * n_tp)
        k_scale = rms_factor(full[:, 2 * t + 1:2 * t + 2], hd * n_tp)

        def rotate(col, scale, gain):
            val = raw[t, :, col:col + hd].astype(F32) * scale * gain.astype(F32)
            return (val * cos_t[t] + pltpu.roll(val, hd // 2, 1) * sin_t[t]).astype(BF16).astype(F32)
        for j in range(heads):
            q_out[pl.ds(t * heads + j, rows, stride=16), :] = rotate(j * hd, q_scale, gq_ref[j:j + 1, :])
        k_out[t] = rotate(q_loc, k_scale, gk_ref[...])


def head(x_seq, cache_len, w_q, w_k, w_v, g_q, g_k, n_tp):
    n_steps, rows, d_model = x_seq.shape
    q_loc, hd = w_q.shape[1], w_k.shape[1]
    width = q_loc + 2 * hd
    half = hd // 2
    inv_freq = np.float32(ROPE_THETA) ** (-(np.arange(half, dtype=np.float32) * np.float32(2.0 / hd)))
    freq = jnp.asarray(np.concatenate([inv_freq, inv_freq]).reshape(1, hd), F32)
    vmem = pl.BlockSpec(memory_space=pltpu.VMEM)
    hbm = pl.BlockSpec(memory_space=pl.ANY)
    return pl.pallas_call(
        functools.partial(head_kernel, (n_steps, rows, d_model, q_loc, hd, n_tp)),
        name='head',
        out_shape=(jax.ShapeDtypeStruct((rows * 16, hd), F32),
                   jax.ShapeDtypeStruct((n_steps, rows, hd), F32),
                   jax.ShapeDtypeStruct((n_steps, rows, hd), F32)),
        in_specs=[vmem] * 4 + [hbm] * 4,
        out_specs=(vmem,) * 3,
        scratch_shapes=[
            pltpu.VMEM((n_steps, rows, d_model), BF16),
            pltpu.VMEM((d_model, width), BF16),
            pltpu.VMEM((n_steps, rows, width), BF16),
            pltpu.VMEM((n_steps, rows, hd), F32),
            pltpu.VMEM((n_steps, rows, hd), F32),
            pltpu.VMEM((n_tp, 8, rows), F32),
            pltpu.SemaphoreType.DMA((n_steps,)),
            pltpu.SemaphoreType.DMA((3, 4)),
            pltpu.SemaphoreType.DMA((n_tp - 1,)),
            pltpu.SemaphoreType.DMA((n_tp - 1,)),
        ],
        compiler_params=pltpu.CompilerParams(collective_id=0, has_side_effects=True, vmem_limit_bytes=67043328),
    )(cache_len.reshape(1, -1), g_q.reshape(-1, hd), g_k.reshape(1, -1), freq, x_seq, w_q, w_k, w_v)


def attn_kernel(dims, len_ref, q_ref, kn_ref, vn_ref, k_ref, v_ref, o_ref, ko_ref, vo_ref, s_scr, e_scr, l_scr, o_scr):
    n_steps, nb, heads, hd, seq_max = dims
    first = pl.program_id(0) * nb
    win = 32
    row_step = lax.broadcasted_iota(jnp.int32, (16, seq_max), 0) // heads
    col = lax.broadcasted_iota(jnp.int32, (16, seq_max), 1)
    ahead = col - row_step
    win_row = lax.broadcasted_iota(jnp.int32, (win, hd), 0)
    for src, new, dst in ((k_ref, kn_ref, ko_ref), (v_ref, vn_ref, vo_ref)):
        dst[...] = src[...]
        for i in range(nb):
            ln = len_ref[first + i]
            base = pl.multiple_of(jnp.minimum((ln // 16) * 16, seq_max - win), 16)
            rel = win_row + (base - ln)
            cut = src[i, pl.ds(base, win), :].astype(F32)
            for t in range(n_steps):
                cut = jnp.where(rel == t, new[t, i:i + 1, :], cut)
            dst[i, pl.ds(base, win), :] = cut.astype(BF16)
    for i in range(nb):
        s = lax.dot_general(q_ref[i].astype(BF16), ko_ref[i], (((1,), (1,)), ((), ())), preferred_element_type=F32) * hd ** -0.5
        s_scr[i * 16:(i + 1) * 16, :] = jnp.where(ahead <= len_ref[first + i], s, -jnp.inf)
    for i in range(0, nb, 2):
        rs = slice(i * 16, (i + 2) * 16)
        s = s_scr[rs, :]
        e = jnp.exp(s - jnp.max(s, axis=-1, keepdims=True))
        l_scr[rs, :] = jnp.broadcast_to(jnp.sum(e, axis=-1, keepdims=True), (32, hd))
        e_scr[rs, :] = e.astype(BF16)
    for i in range(nb):
        rs = slice(i * 16, (i + 1) * 16)
        o_scr[rs, :] = jnp.dot(e_scr[rs, :], vo_ref[i], preferred_element_type=F32)
    o_scr[...] = o_scr[...] / l_scr[...]
    for t in range(n_steps):
        for j in range(heads):
            o_ref[t, :, j * hd:(j + 1) * hd] = o_scr[pl.ds(t * heads + j, nb, stride=16), :].astype(BF16)


def attend(q, kn, vn, k_cache, v_cache, cache_len, heads):
    n_rows, _, seq_max, hd = k_cache.shape
    n_steps = kn.shape[0]
    nb = 32
    cache_spec = pl.BlockSpec((nb, seq_max, hd), lambda i, ln: (i, 0, 0))
    new_spec = pl.BlockSpec((n_steps, nb, hd), lambda i, ln: (0, i, 0))
    cache_shape = jax.ShapeDtypeStruct((n_rows, seq_max, hd), BF16)
    flops = 4 * n_rows * 16 * seq_max * hd
    return pl.pallas_call(
        functools.partial(attn_kernel, (n_steps, nb, heads, hd, seq_max)),
        name='attend',
        grid_spec=pltpu.PrefetchScalarGridSpec(
            num_scalar_prefetch=1,
            grid=(n_rows // nb,),
            in_specs=[pl.BlockSpec((nb, 16, hd), lambda i, ln: (i, 0, 0)), new_spec, new_spec, cache_spec, cache_spec],
            out_specs=(pl.BlockSpec((n_steps, nb, heads * hd), lambda i, ln: (0, i, 0)), cache_spec, cache_spec),
            scratch_shapes=[pltpu.VMEM((nb * 16, seq_max), F32), pltpu.VMEM((nb * 16, seq_max), BF16), pltpu.VMEM((nb * 16, hd), F32), pltpu.VMEM((nb * 16, hd), F32)],
        ),
        out_shape=(jax.ShapeDtypeStruct((n_steps, n_rows, heads * hd), BF16), cache_shape, cache_shape),
        compiler_params=pltpu.CompilerParams(vmem_limit_bytes=67043328),
        cost_estimate=pl.CostEstimate(flops=flops, bytes_accessed=4 * n_rows * seq_max * hd * 2, transcendentals=n_rows * 16 * seq_max),
    )(cache_len, q.reshape(n_rows, 16, hd), kn, vn, k_cache[:, 0], v_cache[:, 0])


def local_layer(n_tp, x_seq, cache_len, k_cache, v_cache, w_q, w_k, w_v, w_o, w_gate, w_up, w_down, g_q, g_k, g_attn, g_mlp):
    heads = w_q.shape[1] // k_cache.shape[3]
    q, kn, vn = head(x_seq, cache_len, w_q, w_k, w_v, g_q, g_k, n_tp)
    o, k_out, v_out = attend(q, kn, vn, k_cache, v_cache, cache_len, heads)
    y = tail(o, x_seq, w_o, w_gate, w_up, w_down, g_attn, g_mlp)
    return y, k_out[:, None], v_out[:, None]


def solution(mesh):
    tp_size = mesh.shape['tp']
    data_spec = P(None, 'dp', None)
    cache_spec = P('dp', 'tp', None, None)
    col_spec = P(None, 'tp')
    row_spec = P('tp', None)
    arg_specs = (data_spec, P('dp'), cache_spec, cache_spec, col_spec, col_spec, col_spec, row_spec, col_spec, col_spec, row_spec, P('tp'), P('tp'), P(None), P(None))
    out_specs = (data_spec, cache_spec, cache_spec)
    return jax.shard_map(functools.partial(local_layer, tp_size), mesh=mesh, in_specs=arg_specs, out_specs=out_specs, check_vma=False)
```

```python
import functools

import jax
import jax.numpy as jnp
import numpy as np
from jax import lax
from jax.experimental import pallas as pl
from jax.experimental.pallas import tpu as pltpu
from jax.sharding import PartitionSpec as P

ROPE_THETA = 500000.0
NORM_EPS = 1e-6
F32 = jnp.float32
BF16 = jnp.bfloat16


def rms_factor(sq_sum, full_width):
    return lax.rsqrt(sq_sum / full_width + NORM_EPS)


def tail_kernel(dims, o_ref, ga_ref, gm_ref, x_hbm, wo_hbm, w1_hbm, w3_hbm, w2_hbm, y_hbm,
                buf, r0, r1, r2, st, own, act, gains, w1, w3, w2,
                send_sem, recv_sem, w_sem, o_sem, x_sem, y_sem, free_sem):
    n_chunks, rows, d_model, q_loc, ff_loc = dims
    blk = rows // 8
    half_d = d_model // 2
    tp = lax.axis_index('tp')
    core = lax.rem(tp, 2)
    xb = lax.rem(lax.div(tp, 2), 2)
    yb = lax.div(tp, 4)
    sib = tp + 1 - 2 * core
    x_nb = tp + 2 - 4 * xb
    y_nb = tp + 4 - 8 * yb
    oc, ox, oy = 1 - core, 1 - xb, 1 - yb
    cols = (pl.ds(0, half_d), pl.ds(half_d, half_d))
    me = core * 4 + xb * 2 + yb

    n_wo = 4
    wo_tile = d_model // n_wo

    def wo_copy(j):
        cs = pl.ds(j * wo_tile, wo_tile)
        return pltpu.make_async_copy(wo_hbm.at[:, cs], w2.at[pl.ds(0, q_loc), cs], o_sem.at[j])

    def x_copy():
        return pltpu.make_async_copy(x_hbm.at[:, me], own, x_sem)

    n_k = 4
    k_rows = ff_loc // n_k

    def w_copy(i, j):
        src, dst = ((w1_hbm, w1), (w3_hbm, w3), (w2_hbm, w2))[i]
        rs = pl.ds(j * k_rows, k_rows)
        return pltpu.make_async_copy(src.at[rs], dst.at[rs], w_sem.at[i, j])

    for j in range(n_wo):
        wo_copy(j).start()
    x_copy().start()

    barrier = pltpu.get_barrier_semaphore()
    for peer in (sib, x_nb, y_nb):
        pl.semaphore_signal(barrier, inc=1, device_id={'tp': peer}, device_id_type=pl.DeviceIdType.MESH)
    for i, g_ref in enumerate((ga_ref, gm_ref)):
        for j in range(d_model // 128):
            gains[i:i + 1, j * 128:(j + 1) * 128] = g_ref[j:j + 1, :].astype(F32)
    pl.semaphore_wait(barrier, 3)

    def xfer(k, c, s):
        ab = s % 2
        cs = cols[ab]
        b = buf.at[c]
        if s < 2:
            src, dst, peer = b.at[oc, :, :, :, cs], r0.at[c, :, :, :, cs], sib
        elif s == 2:
            src, dst, peer = b.at[core, ox, :, :, cs], r1.at[c, :, :, cs], x_nb
        elif s == 3:
            src, dst, peer = b.at[core, :, oy, :, cs], r1.at[c, :, :, cs], y_nb
        elif s < 6:
            src, dst, peer = st.at[c, :, cs], r2.at[c, :, cs], (y_nb, x_nb)[ab]
        else:
            if s < 8:
                src, peer = b.at[core, xb, yb, :, cs], (y_nb, x_nb)[ab]
            elif s == 8:
                src, peer = b.at[core, xb, :, :, cs], x_nb
            elif s == 9:
                src, peer = b.at[core, :, yb, :, cs], y_nb
            else:
                src, peer = b.at[core, :, :, :, cs], sib
            dst = src
        return pltpu.make_async_remote_copy(
            src_ref=src, dst_ref=dst, send_sem=send_sem.at[k, c, s], recv_sem=recv_sem.at[k, c, s],
            device_id={'tp': peer}, device_id_type=pl.DeviceIdType.MESH)

    def start(k, c, s):
        xfer(k, c, s).start()

    def s0(k, c, ab):
        start(k, c, ab)

    def s1(k, c, ab):
        cs = cols[ab]
        x = xfer(k, c, ab)
        x.wait_recv()
        if ab == 0:
            buf[c, core, ox, :, :, cs] = buf[c, core, ox, :, :, cs] + r0[c, ox, :, :, cs]
            start(k, c, 2)
            buf[c, core, xb, :, :, cs] = buf[c, core, xb, :, :, cs] + r0[c, xb, :, :, cs]
        else:
            for i in range(2):
                buf[c, core, i, oy, :, cs] = buf[c, core, i, oy, :, cs] + r0[c, i, oy, :, cs]
            start(k, c, 3)
            for i in range(2):
                buf[c, core, i, yb, :, cs] = buf[c, core, i, yb, :, cs] + r0[c, i, yb, :, cs]
        x.wait_send()
        if ab == 1:
            pl.semaphore_signal(free_sem.at[k, c], inc=1, device_id={'tp': sib}, device_id_type=pl.DeviceIdType.MESH)

    def s2(k, c, ab):
        cs = cols[ab]
        x = xfer(k, c, 2 + ab)
        x.wait_recv()
        if ab == 0:
            st[c, :, cs] = buf[c, core, xb, oy, :, cs] + r1[c, oy, :, cs]
            start(k, c, 4)
            buf[c, core, xb, yb, :, cs] = buf[c, core, xb, yb, :, cs] + r1[c, yb, :, cs]
        else:
            st[c, :, cs] = buf[c, core, ox, yb, :, cs] + r1[c, ox, :, cs]
            start(k, c, 5)
            buf[c, core, xb, yb, :, cs] = buf[c, core, xb, yb, :, cs] + r1[c, xb, :, cs]
        x.wait_send()

    v_tile = 512

    def s3(k, c):
        xfer(k, c, 4).wait_recv()
        xfer(k, c, 5).wait_recv()
        sq = jnp.zeros((blk, v_tile), F32)
        for j in range(d_model // v_tile):
            cs = pl.ds(j * v_tile, v_tile)
            tot = (buf[c, core, xb, yb, :, cs].astype(F32) + r2[c, :, cs].astype(F32)).astype(BF16)
            buf[c, core, xb, yb, :, cs] = tot
            tot = tot.astype(F32)
            sq = sq + tot * tot
        scale = rms_factor(jnp.sum(sq, axis=-1, keepdims=True), d_model)
        for ab in range(2):
            for j in range(half_d // v_tile):
                cs = pl.ds(ab * half_d + j * v_tile, v_tile)
                res = (own[c, :, cs].astype(F32) + buf[c, core, xb, yb, :, cs].astype(F32) * scale * gains[k:k + 1, cs]).astype(BF16)
                buf[c, core, xb, yb, :, cs] = res
                if k == 0:
                    own[c, :, cs] = res
            start(k, c, 6 + ab)
        xfer(k, c, 4).wait_send()
        xfer(k, c, 5).wait_send()

    def g2(k, c, ab):
        xfer(k, c, 6 + ab).wait_recv()
        start(k, c, 8 + ab)

    def g3(k, c, ab):
        xfer(k, c, 8 + ab).wait_recv()
        if ab == 0:
            pl.semaphore_wait(free_sem.at[k, c], 1)
        start(k, c, 10 + ab)

    def done(k, c):
        for s in (10, 11):
            xfer(k, c, s).wait_recv()
        for s in range(6, 12):
            xfer(k, c, s).wait_send()

    def y_copy(c):
        return pltpu.make_async_copy(buf.at[c], y_hbm.at[c], y_sem.at[c])

    def fin(k, c):
        done(k, c)
        y_copy(c).start()

    def both(fn, k, c):
        fn(k, c, 0)
        fn(k, c, 1)

    def p1(c):
        def body(j, carry):
            cs = pl.ds(pl.multiple_of(j * wo_tile, wo_tile), wo_tile)
            acc = jnp.dot(o_ref[c], w2[0:q_loc, cs], preferred_element_type=F32)
            buf[c, :, :, :, :, cs] = acc.astype(BF16).reshape(2, 2, 2, blk, wo_tile)
            return carry
        for ab in range(2):
            if c == 0:
                for j in range(ab * n_wo // 2, (ab + 1) * n_wo // 2):
                    wo_copy(j).wait()
                    body(j, 0)
            else:
                lax.fori_loop(ab * n_wo // 2, (ab + 1) * n_wo // 2, body, 0)
            s0(0, c, ab)

    gu_tile = 256
    gu_tiles = [(f, min(gu_tile, ff_loc - f)) for f in range(0, ff_loc, gu_tile)]

    def dot_t(w_rows, h):
        return lax.dot_general(w_rows, h, (((1,), (1,)), ((), ())), preferred_element_type=F32)

    def p2(services):
        def chunk(c, carry):
            def serve(point):
                for (sc, sp), fns in services.items():
                    if sp == point:
                        @pl.when(c == sc)
                        def _(fns=fns):
                            for fn in fns:
                                fn()

            for j, (f0, fw) in enumerate(gu_tiles):
                serve(j)
                h = buf[c].reshape(rows, d_model)
                g = dot_t(w1[f0:f0 + fw, :], h)
                up = dot_t(w3[f0:f0 + fw, :], h)
                act[:, f0:f0 + fw] = jnp.transpose(g * jax.nn.sigmoid(g) * up).astype(BF16)

            base = len(gu_tiles)

            def down(cs):
                acc = jnp.dot(act[...], w2[:, cs], preferred_element_type=F32)
                buf[c, :, :, :, :, cs] = acc.astype(BF16).reshape(2, 2, 2, blk, half_d)
            for ab in range(2):
                serve(base + ab)
                down(cols[ab])
                s0(1, c, ab)
            return carry
        lax.fori_loop(0, n_chunks, chunk, 0)

    p1(0)
    for j in range(n_k):
        for i in range(2):
            w_copy(i, j).start()
    p1(1)
    both(s1, 0, 0)
    p1(2)
    for j in range(n_k):
        w_copy(2, j).start()
    both(s1, 0, 1)
    both(s2, 0, 0)
    x_copy().wait()
    s3(0, 0)
    both(s2, 0, 1)
    both(g2, 0, 0)
    s3(0, 1)
    both(s1, 0, 2)
    both(g3, 0, 0)
    for j in range(n_k):
        for i in range(3):
            w_copy(i, j).wait()
    done(0, 0)

    F = functools.partial
    p2({
        (0, 0): [F(both, g2, 0, 1)],
        (0, 2): [F(both, s2, 0, 2)],
        (0, 5): [F(both, g3, 0, 1)],
        (0, 6): [F(s3, 0, 2)],
        (1, 0): [F(done, 0, 1), F(both, g2, 0, 2)],
        (1, 1): [F(both, s1, 1, 0)],
        (1, 4): [F(both, g3, 0, 2)],
        (1, 6): [F(both, s2, 1, 0)],
        (2, 0): [F(done, 0, 2), F(s3, 1, 0)],
        (2, 1): [F(both, s1, 1, 1)],
        (2, 3): [F(both, g2, 1, 0)],
        (2, 5): [F(both, s2, 1, 1)],
        (2, 7): [F(both, g3, 1, 0)],
    })
    s3(1, 1)
    fin(1, 0)
    both(s1, 1, 2)
    both(g2, 1, 1)
    both(s2, 1, 2)
    both(g3, 1, 1)
    s3(1, 2)
    fin(1, 1)
    both(g2, 1, 2)
    both(g3, 1, 2)
    fin(1, 2)
    for c in range(n_chunks):
        y_copy(c).wait()


def tail(o, x_seq, w_o, w1, w3, w2, g_attn, g_mlp):
    n_chunks, rows, d_model = x_seq.shape
    q_loc = o.shape[-1]
    ff_loc = w2.shape[0]
    blk = rows // 8
    dims = (n_chunks, rows, d_model, q_loc, ff_loc)
    vmem = pl.BlockSpec(memory_space=pltpu.VMEM)
    hbm = pl.BlockSpec(memory_space=pl.ANY)
    y = pl.pallas_call(
        functools.partial(tail_kernel, dims),
        name='tail',
        out_shape=jax.ShapeDtypeStruct((n_chunks, 2, 2, 2, blk, d_model), BF16),
        in_specs=[vmem, vmem, vmem, hbm, hbm, hbm, hbm, hbm],
        out_specs=hbm,
        scratch_shapes=[
            pltpu.VMEM((n_chunks, 2, 2, 2, blk, d_model), BF16),
            pltpu.VMEM((n_chunks, 2, 2, blk, d_model), BF16),
            pltpu.VMEM((n_chunks, 2, blk, d_model), BF16),
            pltpu.VMEM((n_chunks, blk, d_model), BF16),
            pltpu.VMEM((n_chunks, blk, d_model), BF16),
            pltpu.VMEM((n_chunks, blk, d_model), BF16),
            pltpu.VMEM((rows, ff_loc), BF16),
            pltpu.VMEM((2, d_model), F32),
            pltpu.VMEM((ff_loc, d_model), BF16),
            pltpu.VMEM((ff_loc, d_model), BF16),
            pltpu.VMEM((ff_loc, d_model), BF16),
            pltpu.SemaphoreType.DMA((2, n_chunks, 12)),
            pltpu.SemaphoreType.DMA((2, n_chunks, 12)),
            pltpu.SemaphoreType.DMA((3, 4)),
            pltpu.SemaphoreType.DMA((4,)),
            pltpu.SemaphoreType.DMA,
            pltpu.SemaphoreType.DMA((n_chunks,)),
            pltpu.SemaphoreType.REGULAR((2, n_chunks)),
        ],
        compiler_params=pltpu.CompilerParams(collective_id=1, has_side_effects=True, vmem_limit_bytes=67043328),
    )(o, g_attn.reshape(-1, 128), g_mlp.reshape(-1, 128), x_seq.reshape(n_chunks, 8, blk, d_model), w_o, w1.T, w3.T, w2)
    return y.reshape(n_chunks, rows, d_model)


def head_kernel(dims, len_ref, gq_ref, gk_ref, freq_ref, x_hbm, wq_hbm, wk_hbm, wv_hbm, q_out, k_out, v_out,
                x, w, raw, cos_t, sin_t, sums, x_sem, w_sem, send_sem, recv_sem):
    n_steps, rows, d_model, q_loc, hd, n_tp = dims
    heads = q_loc // hd
    width = q_loc + 2 * hd
    tp = lax.axis_index('tp')

    def x_copy(t):
        return pltpu.make_async_copy(x_hbm.at[t], x.at[t], x_sem.at[t])

    n_k = 4
    k_rows = d_model // n_k

    def w_copies(j):
        rs = pl.ds(j * k_rows, k_rows)
        return (pltpu.make_async_copy(wq_hbm.at[rs], w.at[rs, pl.ds(0, q_loc)], w_sem.at[0, j]),
                pltpu.make_async_copy(wk_hbm.at[rs], w.at[rs, pl.ds(q_loc, hd)], w_sem.at[1, j]),
                pltpu.make_async_copy(wv_hbm.at[rs], w.at[rs, pl.ds(q_loc + hd, hd)], w_sem.at[2, j]))

    x_copy(0).start()
    for j in range(n_k):
        for cp in w_copies(j):
            cp.start()
    for t in range(1, n_steps):
        x_copy(t).start()

    barrier = pltpu.get_barrier_semaphore()
    peers = [lax.rem(tp + d, n_tp) for d in range(1, n_tp)]
    for p in peers:
        pl.semaphore_signal(barrier, inc=1, device_id={'tp': p}, device_id_type=pl.DeviceIdType.MESH)

    lens = jnp.transpose(jnp.broadcast_to(len_ref[...].astype(F32), (rows, rows)))
    lane = lax.broadcasted_iota(jnp.int32, (rows, hd), 1)
    sign = jnp.where(lane < hd // 2, -1.0, 1.0).astype(F32)
    for t in range(n_steps):
        ang = (lens + float(t)) * freq_ref[...]
        cos_t[t] = jnp.cos(ang)
        sin_t[t] = jnp.sin(ang) * sign

    for j in range(n_k):
        for cp in w_copies(j):
            cp.wait()
    sq_lane = lax.broadcasted_iota(jnp.int32, (rows, rows), 1)

    def send(t, d):
        return pltpu.make_async_remote_copy(
            src_ref=sums.at[t, tp], dst_ref=sums.at[t, tp], send_sem=send_sem.at[t, d], recv_sem=recv_sem.at[t, d],
            device_id={'tp': peers[d]}, device_id_type=pl.DeviceIdType.MESH)

    def project(t):
        x_copy(t).wait()
        res = jnp.dot(x[t], w[...], preferred_element_type=F32).astype(BF16)
        raw[t] = res
        q = res[:, :q_loc].astype(F32)
        k = res[:, q_loc:q_loc + hd].astype(F32)
        part = jnp.where(sq_lane == 0, jnp.sum(q * q, axis=-1, keepdims=True), jnp.sum(k * k, axis=-1, keepdims=True))
        sums[t, tp] = jnp.transpose(part)[0:8]
        if t == 0:
            pl.semaphore_wait(barrier, n_tp - 1)
        for d in range(n_tp - 1):
            send(t, d).start()
        v_out[t] = res[:, q_loc + hd:width].astype(F32)

    def rotate_all(t):
        for d in range(n_tp - 1):
            send(t, d).wait()
        tot = sums[t, 0]
        for d in range(1, n_tp):
            tot = tot + sums[t, d]
        full = jnp.transpose(jnp.concatenate([tot, jnp.zeros((rows - 8, rows), F32)], axis=0))
        q_scale = rms_factor(full[:, 0:1], q_loc * n_tp)
        k_scale = rms_factor(full[:, 1:2], hd * n_tp)

        def rotate(col, scale, gain):
            val = raw[t, :, col:col + hd].astype(F32) * scale * gain.astype(F32)
            return (val * cos_t[t] + pltpu.roll(val, hd // 2, 1) * sin_t[t]).astype(BF16).astype(F32)
        for j in range(heads):
            q_out[pl.ds(t * heads + j, rows, stride=16), :] = rotate(j * hd, q_scale, gq_ref[j:j + 1, :])
        k_out[t] = rotate(q_loc, k_scale, gk_ref[...])

    for t in range(n_steps):
        project(t)
    q_out[pl.ds(n_steps * heads, rows, stride=16), :] = jnp.zeros((rows, hd), F32)
    for t in range(n_steps):
        rotate_all(t)


def head(x_seq, cache_len, w_q, w_k, w_v, g_q, g_k, n_tp):
    n_steps, rows, d_model = x_seq.shape
    q_loc, hd = w_q.shape[1], w_k.shape[1]
    width = q_loc + 2 * hd
    half = hd // 2
    inv_freq = np.float32(ROPE_THETA) ** (-(np.arange(half, dtype=np.float32) * np.float32(2.0 / hd)))
    freq = jnp.asarray(np.concatenate([inv_freq, inv_freq]).reshape(1, hd), F32)
    vmem = pl.BlockSpec(memory_space=pltpu.VMEM)
    hbm = pl.BlockSpec(memory_space=pl.ANY)
    return pl.pallas_call(
        functools.partial(head_kernel, (n_steps, rows, d_model, q_loc, hd, n_tp)),
        name='head',
        out_shape=(jax.ShapeDtypeStruct((rows * 16, hd), F32),
                   jax.ShapeDtypeStruct((n_steps, rows, hd), F32),
                   jax.ShapeDtypeStruct((n_steps, rows, hd), F32)),
        in_specs=[vmem] * 4 + [hbm] * 4,
        out_specs=(vmem,) * 3,
        scratch_shapes=[
            pltpu.VMEM((n_steps, rows, d_model), BF16),
            pltpu.VMEM((d_model, width), BF16),
            pltpu.VMEM((n_steps, rows, width), BF16),
            pltpu.VMEM((n_steps, rows, hd), F32),
            pltpu.VMEM((n_steps, rows, hd), F32),
            pltpu.VMEM((n_steps, n_tp, 8, rows), F32),
            pltpu.SemaphoreType.DMA((n_steps,)),
            pltpu.SemaphoreType.DMA((3, 4)),
            pltpu.SemaphoreType.DMA((n_steps, n_tp - 1)),
            pltpu.SemaphoreType.DMA((n_steps, n_tp - 1)),
        ],
        compiler_params=pltpu.CompilerParams(collective_id=0, has_side_effects=True, vmem_limit_bytes=67043328),
    )(cache_len.reshape(1, -1), g_q.reshape(-1, hd), g_k.reshape(1, -1), freq, x_seq, w_q, w_k, w_v)


def attn_kernel(dims, len_ref, q_ref, kn_ref, vn_ref, k_ref, v_ref, o_ref, ko_ref, vo_ref, s_scr, e_scr, l_scr, o_scr):
    n_steps, nb, heads, hd, seq_max = dims
    first = pl.program_id(0) * nb
    win = 32
    row_step = lax.broadcasted_iota(jnp.int32, (16, seq_max), 0) // heads
    col = lax.broadcasted_iota(jnp.int32, (16, seq_max), 1)
    ahead = col - row_step
    win_row = lax.broadcasted_iota(jnp.int32, (win, hd), 0)
    for src, new, dst in ((k_ref, kn_ref, ko_ref), (v_ref, vn_ref, vo_ref)):
        dst[...] = src[...]
        for i in range(nb):
            ln = len_ref[first + i]
            base = pl.multiple_of(jnp.minimum((ln // 16) * 16, seq_max - win), 16)
            rel = win_row + (base - ln)
            cut = src[i, pl.ds(base, win), :].astype(F32)
            for t in range(n_steps):
                cut = jnp.where(rel == t, new[t, i:i + 1, :], cut)
            dst[i, pl.ds(base, win), :] = cut.astype(BF16)
    for i in range(nb):
        s = lax.dot_general(q_ref[i].astype(BF16), ko_ref[i], (((1,), (1,)), ((), ())), preferred_element_type=F32) * hd ** -0.5
        s_scr[i * 16:(i + 1) * 16, :] = jnp.where(ahead <= len_ref[first + i], s, -jnp.inf)
    for i in range(0, nb, 2):
        rs = slice(i * 16, (i + 2) * 16)
        s = s_scr[rs, :]
        e = jnp.exp(s - jnp.max(s, axis=-1, keepdims=True))
        l_scr[rs, :] = jnp.broadcast_to(jnp.sum(e, axis=-1, keepdims=True), (32, hd))
        e_scr[rs, :] = e.astype(BF16)
    for i in range(nb):
        rs = slice(i * 16, (i + 1) * 16)
        o_scr[rs, :] = jnp.dot(e_scr[rs, :], vo_ref[i], preferred_element_type=F32)
    o_scr[...] = o_scr[...] / l_scr[...]
    for t in range(n_steps):
        for j in range(heads):
            o_ref[t, :, j * hd:(j + 1) * hd] = o_scr[pl.ds(t * heads + j, nb, stride=16), :].astype(BF16)


def attend(q, kn, vn, k_cache, v_cache, cache_len, heads):
    n_rows, _, seq_max, hd = k_cache.shape
    n_steps = kn.shape[0]
    nb = 32
    cache_spec = pl.BlockSpec((nb, seq_max, hd), lambda i, ln: (i, 0, 0))
    new_spec = pl.BlockSpec((n_steps, nb, hd), lambda i, ln: (0, i, 0))
    cache_shape = jax.ShapeDtypeStruct((n_rows, seq_max, hd), BF16)
    flops = 4 * n_rows * 16 * seq_max * hd
    return pl.pallas_call(
        functools.partial(attn_kernel, (n_steps, nb, heads, hd, seq_max)),
        name='attend',
        grid_spec=pltpu.PrefetchScalarGridSpec(
            num_scalar_prefetch=1,
            grid=(n_rows // nb,),
            in_specs=[pl.BlockSpec((nb, 16, hd), lambda i, ln: (i, 0, 0)), new_spec, new_spec, cache_spec, cache_spec],
            out_specs=(pl.BlockSpec((n_steps, nb, heads * hd), lambda i, ln: (0, i, 0)), cache_spec, cache_spec),
            scratch_shapes=[pltpu.VMEM((nb * 16, seq_max), F32), pltpu.VMEM((nb * 16, seq_max), BF16), pltpu.VMEM((nb * 16, hd), F32), pltpu.VMEM((nb * 16, hd), F32)],
        ),
        out_shape=(jax.ShapeDtypeStruct((n_steps, n_rows, heads * hd), BF16), cache_shape, cache_shape),
        compiler_params=pltpu.CompilerParams(vmem_limit_bytes=67043328),
        cost_estimate=pl.CostEstimate(flops=flops, bytes_accessed=4 * n_rows * seq_max * hd * 2, transcendentals=n_rows * 16 * seq_max),
    )(cache_len, q.reshape(n_rows, 16, hd), kn, vn, k_cache[:, 0], v_cache[:, 0])


def local_layer(n_tp, x_seq, cache_len, k_cache, v_cache, w_q, w_k, w_v, w_o, w_gate, w_up, w_down, g_q, g_k, g_attn, g_mlp):
    heads = w_q.shape[1] // k_cache.shape[3]
    q, kn, vn = head(x_seq, cache_len, w_q, w_k, w_v, g_q, g_k, n_tp)
    o, k_out, v_out = attend(q, kn, vn, k_cache, v_cache, cache_len, heads)
    y = tail(o, x_seq, w_o, w_gate, w_up, w_down, g_attn, g_mlp)
    return y, k_out[:, None], v_out[:, None]


def solution(mesh):
    tp_size = mesh.shape['tp']
    data_spec = P(None, 'dp', None)
    cache_spec = P('dp', 'tp', None, None)
    col_spec = P(None, 'tp')
    row_spec = P('tp', None)
    arg_specs = (data_spec, P('dp'), cache_spec, cache_spec, col_spec, col_spec, col_spec, row_spec, col_spec, col_spec, row_spec, P('tp'), P('tp'), P(None), P(None))
    out_specs = (data_spec, cache_spec, cache_spec)
    return jax.shard_map(functools.partial(local_layer, tp_size), mesh=mesh, in_specs=arg_specs, out_specs=out_specs, check_vma=False)
```

```python
import functools

import jax
import jax.numpy as jnp
import numpy as np
from jax import lax
from jax.experimental import pallas as pl
from jax.experimental.pallas import tpu as pltpu
from jax.sharding import PartitionSpec as P

ROPE_THETA = 500000.0
NORM_EPS = 1e-6
F32 = jnp.float32
BF16 = jnp.bfloat16


def rms_factor(sq_sum, full_width):
    return lax.rsqrt(sq_sum / full_width + NORM_EPS)


def tail_kernel(dims, o_ref, ga_ref, gm_ref, x_hbm, wo_hbm, w1_hbm, w3_hbm, w2_hbm, y_hbm,
                buf, r0, r1, r2, st, own, act, gains, w1, w3, w2,
                send_sem, recv_sem, w_sem, o_sem, x_sem, y_sem, free_sem):
    n_chunks, rows, d_model, q_loc, ff_loc = dims
    blk = rows // 8
    half_d = d_model // 2
    tp = lax.axis_index('tp')
    core = lax.rem(tp, 2)
    xb = lax.rem(lax.div(tp, 2), 2)
    yb = lax.div(tp, 4)
    sib = tp + 1 - 2 * core
    x_nb = tp + 2 - 4 * xb
    y_nb = tp + 4 - 8 * yb
    oc, ox, oy = 1 - core, 1 - xb, 1 - yb
    n_p = 4
    wide = d_model // n_p
    cols = [pl.ds(p * wide, wide) for p in range(n_p)]
    me = core * 4 + xb * 2 + yb

    n_wo = 4
    wo_tile = d_model // n_wo

    def wo_copy(j):
        cs = pl.ds(j * wo_tile, wo_tile)
        return pltpu.make_async_copy(wo_hbm.at[:, cs], w2.at[pl.ds(0, q_loc), cs], o_sem.at[j])

    def x_copy():
        return pltpu.make_async_copy(x_hbm.at[:, me], own, x_sem)

    n_k = 4
    k_rows = ff_loc // n_k

    def w_copy(i, j):
        src, dst = ((w1_hbm, w1), (w3_hbm, w3), (w2_hbm, w2))[i]
        rs = pl.ds(j * k_rows, k_rows)
        return pltpu.make_async_copy(src.at[rs], dst.at[rs], w_sem.at[i, j])

    for j in range(n_wo):
        wo_copy(j).start()
    x_copy().start()

    barrier = pltpu.get_barrier_semaphore()
    for peer in (sib, x_nb, y_nb):
        pl.semaphore_signal(barrier, inc=1, device_id={'tp': peer}, device_id_type=pl.DeviceIdType.MESH)
    for i, g_ref in enumerate((ga_ref, gm_ref)):
        for j in range(d_model // 128):
            gains[i:i + 1, j * 128:(j + 1) * 128] = g_ref[j:j + 1, :].astype(F32)
    pl.semaphore_wait(barrier, 3)

    def xfer(k, c, ph, p):
        odd = p % 2
        cs = cols[p]
        b = buf.at[c]
        if ph == 0:
            src, dst, peer = b.at[oc, :, :, :, cs], r0.at[c, :, :, :, cs], sib
        elif ph == 1:
            src = b.at[core, :, oy, :, cs] if odd else b.at[core, ox, :, :, cs]
            dst, peer = r1.at[c, :, :, cs], (x_nb, y_nb)[odd]
        elif ph == 2:
            src, dst, peer = st.at[c, :, cs], r2.at[c, :, cs], (y_nb, x_nb)[odd]
        else:
            if ph == 3:
                src, peer = b.at[core, xb, yb, :, cs], (y_nb, x_nb)[odd]
            elif ph == 4:
                src = b.at[core, :, yb, :, cs] if odd else b.at[core, xb, :, :, cs]
                peer = (x_nb, y_nb)[odd]
            else:
                src, peer = b.at[core, :, :, :, cs], sib
            dst = src
        return pltpu.make_async_remote_copy(
            src_ref=src, dst_ref=dst, send_sem=send_sem.at[k, c, ph * n_p + p], recv_sem=recv_sem.at[k, c, ph * n_p + p],
            device_id={'tp': peer}, device_id_type=pl.DeviceIdType.MESH)

    def start(k, c, ph, p):
        xfer(k, c, ph, p).start()

    def s1(k, c, p):
        cs = cols[p]
        x = xfer(k, c, 0, p)
        x.wait_recv()
        if p % 2 == 0:
            buf[c, core, ox, :, :, cs] = buf[c, core, ox, :, :, cs] + r0[c, ox, :, :, cs]
            start(k, c, 1, p)
            buf[c, core, xb, :, :, cs] = buf[c, core, xb, :, :, cs] + r0[c, xb, :, :, cs]
        else:
            for i in range(2):
                buf[c, core, i, oy, :, cs] = buf[c, core, i, oy, :, cs] + r0[c, i, oy, :, cs]
            start(k, c, 1, p)
            for i in range(2):
                buf[c, core, i, yb, :, cs] = buf[c, core, i, yb, :, cs] + r0[c, i, yb, :, cs]
        x.wait_send()
        if p == n_p - 1:
            pl.semaphore_signal(free_sem.at[k, c], inc=1, device_id={'tp': sib}, device_id_type=pl.DeviceIdType.MESH)

    def s2(k, c, p):
        cs = cols[p]
        x = xfer(k, c, 1, p)
        x.wait_recv()
        if p % 2 == 0:
            st[c, :, cs] = buf[c, core, xb, oy, :, cs] + r1[c, oy, :, cs]
            start(k, c, 2, p)
            buf[c, core, xb, yb, :, cs] = buf[c, core, xb, yb, :, cs] + r1[c, yb, :, cs]
        else:
            st[c, :, cs] = buf[c, core, ox, yb, :, cs] + r1[c, ox, :, cs]
            start(k, c, 2, p)
            buf[c, core, xb, yb, :, cs] = buf[c, core, xb, yb, :, cs] + r1[c, xb, :, cs]
        x.wait_send()

    v_tile = 256

    def s3(k, c):
        sq = jnp.zeros((blk, v_tile), F32)
        for j in range(d_model // v_tile):
            if j * v_tile % wide == 0:
                xfer(k, c, 2, j * v_tile // wide).wait_recv()
            cs = pl.ds(j * v_tile, v_tile)
            tot = (buf[c, core, xb, yb, :, cs].astype(F32) + r2[c, :, cs].astype(F32)).astype(BF16)
            buf[c, core, xb, yb, :, cs] = tot
            tot = tot.astype(F32)
            sq = sq + tot * tot
        scale = rms_factor(jnp.sum(sq, axis=-1, keepdims=True), d_model)
        for p in range(n_p):
            for j in range(wide // v_tile):
                cs = pl.ds(p * wide + j * v_tile, v_tile)
                res = (own[c, :, cs].astype(F32) + buf[c, core, xb, yb, :, cs].astype(F32) * scale * gains[k:k + 1, cs]).astype(BF16)
                buf[c, core, xb, yb, :, cs] = res
                if k == 0:
                    own[c, :, cs] = res
            start(k, c, 3, p)
        for p in range(n_p):
            xfer(k, c, 2, p).wait_send()

    def g2(k, c, p):
        xfer(k, c, 3, p).wait_recv()
        start(k, c, 4, p)

    def g3(k, c, p):
        xfer(k, c, 4, p).wait_recv()
        if p == 0:
            pl.semaphore_wait(free_sem.at[k, c], 1)
        start(k, c, 5, p)

    def done(k, c):
        for p in range(n_p):
            xfer(k, c, 5, p).wait_recv()
        for ph in range(3, 6):
            for p in range(n_p):
                xfer(k, c, ph, p).wait_send()

    def y_copy(c):
        return pltpu.make_async_copy(buf.at[c], y_hbm.at[c], y_sem.at[c])

    def fin(k, c):
        done(k, c)
        y_copy(c).start()

    def both(fn, k, c):
        for p in range(n_p):
            fn(k, c, p)

    def p1(c):
        for p in range(n_p):
            if c == 0:
                wo_copy(p).wait()
            acc = jnp.dot(o_ref[c], w2[0:q_loc, cols[p]], preferred_element_type=F32)
            buf[c, :, :, :, :, cols[p]] = acc.astype(BF16).reshape(2, 2, 2, blk, wide)
            start(0, c, 0, p)

    gu_tile = 256
    gu_tiles = [(f, min(gu_tile, ff_loc - f)) for f in range(0, ff_loc, gu_tile)]

    def dot_t(w_rows, h):
        return lax.dot_general(w_rows, h, (((1,), (1,)), ((), ())), preferred_element_type=F32)

    def p2(services):
        def chunk(c, carry):
            def serve(point):
                for (sc, sp), fns in services.items():
                    if sp == point:
                        @pl.when(c == sc)
                        def _(fns=fns):
                            for fn in fns:
                                fn()

            for j, (f0, fw) in enumerate(gu_tiles):
                serve(j)
                h = buf[c].reshape(rows, d_model)
                g = dot_t(w1[f0:f0 + fw, :], h)
                up = dot_t(w3[f0:f0 + fw, :], h)
                act[:, f0:f0 + fw] = jnp.transpose(g * jax.nn.sigmoid(g) * up).astype(BF16)

            base = len(gu_tiles)

            def down(cs):
                acc = jnp.dot(act[...], w2[:, cs], preferred_element_type=F32)
                buf[c, :, :, :, :, cs] = acc.astype(BF16).reshape(2, 2, 2, blk, half_d)
            for ab in range(2):
                serve(base + ab)
                down(pl.ds(ab * half_d, half_d))
                start(1, c, 0, 2 * ab)
                start(1, c, 0, 2 * ab + 1)
            return carry
        lax.fori_loop(0, n_chunks, chunk, 0)

    p1(0)
    for j in range(n_k):
        for i in range(2):
            w_copy(i, j).start()
    both(s1, 0, 0)
    p1(1)
    p1(2)
    for j in range(n_k):
        w_copy(2, j).start()
    both(s2, 0, 0)
    both(s1, 0, 1)
    x_copy().wait()
    s3(0, 0)
    both(s2, 0, 1)
    both(g2, 0, 0)
    s3(0, 1)
    both(s1, 0, 2)
    both(g3, 0, 0)
    for j in range(n_k):
        for i in range(3):
            w_copy(i, j).wait()
    done(0, 0)

    F = functools.partial
    p2({
        (0, 0): [F(both, g2, 0, 1)],
        (0, 2): [F(both, s2, 0, 2)],
        (0, 5): [F(both, g3, 0, 1)],
        (0, 6): [F(s3, 0, 2)],
        (1, 0): [F(done, 0, 1), F(both, g2, 0, 2)],
        (1, 1): [F(both, s1, 1, 0)],
        (1, 4): [F(both, g3, 0, 2)],
        (1, 6): [F(both, s2, 1, 0)],
        (2, 0): [F(done, 0, 2), F(s3, 1, 0)],
        (2, 1): [F(both, s1, 1, 1)],
        (2, 3): [F(both, g2, 1, 0)],
        (2, 5): [F(both, s2, 1, 1)],
        (2, 7): [F(both, g3, 1, 0)],
    })
    both(s1, 1, 2)
    s3(1, 1)
    both(s2, 1, 2)
    both(g2, 1, 1)
    s3(1, 2)
    both(g3, 1, 1)
    both(g2, 1, 2)
    fin(1, 0)
    fin(1, 1)
    both(g3, 1, 2)
    fin(1, 2)
    for c in range(n_chunks):
        y_copy(c).wait()


def tail(o, x_seq, w_o, w1, w3, w2, g_attn, g_mlp):
    n_chunks, rows, d_model = x_seq.shape
    q_loc = o.shape[-1]
    ff_loc = w2.shape[0]
    blk = rows // 8
    dims = (n_chunks, rows, d_model, q_loc, ff_loc)
    vmem = pl.BlockSpec(memory_space=pltpu.VMEM)
    hbm = pl.BlockSpec(memory_space=pl.ANY)
    y = pl.pallas_call(
        functools.partial(tail_kernel, dims),
        name='tail',
        out_shape=jax.ShapeDtypeStruct((n_chunks, 2, 2, 2, blk, d_model), BF16),
        in_specs=[vmem, vmem, vmem, hbm, hbm, hbm, hbm, hbm],
        out_specs=hbm,
        scratch_shapes=[
            pltpu.VMEM((n_chunks, 2, 2, 2, blk, d_model), BF16),
            pltpu.VMEM((n_chunks, 2, 2, blk, d_model), BF16),
            pltpu.VMEM((n_chunks, 2, blk, d_model), BF16),
            pltpu.VMEM((n_chunks, blk, d_model), BF16),
            pltpu.VMEM((n_chunks, blk, d_model), BF16),
            pltpu.VMEM((n_chunks, blk, d_model), BF16),
            pltpu.VMEM((rows, ff_loc), BF16),
            pltpu.VMEM((2, d_model), F32),
            pltpu.VMEM((ff_loc, d_model), BF16),
            pltpu.VMEM((ff_loc, d_model), BF16),
            pltpu.VMEM((ff_loc, d_model), BF16),
            pltpu.SemaphoreType.DMA((2, n_chunks, 24)),
            pltpu.SemaphoreType.DMA((2, n_chunks, 24)),
            pltpu.SemaphoreType.DMA((3, 4)),
            pltpu.SemaphoreType.DMA((4,)),
            pltpu.SemaphoreType.DMA,
            pltpu.SemaphoreType.DMA((n_chunks,)),
            pltpu.SemaphoreType.REGULAR((2, n_chunks)),
        ],
        compiler_params=pltpu.CompilerParams(collective_id=1, has_side_effects=True, vmem_limit_bytes=67043328),
    )(o, g_attn.reshape(-1, 128), g_mlp.reshape(-1, 128), x_seq.reshape(n_chunks, 8, blk, d_model), w_o, w1.T, w3.T, w2)
    return y.reshape(n_chunks, rows, d_model)


def head_kernel(dims, len_ref, gq_ref, gk_ref, freq_ref, x_hbm, wq_hbm, wk_hbm, wv_hbm, q_out, k_out, v_out,
                x, w, raw, cos_t, sin_t, sums, x_sem, w_sem, send_sem, recv_sem):
    n_steps, rows, d_model, q_loc, hd, n_tp = dims
    heads = q_loc // hd
    width = q_loc + 2 * hd
    tp = lax.axis_index('tp')

    def x_copy(t):
        return pltpu.make_async_copy(x_hbm.at[t], x.at[t], x_sem.at[t])

    n_k = 4
    k_rows = d_model // n_k

    def w_copies(j):
        rs = pl.ds(j * k_rows, k_rows)
        return (pltpu.make_async_copy(wq_hbm.at[rs], w.at[rs, pl.ds(0, q_loc)], w_sem.at[0, j]),
                pltpu.make_async_copy(wk_hbm.at[rs], w.at[rs, pl.ds(q_loc, hd)], w_sem.at[1, j]),
                pltpu.make_async_copy(wv_hbm.at[rs], w.at[rs, pl.ds(q_loc + hd, hd)], w_sem.at[2, j]))

    x_copy(0).start()
    for j in range(n_k):
        for cp in w_copies(j):
            cp.start()
    for t in range(1, n_steps):
        x_copy(t).start()

    barrier = pltpu.get_barrier_semaphore()
    peers = [lax.rem(tp + d, n_tp) for d in range(1, n_tp)]
    for p in peers:
        pl.semaphore_signal(barrier, inc=1, device_id={'tp': p}, device_id_type=pl.DeviceIdType.MESH)

    lens = jnp.transpose(jnp.broadcast_to(len_ref[...].astype(F32), (rows, rows)))
    lane = lax.broadcasted_iota(jnp.int32, (rows, hd), 1)
    sign = jnp.where(lane < hd // 2, -1.0, 1.0).astype(F32)
    for t in range(n_steps):
        ang = (lens + float(t)) * freq_ref[...]
        cos_t[t] = jnp.cos(ang)
        sin_t[t] = jnp.sin(ang) * sign

    for j in range(n_k):
        for cp in w_copies(j)[:2]:
            cp.wait()
    sq_lane = lax.broadcasted_iota(jnp.int32, (rows, rows), 1)

    def send(t, d):
        return pltpu.make_async_remote_copy(
            src_ref=sums.at[t, tp], dst_ref=sums.at[t, tp], send_sem=send_sem.at[t, d], recv_sem=recv_sem.at[t, d],
            device_id={'tp': peers[d]}, device_id_type=pl.DeviceIdType.MESH)

    def project(t):
        x_copy(t).wait()
        res = jnp.dot(x[t], w[:, 0:q_loc + hd], preferred_element_type=F32).astype(BF16)
        raw[t] = res
        q = res[:, :q_loc].astype(F32)
        k = res[:, q_loc:q_loc + hd].astype(F32)
        part = jnp.where(sq_lane == 0, jnp.sum(q * q, axis=-1, keepdims=True), jnp.sum(k * k, axis=-1, keepdims=True))
        sums[t, tp] = jnp.transpose(part)[0:8]
        if t == 0:
            pl.semaphore_wait(barrier, n_tp - 1)
        for d in range(n_tp - 1):
            send(t, d).start()

    def rotate_all(t):
        for d in range(n_tp - 1):
            send(t, d).wait()
        tot = sums[t, 0]
        for d in range(1, n_tp):
            tot = tot + sums[t, d]
        full = jnp.transpose(jnp.concatenate([tot, jnp.zeros((rows - 8, rows), F32)], axis=0))
        q_scale = rms_factor(full[:, 0:1], q_loc * n_tp)
        k_scale = rms_factor(full[:, 1:2], hd * n_tp)

        def rotate(col, scale, gain):
            val = raw[t, :, col:col + hd].astype(F32) * scale * gain.astype(F32)
            return (val * cos_t[t] + pltpu.roll(val, hd // 2, 1) * sin_t[t]).astype(BF16).astype(F32)
        for j in range(heads):
            q_out[pl.ds(t * heads + j, rows, stride=16), :] = rotate(j * hd, q_scale, gq_ref[j:j + 1, :])
        k_out[t] = rotate(q_loc, k_scale, gk_ref[...])

    for t in range(n_steps):
        project(t)
    for j in range(n_k):
        w_copies(j)[2].wait()
    for t in range(n_steps):
        v_out[t] = jnp.dot(x[t], w[:, q_loc + hd:width], preferred_element_type=F32).astype(BF16).astype(F32)
    q_out[pl.ds(n_steps * heads, rows, stride=16), :] = jnp.zeros((rows, hd), F32)
    for t in range(n_steps):
        rotate_all(t)


def head(x_seq, cache_len, w_q, w_k, w_v, g_q, g_k, n_tp):
    n_steps, rows, d_model = x_seq.shape
    q_loc, hd = w_q.shape[1], w_k.shape[1]
    width = q_loc + 2 * hd
    half = hd // 2
    inv_freq = np.float32(ROPE_THETA) ** (-(np.arange(half, dtype=np.float32) * np.float32(2.0 / hd)))
    freq = jnp.asarray(np.concatenate([inv_freq, inv_freq]).reshape(1, hd), F32)
    vmem = pl.BlockSpec(memory_space=pltpu.VMEM)
    hbm = pl.BlockSpec(memory_space=pl.ANY)
    return pl.pallas_call(
        functools.partial(head_kernel, (n_steps, rows, d_model, q_loc, hd, n_tp)),
        name='head',
        out_shape=(jax.ShapeDtypeStruct((rows * 16, hd), F32),
                   jax.ShapeDtypeStruct((n_steps, rows, hd), F32),
                   jax.ShapeDtypeStruct((n_steps, rows, hd), F32)),
        in_specs=[vmem] * 4 + [hbm] * 4,
        out_specs=(vmem,) * 3,
        scratch_shapes=[
            pltpu.VMEM((n_steps, rows, d_model), BF16),
            pltpu.VMEM((d_model, width), BF16),
            pltpu.VMEM((n_steps, rows, q_loc + hd), BF16),
            pltpu.VMEM((n_steps, rows, hd), F32),
            pltpu.VMEM((n_steps, rows, hd), F32),
            pltpu.VMEM((n_steps, n_tp, 8, rows), F32),
            pltpu.SemaphoreType.DMA((n_steps,)),
            pltpu.SemaphoreType.DMA((3, 4)),
            pltpu.SemaphoreType.DMA((n_steps, n_tp - 1)),
            pltpu.SemaphoreType.DMA((n_steps, n_tp - 1)),
        ],
        compiler_params=pltpu.CompilerParams(collective_id=0, has_side_effects=True, vmem_limit_bytes=67043328),
    )(cache_len.reshape(1, -1), g_q.reshape(-1, hd), g_k.reshape(1, -1), freq, x_seq, w_q, w_k, w_v)


def attn_kernel(dims, len_ref, q_ref, kn_ref, vn_ref, k_ref, v_ref, o_ref, ko_ref, vo_ref, s_scr, e_scr, l_scr, o_scr):
    n_steps, nb, heads, hd, seq_max = dims
    first = pl.program_id(0) * nb
    win = 32
    row_step = lax.broadcasted_iota(jnp.int32, (16, seq_max), 0) // heads
    col = lax.broadcasted_iota(jnp.int32, (16, seq_max), 1)
    ahead = col - row_step
    win_row = lax.broadcasted_iota(jnp.int32, (win, hd), 0)
    for src, new, dst in ((k_ref, kn_ref, ko_ref), (v_ref, vn_ref, vo_ref)):
        dst[...] = src[...]
        for i in range(nb):
            ln = len_ref[first + i]
            base = pl.multiple_of(jnp.minimum((ln // 16) * 16, seq_max - win), 16)
            rel = win_row + (base - ln)
            cut = src[i, pl.ds(base, win), :].astype(F32)
            for t in range(n_steps):
                cut = jnp.where(rel == t, new[t, i:i + 1, :], cut)
            dst[i, pl.ds(base, win), :] = cut.astype(BF16)
    for i in range(nb):
        s = lax.dot_general(q_ref[i].astype(BF16), ko_ref[i], (((1,), (1,)), ((), ())), preferred_element_type=F32) * hd ** -0.5
        s_scr[i * 16:(i + 1) * 16, :] = jnp.where(ahead <= len_ref[first + i], s, -jnp.inf)
    for i in range(0, nb, 2):
        rs = slice(i * 16, (i + 2) * 16)
        s = s_scr[rs, :]
        e = jnp.exp(s - jnp.max(s, axis=-1, keepdims=True))
        l_scr[rs, :] = jnp.broadcast_to(jnp.sum(e, axis=-1, keepdims=True), (32, hd))
        e_scr[rs, :] = e.astype(BF16)
    for i in range(nb):
        rs = slice(i * 16, (i + 1) * 16)
        o_scr[rs, :] = jnp.dot(e_scr[rs, :], vo_ref[i], preferred_element_type=F32)
    o_scr[...] = o_scr[...] / l_scr[...]
    for t in range(n_steps):
        for j in range(heads):
            o_ref[t, :, j * hd:(j + 1) * hd] = o_scr[pl.ds(t * heads + j, nb, stride=16), :].astype(BF16)


def attend(q, kn, vn, k_cache, v_cache, cache_len, heads):
    n_rows, _, seq_max, hd = k_cache.shape
    n_steps = kn.shape[0]
    nb = 32
    cache_spec = pl.BlockSpec((nb, seq_max, hd), lambda i, ln: (i, 0, 0))
    new_spec = pl.BlockSpec((n_steps, nb, hd), lambda i, ln: (0, i, 0))
    cache_shape = jax.ShapeDtypeStruct((n_rows, seq_max, hd), BF16)
    flops = 4 * n_rows * 16 * seq_max * hd
    return pl.pallas_call(
        functools.partial(attn_kernel, (n_steps, nb, heads, hd, seq_max)),
        name='attend',
        grid_spec=pltpu.PrefetchScalarGridSpec(
            num_scalar_prefetch=1,
            grid=(n_rows // nb,),
            in_specs=[pl.BlockSpec((nb, 16, hd), lambda i, ln: (i, 0, 0)), new_spec, new_spec, cache_spec, cache_spec],
            out_specs=(pl.BlockSpec((n_steps, nb, heads * hd), lambda i, ln: (0, i, 0)), cache_spec, cache_spec),
            scratch_shapes=[pltpu.VMEM((nb * 16, seq_max), F32), pltpu.VMEM((nb * 16, seq_max), BF16), pltpu.VMEM((nb * 16, hd), F32), pltpu.VMEM((nb * 16, hd), F32)],
        ),
        out_shape=(jax.ShapeDtypeStruct((n_steps, n_rows, heads * hd), BF16), cache_shape, cache_shape),
        compiler_params=pltpu.CompilerParams(vmem_limit_bytes=67043328),
        cost_estimate=pl.CostEstimate(flops=flops, bytes_accessed=4 * n_rows * seq_max * hd * 2, transcendentals=n_rows * 16 * seq_max),
    )(cache_len, q.reshape(n_rows, 16, hd), kn, vn, k_cache[:, 0], v_cache[:, 0])


def local_layer(n_tp, x_seq, cache_len, k_cache, v_cache, w_q, w_k, w_v, w_o, w_gate, w_up, w_down, g_q, g_k, g_attn, g_mlp):
    heads = w_q.shape[1] // k_cache.shape[3]
    q, kn, vn = head(x_seq, cache_len, w_q, w_k, w_v, g_q, g_k, n_tp)
    o, k_out, v_out = attend(q, kn, vn, k_cache, v_cache, cache_len, heads)
    y = tail(o, x_seq, w_o, w_gate, w_up, w_down, g_attn, g_mlp)
    return y, k_out[:, None], v_out[:, None]


def solution(mesh):
    tp_size = mesh.shape['tp']
    data_spec = P(None, 'dp', None)
    cache_spec = P('dp', 'tp', None, None)
    col_spec = P(None, 'tp')
    row_spec = P('tp', None)
    arg_specs = (data_spec, P('dp'), cache_spec, cache_spec, col_spec, col_spec, col_spec, row_spec, col_spec, col_spec, row_spec, P('tp'), P('tp'), P(None), P(None))
    out_specs = (data_spec, cache_spec, cache_spec)
    return jax.shard_map(functools.partial(local_layer, tp_size), mesh=mesh, in_specs=arg_specs, out_specs=out_specs, check_vma=False)
```

```python
import functools

import jax
import jax.numpy as jnp
import numpy as np
from jax import lax
from jax.experimental import pallas as pl
from jax.experimental.pallas import tpu as pltpu
from jax.sharding import PartitionSpec as P

ROPE_THETA = 500000.0
NORM_EPS = 1e-6
F32 = jnp.float32
BF16 = jnp.bfloat16


def rms_factor(sq_sum, full_width):
    return lax.rsqrt(sq_sum / full_width + NORM_EPS)


def tail_kernel(dims, o_ref, ga_ref, gm_ref, x_hbm, wo_hbm, w1_hbm, w3_hbm, w2_hbm, y_hbm,
                buf, r0, r1, r2, st, own, act, gains, w1, w3, w2,
                send_sem, recv_sem, w_sem, o_sem, x_sem, y_sem, free_sem):
    n_chunks, rows, d_model, q_loc, ff_loc = dims
    blk = rows // 8
    half_d = d_model // 2
    tp = lax.axis_index('tp')
    core = lax.rem(tp, 2)
    xb = lax.rem(lax.div(tp, 2), 2)
    yb = lax.div(tp, 4)
    sib = tp + 1 - 2 * core
    x_nb = tp + 2 - 4 * xb
    y_nb = tp + 4 - 8 * yb
    oc, ox, oy = 1 - core, 1 - xb, 1 - yb
    n_p = 4
    wide = d_model // n_p
    cols = [pl.ds(p * wide, wide) for p in range(n_p)]
    me = core * 4 + xb * 2 + yb

    n_wo = 4
    wo_tile = d_model // n_wo

    def wo_copy(j):
        cs = pl.ds(j * wo_tile, wo_tile)
        return pltpu.make_async_copy(wo_hbm.at[:, cs], w2.at[pl.ds(0, q_loc), cs], o_sem.at[j])

    def x_copy():
        return pltpu.make_async_copy(x_hbm.at[:, me], own, x_sem)

    n_k = 4
    k_rows = ff_loc // n_k

    def w_copy(i, j):
        src, dst = ((w1_hbm, w1), (w3_hbm, w3), (w2_hbm, w2))[i]
        rs = pl.ds(j * k_rows, k_rows)
        return pltpu.make_async_copy(src.at[rs], dst.at[rs], w_sem.at[i, j])

    for j in range(n_wo):
        wo_copy(j).start()
    x_copy().start()

    barrier = pltpu.get_barrier_semaphore()
    for peer in (sib, x_nb, y_nb):
        pl.semaphore_signal(barrier, inc=1, device_id={'tp': peer}, device_id_type=pl.DeviceIdType.MESH)
    for i, g_ref in enumerate((ga_ref, gm_ref)):
        for j in range(d_model // 128):
            gains[i:i + 1, j * 128:(j + 1) * 128] = g_ref[j:j + 1, :].astype(F32)
    pl.semaphore_wait(barrier, 3)

    def xfer(k, c, ph, p):
        odd = p % 2
        cs = cols[p]
        b = buf.at[c]
        if ph == 0:
            src, dst, peer = b.at[oc, :, :, :, cs], r0.at[c, :, :, :, cs], sib
        elif ph == 1:
            src = b.at[core, :, oy, :, cs] if odd else b.at[core, ox, :, :, cs]
            dst, peer = r1.at[c, :, :, cs], (x_nb, y_nb)[odd]
        elif ph == 2:
            src, dst, peer = st.at[c, :, cs], r2.at[c, :, cs], (y_nb, x_nb)[odd]
        else:
            if ph == 3:
                src, peer = b.at[core, xb, yb, :, cs], (y_nb, x_nb)[odd]
            elif ph == 4:
                src = b.at[core, :, yb, :, cs] if odd else b.at[core, xb, :, :, cs]
                peer = (x_nb, y_nb)[odd]
            else:
                src, peer = b.at[core, :, :, :, cs], sib
            dst = src
        return pltpu.make_async_remote_copy(
            src_ref=src, dst_ref=dst, send_sem=send_sem.at[k, c, ph * n_p + p], recv_sem=recv_sem.at[k, c, ph * n_p + p],
            device_id={'tp': peer}, device_id_type=pl.DeviceIdType.MESH)

    def start(k, c, ph, p):
        xfer(k, c, ph, p).start()

    def s1(k, c, p):
        cs = cols[p]
        x = xfer(k, c, 0, p)
        x.wait_recv()
        if p % 2 == 0:
            buf[c, core, ox, :, :, cs] = buf[c, core, ox, :, :, cs] + r0[c, ox, :, :, cs]
            start(k, c, 1, p)
            buf[c, core, xb, :, :, cs] = buf[c, core, xb, :, :, cs] + r0[c, xb, :, :, cs]
        else:
            for i in range(2):
                buf[c, core, i, oy, :, cs] = buf[c, core, i, oy, :, cs] + r0[c, i, oy, :, cs]
            start(k, c, 1, p)
            for i in range(2):
                buf[c, core, i, yb, :, cs] = buf[c, core, i, yb, :, cs] + r0[c, i, yb, :, cs]
        x.wait_send()
        if p == n_p - 1:
            pl.semaphore_signal(free_sem.at[k, c], inc=1, device_id={'tp': sib}, device_id_type=pl.DeviceIdType.MESH)

    def s2(k, c, p):
        cs = cols[p]
        x = xfer(k, c, 1, p)
        x.wait_recv()
        if p % 2 == 0:
            st[c, :, cs] = buf[c, core, xb, oy, :, cs] + r1[c, oy, :, cs]
            start(k, c, 2, p)
            buf[c, core, xb, yb, :, cs] = buf[c, core, xb, yb, :, cs] + r1[c, yb, :, cs]
        else:
            st[c, :, cs] = buf[c, core, ox, yb, :, cs] + r1[c, ox, :, cs]
            start(k, c, 2, p)
            buf[c, core, xb, yb, :, cs] = buf[c, core, xb, yb, :, cs] + r1[c, xb, :, cs]
        x.wait_send()

    v_tile = 256

    def s3(k, c):
        sq = jnp.zeros((blk, v_tile), F32)
        for j in range(d_model // v_tile):
            if j * v_tile % wide == 0:
                xfer(k, c, 2, j * v_tile // wide).wait_recv()
            cs = pl.ds(j * v_tile, v_tile)
            tot = (buf[c, core, xb, yb, :, cs].astype(F32) + r2[c, :, cs].astype(F32)).astype(BF16)
            buf[c, core, xb, yb, :, cs] = tot
            tot = tot.astype(F32)
            sq = sq + tot * tot
        scale = rms_factor(jnp.sum(sq, axis=-1, keepdims=True), d_model)
        for p in range(n_p):
            for j in range(wide // v_tile):
                cs = pl.ds(p * wide + j * v_tile, v_tile)
                res = (own[c, :, cs].astype(F32) + buf[c, core, xb, yb, :, cs].astype(F32) * scale * gains[k:k + 1, cs]).astype(BF16)
                buf[c, core, xb, yb, :, cs] = res
                if k == 0:
                    own[c, :, cs] = res
            start(k, c, 3, p)
        for p in range(n_p):
            xfer(k, c, 2, p).wait_send()

    def g2(k, c, p):
        xfer(k, c, 3, p).wait_recv()
        start(k, c, 4, p)

    def g3(k, c, p):
        xfer(k, c, 4, p).wait_recv()
        if p == 0:
            pl.semaphore_wait(free_sem.at[k, c], 1)
        start(k, c, 5, p)

    def done(k, c):
        for p in range(n_p):
            xfer(k, c, 5, p).wait_recv()
        for ph in range(3, 6):
            for p in range(n_p):
                xfer(k, c, ph, p).wait_send()

    def y_copy(c):
        return pltpu.make_async_copy(buf.at[c], y_hbm.at[c], y_sem.at[c])

    def fin(k, c):
        done(k, c)
        y_copy(c).start()

    def both(fn, k, c):
        for p in range(n_p):
            fn(k, c, p)

    def p1(c):
        for p in range(n_p):
            if c == 0:
                wo_copy(p).wait()
            acc = jnp.dot(o_ref[c], w2[0:q_loc, cols[p]], preferred_element_type=F32)
            buf[c, :, :, :, :, cols[p]] = acc.astype(BF16).reshape(2, 2, 2, blk, wide)
            start(0, c, 0, p)

    gu_tile = 256
    gu_tiles = [(f, min(gu_tile, ff_loc - f)) for f in range(0, ff_loc, gu_tile)]

    def dot_t(w_rows, h):
        return lax.dot_general(w_rows, h, (((1,), (1,)), ((), ())), preferred_element_type=F32)

    def p2(services):
        def chunk(c, carry):
            def serve(point):
                for (sc, sp), fns in services.items():
                    if sp == point:
                        @pl.when(c == sc)
                        def _(fns=fns):
                            for fn in fns:
                                fn()

            for j, (f0, fw) in enumerate(gu_tiles):
                serve(j)
                h = buf[c].reshape(rows, d_model)
                g = dot_t(w1[f0:f0 + fw, :], h)
                up = dot_t(w3[f0:f0 + fw, :], h)
                act[:, f0:f0 + fw] = jnp.transpose(g * jax.nn.sigmoid(g) * up).astype(BF16)

            base = len(gu_tiles)

            def down(cs):
                acc = jnp.dot(act[...], w2[:, cs], preferred_element_type=F32)
                buf[c, :, :, :, :, cs] = acc.astype(BF16).reshape(2, 2, 2, blk, half_d)
            for ab in range(2):
                serve(base + ab)
                down(pl.ds(ab * half_d, half_d))
                start(1, c, 0, 2 * ab)
                start(1, c, 0, 2 * ab + 1)
            return carry
        lax.fori_loop(0, n_chunks, chunk, 0)

    p1(0)
    for j in range(n_k):
        for i in range(2):
            w_copy(i, j).start()
    both(s1, 0, 0)
    p1(1)
    p1(2)
    for j in range(n_k):
        w_copy(2, j).start()
    both(s2, 0, 0)
    both(s1, 0, 1)
    x_copy().wait()
    s3(0, 0)
    both(s2, 0, 1)
    both(g2, 0, 0)
    s3(0, 1)
    both(s1, 0, 2)
    both(g3, 0, 0)
    for j in range(n_k):
        for i in range(3):
            w_copy(i, j).wait()
    done(0, 0)

    F = functools.partial
    p2({
        (0, 0): [F(both, g2, 0, 1)],
        (0, 2): [F(both, s2, 0, 2)],
        (0, 5): [F(both, g3, 0, 1)],
        (0, 6): [F(s3, 0, 2)],
        (1, 0): [F(done, 0, 1), F(both, g2, 0, 2)],
        (1, 1): [F(both, s1, 1, 0)],
        (1, 4): [F(both, g3, 0, 2)],
        (1, 6): [F(both, s2, 1, 0)],
        (2, 0): [F(done, 0, 2), F(s3, 1, 0)],
        (2, 1): [F(both, s1, 1, 1)],
        (2, 3): [F(both, g2, 1, 0)],
        (2, 5): [F(both, s2, 1, 1)],
        (2, 7): [F(both, g3, 1, 0)],
    })
    both(s1, 1, 2)
    s3(1, 1)
    both(s2, 1, 2)
    both(g2, 1, 1)
    s3(1, 2)
    both(g3, 1, 1)
    both(g2, 1, 2)
    fin(1, 0)
    fin(1, 1)
    both(g3, 1, 2)
    fin(1, 2)
    for c in range(n_chunks):
        y_copy(c).wait()


def tail(o, x_seq, w_o, w1, w3, w2, g_attn, g_mlp):
    n_chunks, rows, d_model = x_seq.shape
    q_loc = o.shape[-1]
    ff_loc = w2.shape[0]
    blk = rows // 8
    dims = (n_chunks, rows, d_model, q_loc, ff_loc)
    vmem = pl.BlockSpec(memory_space=pltpu.VMEM)
    hbm = pl.BlockSpec(memory_space=pl.ANY)
    y = pl.pallas_call(
        functools.partial(tail_kernel, dims),
        name='tail',
        out_shape=jax.ShapeDtypeStruct((n_chunks, 2, 2, 2, blk, d_model), BF16),
        in_specs=[vmem, vmem, vmem, hbm, hbm, hbm, hbm, hbm],
        out_specs=hbm,
        scratch_shapes=[
            pltpu.VMEM((n_chunks, 2, 2, 2, blk, d_model), BF16),
            pltpu.VMEM((n_chunks, 2, 2, blk, d_model), BF16),
            pltpu.VMEM((n_chunks, 2, blk, d_model), BF16),
            pltpu.VMEM((n_chunks, blk, d_model), BF16),
            pltpu.VMEM((n_chunks, blk, d_model), BF16),
            pltpu.VMEM((n_chunks, blk, d_model), BF16),
            pltpu.VMEM((rows, ff_loc), BF16),
            pltpu.VMEM((2, d_model), F32),
            pltpu.VMEM((ff_loc, d_model), BF16),
            pltpu.VMEM((ff_loc, d_model), BF16),
            pltpu.VMEM((ff_loc, d_model), BF16),
            pltpu.SemaphoreType.DMA((2, n_chunks, 24)),
            pltpu.SemaphoreType.DMA((2, n_chunks, 24)),
            pltpu.SemaphoreType.DMA((3, 4)),
            pltpu.SemaphoreType.DMA((4,)),
            pltpu.SemaphoreType.DMA,
            pltpu.SemaphoreType.DMA((n_chunks,)),
            pltpu.SemaphoreType.REGULAR((2, n_chunks)),
        ],
        compiler_params=pltpu.CompilerParams(collective_id=1, has_side_effects=True, vmem_limit_bytes=67043328),
    )(o, g_attn.reshape(-1, 128), g_mlp.reshape(-1, 128), x_seq.reshape(n_chunks, 8, blk, d_model), w_o, w1.T, w3.T, w2)
    return y.reshape(n_chunks, rows, d_model)


def head_kernel(dims, len_ref, gq_ref, gk_ref, freq_ref, x_hbm, wq_hbm, wk_hbm, wv_hbm, q_out, k_out, v_out,
                x, w, raw, cos_t, sin_t, sums, x_sem, w_sem, send_sem, recv_sem):
    n_steps, rows, d_model, q_loc, hd, n_tp = dims
    heads = q_loc // hd
    width = q_loc + 2 * hd
    tp = lax.axis_index('tp')

    def x_copy(t):
        return pltpu.make_async_copy(x_hbm.at[t], x.at[t], x_sem.at[t])

    n_k = 4
    k_rows = d_model // n_k

    def w_copies(j):
        rs = pl.ds(j * k_rows, k_rows)
        return (pltpu.make_async_copy(wq_hbm.at[rs], w.at[rs, pl.ds(0, q_loc)], w_sem.at[0, j]),
                pltpu.make_async_copy(wk_hbm.at[rs], w.at[rs, pl.ds(q_loc, hd)], w_sem.at[1, j]),
                pltpu.make_async_copy(wv_hbm.at[rs], w.at[rs, pl.ds(q_loc + hd, hd)], w_sem.at[2, j]))

    x_copy(0).start()
    for j in range(n_k):
        for cp in w_copies(j):
            cp.start()
    for t in range(1, n_steps):
        x_copy(t).start()

    barrier = pltpu.get_barrier_semaphore()
    peers = [lax.rem(tp + d, n_tp) for d in range(1, n_tp)]
    for p in peers:
        pl.semaphore_signal(barrier, inc=1, device_id={'tp': p}, device_id_type=pl.DeviceIdType.MESH)

    lens = jnp.transpose(jnp.broadcast_to(len_ref[...].astype(F32), (rows, rows)))
    lane = lax.broadcasted_iota(jnp.int32, (rows, hd), 1)
    sign = jnp.where(lane < hd // 2, -1.0, 1.0).astype(F32)
    for t in range(n_steps):
        ang = (lens + float(t)) * freq_ref[...]
        cos_t[t] = jnp.cos(ang)
        sin_t[t] = jnp.sin(ang) * sign

    for j in range(n_k):
        for cp in w_copies(j)[:2]:
            cp.wait()
    sq_lane = lax.broadcasted_iota(jnp.int32, (rows, rows), 1)

    def send(t, d):
        return pltpu.make_async_remote_copy(
            src_ref=sums.at[t, tp], dst_ref=sums.at[t, tp], send_sem=send_sem.at[t, d], recv_sem=recv_sem.at[t, d],
            device_id={'tp': peers[d]}, device_id_type=pl.DeviceIdType.MESH)

    def project(t):
        x_copy(t).wait()
        res = jnp.dot(x[t], w[:, 0:q_loc + hd], preferred_element_type=F32).astype(BF16)
        raw[t] = res
        q = res[:, :q_loc].astype(F32)
        k = res[:, q_loc:q_loc + hd].astype(F32)
        part = jnp.where(sq_lane == 0, jnp.sum(q * q, axis=-1, keepdims=True), jnp.sum(k * k, axis=-1, keepdims=True))
        sums[t, tp] = jnp.transpose(part)[0:8]
        if t == 0:
            pl.semaphore_wait(barrier, n_tp - 1)
        for d in range(n_tp - 1):
            send(t, d).start()

    def rotate_all(t):
        for d in range(n_tp - 1):
            send(t, d).wait()
        tot = sums[t, 0]
        for d in range(1, n_tp):
            tot = tot + sums[t, d]
        full = jnp.transpose(jnp.concatenate([tot, jnp.zeros((rows - 8, rows), F32)], axis=0))
        q_scale = rms_factor(full[:, 0:1], q_loc * n_tp)
        k_scale = rms_factor(full[:, 1:2], hd * n_tp)

        def rotate(col, scale, gain):
            val = raw[t, :, col:col + hd].astype(F32) * scale * gain.astype(F32)
            return (val * cos_t[t] + pltpu.roll(val, hd // 2, 1) * sin_t[t]).astype(BF16).astype(F32)
        for j in range(heads):
            q_out[pl.ds(t * heads + j, rows, stride=16), :] = rotate(j * hd, q_scale, gq_ref[j:j + 1, :])
        k_out[t] = rotate(q_loc, k_scale, gk_ref[...])

    for t in range(n_steps):
        project(t)
    for j in range(n_k):
        w_copies(j)[2].wait()
    for t in range(n_steps):
        v_out[t] = jnp.dot(x[t], w[:, q_loc + hd:width], preferred_element_type=F32).astype(BF16).astype(F32)
    q_out[pl.ds(n_steps * heads, rows, stride=16), :] = jnp.zeros((rows, hd), F32)
    for t in range(n_steps):
        rotate_all(t)


def head(x_seq, cache_len, w_q, w_k, w_v, g_q, g_k, n_tp):
    n_steps, rows, d_model = x_seq.shape
    q_loc, hd = w_q.shape[1], w_k.shape[1]
    width = q_loc + 2 * hd
    half = hd // 2
    inv_freq = np.float32(ROPE_THETA) ** (-(np.arange(half, dtype=np.float32) * np.float32(2.0 / hd)))
    freq = jnp.asarray(np.concatenate([inv_freq, inv_freq]).reshape(1, hd), F32)
    vmem = pl.BlockSpec(memory_space=pltpu.VMEM)
    hbm = pl.BlockSpec(memory_space=pl.ANY)
    return pl.pallas_call(
        functools.partial(head_kernel, (n_steps, rows, d_model, q_loc, hd, n_tp)),
        name='head',
        out_shape=(jax.ShapeDtypeStruct((rows * 16, hd), F32),
                   jax.ShapeDtypeStruct((n_steps, rows, hd), F32),
                   jax.ShapeDtypeStruct((n_steps, rows, hd), F32)),
        in_specs=[vmem] * 4 + [hbm] * 4,
        out_specs=(vmem,) * 3,
        scratch_shapes=[
            pltpu.VMEM((n_steps, rows, d_model), BF16),
            pltpu.VMEM((d_model, width), BF16),
            pltpu.VMEM((n_steps, rows, q_loc + hd), BF16),
            pltpu.VMEM((n_steps, rows, hd), F32),
            pltpu.VMEM((n_steps, rows, hd), F32),
            pltpu.VMEM((n_steps, n_tp, 8, rows), F32),
            pltpu.SemaphoreType.DMA((n_steps,)),
            pltpu.SemaphoreType.DMA((3, 4)),
            pltpu.SemaphoreType.DMA((n_steps, n_tp - 1)),
            pltpu.SemaphoreType.DMA((n_steps, n_tp - 1)),
        ],
        compiler_params=pltpu.CompilerParams(collective_id=0, has_side_effects=True, vmem_limit_bytes=67043328),
    )(cache_len.reshape(1, -1), g_q.reshape(-1, hd), g_k.reshape(1, -1), freq, x_seq, w_q, w_k, w_v)


def attn_kernel(dims, len_ref, q_hbm, kn_hbm, vn_hbm, k_hbm, v_hbm, o_ref, ko_hbm, vo_hbm,
                kb, vb, q, kn, vn, s_scr, e_scr, l_scr, o_scr, n_sem, in_sem, out_sem):
    n_steps, nb, heads, hd, seq_max, n_rows = dims
    n_blocks = n_rows // nb
    win = 32
    row_step = lax.broadcasted_iota(jnp.int32, (16, seq_max), 0) // heads
    col = lax.broadcasted_iota(jnp.int32, (16, seq_max), 1)
    ahead = col - row_step
    win_row = lax.broadcasted_iota(jnp.int32, (win, hd), 0)
    small = [pltpu.make_async_copy(src, dst, n_sem.at[i])
             for i, (src, dst) in enumerate(((kn_hbm, kn), (vn_hbm, vn), (q_hbm, q)))]

    def load(i, blk):
        src, dst = ((k_hbm, kb), (v_hbm, vb))[i]
        rs = pl.ds(blk * nb, nb)
        return pltpu.make_async_copy(src.at[rs], dst.at[rs], in_sem.at[i, blk])

    def store(i, blk):
        src, dst = ((kb, ko_hbm), (vb, vo_hbm))[i]
        rs = pl.ds(blk * nb, nb)
        return pltpu.make_async_copy(src.at[rs], dst.at[rs], out_sem.at[i, blk])

    for i in range(2):
        load(i, 0).start()
    for cp in small:
        cp.start()
    for blk in range(1, n_blocks):
        for i in range(2):
            load(i, blk).start()
    for cp in small:
        cp.wait()

    def block(blk, carry):
        first = blk * nb
        for j, (buf, new) in enumerate(((kb, kn), (vb, vn))):
            load(j, blk).wait()
            new_rows = [new[t, pl.ds(pl.multiple_of(first, nb), nb), :] for t in range(n_steps)]
            for i in range(nb):
                ln = len_ref[first + i]
                base = pl.multiple_of(jnp.minimum((ln // 16) * 16, seq_max - win), 16)
                rel = win_row + (base - ln)
                cut = buf[first + i, pl.ds(base, win), :].astype(F32)
                for t in range(n_steps):
                    cut = jnp.where(rel == t, new_rows[t][i:i + 1, :], cut)
                buf[first + i, pl.ds(base, win), :] = cut.astype(BF16)
            store(j, blk).start()
        for i in range(nb):
            s = lax.dot_general(q[first + i].astype(BF16), kb[first + i], (((1,), (1,)), ((), ())), preferred_element_type=F32) * hd ** -0.5
            s_scr[i * 16:(i + 1) * 16, :] = jnp.where(ahead <= len_ref[first + i], s, -jnp.inf)
        for i in range(0, nb, 2):
            rs = slice(i * 16, (i + 2) * 16)
            s = s_scr[rs, :]
            e = jnp.exp(s - jnp.max(s, axis=-1, keepdims=True))
            l_scr[rs, :] = jnp.broadcast_to(jnp.sum(e, axis=-1, keepdims=True), (32, hd))
            e_scr[rs, :] = e.astype(BF16)
        for i in range(nb):
            rs = slice(i * 16, (i + 1) * 16)
            o_scr[rs, :] = jnp.dot(e_scr[rs, :], vb[first + i], preferred_element_type=F32)
        o_scr[...] = o_scr[...] / l_scr[...]
        for t in range(n_steps):
            for j in range(heads):
                o_ref[t, pl.ds(pl.multiple_of(first, nb), nb), j * hd:(j + 1) * hd] = o_scr[pl.ds(t * heads + j, nb, stride=16), :].astype(BF16)
        return carry
    lax.fori_loop(0, n_blocks, block, 0)
    for blk in range(n_blocks):
        for i in range(2):
            store(i, blk).wait()


def attend(q, kn, vn, k_cache, v_cache, cache_len, heads):
    n_rows, _, seq_max, hd = k_cache.shape
    n_steps = kn.shape[0]
    nb = 32
    hbm = pl.BlockSpec(memory_space=pl.ANY)
    cache_shape = jax.ShapeDtypeStruct((n_rows, seq_max, hd), BF16)
    flops = 4 * n_rows * 16 * seq_max * hd
    return pl.pallas_call(
        functools.partial(attn_kernel, (n_steps, nb, heads, hd, seq_max, n_rows)),
        name='attend',
        in_specs=[pl.BlockSpec(memory_space=pltpu.SMEM)] + [hbm] * 5,
        out_specs=(pl.BlockSpec(memory_space=pltpu.VMEM), hbm, hbm),
        scratch_shapes=[
            pltpu.VMEM((n_rows, seq_max, hd), BF16),
            pltpu.VMEM((n_rows, seq_max, hd), BF16),
            pltpu.VMEM((n_rows, 16, hd), F32),
            pltpu.VMEM((n_steps, n_rows, hd), F32),
            pltpu.VMEM((n_steps, n_rows, hd), F32),
            pltpu.VMEM((nb * 16, seq_max), F32),
            pltpu.VMEM((nb * 16, seq_max), BF16),
            pltpu.VMEM((nb * 16, hd), F32),
            pltpu.VMEM((nb * 16, hd), F32),
            pltpu.SemaphoreType.DMA((3,)),
            pltpu.SemaphoreType.DMA((2, n_rows // nb)),
            pltpu.SemaphoreType.DMA((2, n_rows // nb)),
        ],
        out_shape=(jax.ShapeDtypeStruct((n_steps, n_rows, heads * hd), BF16), cache_shape, cache_shape),
        compiler_params=pltpu.CompilerParams(vmem_limit_bytes=67043328),
        cost_estimate=pl.CostEstimate(flops=flops, bytes_accessed=4 * n_rows * seq_max * hd * 2, transcendentals=n_rows * 16 * seq_max),
    )(cache_len, q.reshape(n_rows, 16, hd), kn, vn, k_cache[:, 0], v_cache[:, 0])


def finish_kernel(n, src, dst, buf, in_sem, out_sem):
    ins = [pltpu.make_async_copy(src.at[i], buf.at[i], in_sem.at[i]) for i in range(n)]
    outs = [pltpu.make_async_copy(buf.at[i], dst.at[i], out_sem.at[i]) for i in range(n)]
    for cp in ins:
        cp.start()
    for a, b in zip(ins, outs):
        a.wait()
        b.start()
    for cp in outs:
        cp.wait()


def finish(y):
    n_steps, rows, d_model = y.shape
    n = 4 * n_steps
    shape = (n, n_steps * rows // n, d_model)
    hbm = pl.BlockSpec(memory_space=pl.ANY)
    out = pl.pallas_call(
        functools.partial(finish_kernel, n),
        name='finish',
        in_specs=[hbm],
        out_specs=hbm,
        scratch_shapes=[pltpu.VMEM(shape, BF16), pltpu.SemaphoreType.DMA((n,)), pltpu.SemaphoreType.DMA((n,))],
        out_shape=jax.ShapeDtypeStruct(shape, BF16),
        compiler_params=pltpu.CompilerParams(vmem_limit_bytes=67043328),
    )(y.reshape(shape))
    return out.reshape(y.shape)


def local_layer(n_tp, x_seq, cache_len, k_cache, v_cache, w_q, w_k, w_v, w_o, w_gate, w_up, w_down, g_q, g_k, g_attn, g_mlp):
    heads = w_q.shape[1] // k_cache.shape[3]
    q, kn, vn = head(x_seq, cache_len, w_q, w_k, w_v, g_q, g_k, n_tp)
    o, k_out, v_out = attend(q, kn, vn, k_cache, v_cache, cache_len, heads)
    y = tail(o, x_seq, w_o, w_gate, w_up, w_down, g_attn, g_mlp)
    return finish(y), k_out[:, None], v_out[:, None]


def solution(mesh):
    tp_size = mesh.shape['tp']
    data_spec = P(None, 'dp', None)
    cache_spec = P('dp', 'tp', None, None)
    col_spec = P(None, 'tp')
    row_spec = P('tp', None)
    arg_specs = (data_spec, P('dp'), cache_spec, cache_spec, col_spec, col_spec, col_spec, row_spec, col_spec, col_spec, row_spec, P('tp'), P('tp'), P(None), P(None))
    out_specs = (data_spec, cache_spec, cache_spec)
    return jax.shard_map(functools.partial(local_layer, tp_size), mesh=mesh, in_specs=arg_specs, out_specs=out_specs, check_vma=False)
```

```python
import functools

import jax
import jax.numpy as jnp
import numpy as np
from jax import lax
from jax.experimental import pallas as pl
from jax.experimental.pallas import tpu as pltpu
from jax.sharding import PartitionSpec as P

ROPE_THETA = 500000.0
NORM_EPS = 1e-6
F32 = jnp.float32
BF16 = jnp.bfloat16


def rms_factor(sq_sum, full_width):
    return lax.rsqrt(sq_sum / full_width + NORM_EPS)


def tail_kernel(dims, o_ref, ga_ref, gm_ref, x_hbm, wo_hbm, w1_hbm, w3_hbm, w2_hbm, y_hbm,
                buf, r0, r1, r2, st, own, act, gains, w1, w3, w2,
                send_sem, recv_sem, w_sem, o_sem, x_sem, y_sem, free_sem):
    n_chunks, rows, d_model, q_loc, ff_loc = dims
    blk = rows // 8
    half_d = d_model // 2
    tp = lax.axis_index('tp')
    core = lax.rem(tp, 2)
    xb = lax.rem(lax.div(tp, 2), 2)
    yb = lax.div(tp, 4)
    sib = tp + 1 - 2 * core
    x_nb = tp + 2 - 4 * xb
    y_nb = tp + 4 - 8 * yb
    oc, ox, oy = 1 - core, 1 - xb, 1 - yb
    n_p = 4
    wide = d_model // n_p
    cols = [pl.ds(p * wide, wide) for p in range(n_p)]
    me = core * 4 + xb * 2 + yb

    n_wo = 4
    wo_tile = d_model // n_wo

    def wo_copy(j):
        cs = pl.ds(j * wo_tile, wo_tile)
        return pltpu.make_async_copy(wo_hbm.at[:, cs], w2.at[pl.ds(0, q_loc), cs], o_sem.at[j])

    def x_copy():
        return pltpu.make_async_copy(x_hbm.at[:, me], own, x_sem)

    n_k = 4
    k_rows = ff_loc // n_k

    def w_copy(i, j):
        src, dst = ((w1_hbm, w1), (w3_hbm, w3), (w2_hbm, w2))[i]
        rs = pl.ds(j * k_rows, k_rows)
        return pltpu.make_async_copy(src.at[rs], dst.at[rs], w_sem.at[i, j])

    for j in range(n_wo):
        wo_copy(j).start()
    x_copy().start()

    barrier = pltpu.get_barrier_semaphore()
    for peer in (sib, x_nb, y_nb):
        pl.semaphore_signal(barrier, inc=1, device_id={'tp': peer}, device_id_type=pl.DeviceIdType.MESH)
    for i, g_ref in enumerate((ga_ref, gm_ref)):
        for j in range(d_model // 128):
            gains[i:i + 1, j * 128:(j + 1) * 128] = g_ref[j:j + 1, :].astype(F32)
    pl.semaphore_wait(barrier, 3)

    def xfer(k, c, ph, p):
        odd = p % 2
        cs = cols[p]
        b = buf.at[c]
        if ph == 0:
            src, dst, peer = b.at[oc, :, :, :, cs], r0.at[c, :, :, :, cs], sib
        elif ph == 1:
            src = b.at[core, :, oy, :, cs] if odd else b.at[core, ox, :, :, cs]
            dst, peer = r1.at[c, :, :, cs], (x_nb, y_nb)[odd]
        elif ph == 2:
            src, dst, peer = st.at[c, :, cs], r2.at[c, :, cs], (y_nb, x_nb)[odd]
        else:
            if ph == 3:
                src, peer = b.at[core, xb, yb, :, cs], (y_nb, x_nb)[odd]
            elif ph == 4:
                src = b.at[core, :, yb, :, cs] if odd else b.at[core, xb, :, :, cs]
                peer = (x_nb, y_nb)[odd]
            else:
                src, peer = b.at[core, :, :, :, cs], sib
            dst = src
        return pltpu.make_async_remote_copy(
            src_ref=src, dst_ref=dst, send_sem=send_sem.at[k, c, ph * n_p + p], recv_sem=recv_sem.at[k, c, ph * n_p + p],
            device_id={'tp': peer}, device_id_type=pl.DeviceIdType.MESH)

    def start(k, c, ph, p):
        xfer(k, c, ph, p).start()

    def s1(k, c, p):
        cs = cols[p]
        x = xfer(k, c, 0, p)
        x.wait_recv()
        if p % 2 == 0:
            buf[c, core, ox, :, :, cs] = buf[c, core, ox, :, :, cs] + r0[c, ox, :, :, cs]
            start(k, c, 1, p)
            buf[c, core, xb, :, :, cs] = buf[c, core, xb, :, :, cs] + r0[c, xb, :, :, cs]
        else:
            for i in range(2):
                buf[c, core, i, oy, :, cs] = buf[c, core, i, oy, :, cs] + r0[c, i, oy, :, cs]
            start(k, c, 1, p)
            for i in range(2):
                buf[c, core, i, yb, :, cs] = buf[c, core, i, yb, :, cs] + r0[c, i, yb, :, cs]
        x.wait_send()
        if p == n_p - 1:
            pl.semaphore_signal(free_sem.at[k, c], inc=1, device_id={'tp': sib}, device_id_type=pl.DeviceIdType.MESH)

    def s2(k, c, p):
        cs = cols[p]
        x = xfer(k, c, 1, p)
        x.wait_recv()
        if p % 2 == 0:
            st[c, :, cs] = buf[c, core, xb, oy, :, cs] + r1[c, oy, :, cs]
            start(k, c, 2, p)
            buf[c, core, xb, yb, :, cs] = buf[c, core, xb, yb, :, cs] + r1[c, yb, :, cs]
        else:
            st[c, :, cs] = buf[c, core, ox, yb, :, cs] + r1[c, ox, :, cs]
            start(k, c, 2, p)
            buf[c, core, xb, yb, :, cs] = buf[c, core, xb, yb, :, cs] + r1[c, xb, :, cs]
        x.wait_send()

    v_tile = 256

    def s3(k, c):
        sq = jnp.zeros((blk, v_tile), F32)
        for j in range(d_model // v_tile):
            if j * v_tile % wide == 0:
                xfer(k, c, 2, j * v_tile // wide).wait_recv()
            cs = pl.ds(j * v_tile, v_tile)
            tot = (buf[c, core, xb, yb, :, cs].astype(F32) + r2[c, :, cs].astype(F32)).astype(BF16)
            buf[c, core, xb, yb, :, cs] = tot
            tot = tot.astype(F32)
            sq = sq + tot * tot
        scale = rms_factor(jnp.sum(sq, axis=-1, keepdims=True), d_model)
        for p in range(n_p):
            for j in range(wide // v_tile):
                cs = pl.ds(p * wide + j * v_tile, v_tile)
                res = (own[c, :, cs].astype(F32) + buf[c, core, xb, yb, :, cs].astype(F32) * scale * gains[k:k + 1, cs]).astype(BF16)
                buf[c, core, xb, yb, :, cs] = res
                if k == 0:
                    own[c, :, cs] = res
            start(k, c, 3, p)
        for p in range(n_p):
            xfer(k, c, 2, p).wait_send()

    def g2(k, c, p):
        xfer(k, c, 3, p).wait_recv()
        start(k, c, 4, p)

    def g3(k, c, p):
        xfer(k, c, 4, p).wait_recv()
        if p == 0:
            pl.semaphore_wait(free_sem.at[k, c], 1)
        start(k, c, 5, p)

    def done(k, c):
        for p in range(n_p):
            xfer(k, c, 5, p).wait_recv()
        for ph in range(3, 6):
            for p in range(n_p):
                xfer(k, c, ph, p).wait_send()

    def y_copy(c, p):
        cs = cols[p]
        return pltpu.make_async_copy(buf.at[c, :, :, :, :, cs], y_hbm.at[c, :, :, :, :, cs], y_sem.at[c, p])

    def fin(k, c):
        for p in range(n_p):
            xfer(k, c, 5, p).wait_recv()
            y_copy(c, p).start()
        for ph in range(3, 6):
            for p in range(n_p):
                xfer(k, c, ph, p).wait_send()

    def both(fn, k, c):
        for p in range(n_p):
            fn(k, c, p)

    def p1(c):
        for p in range(n_p):
            if c == 0:
                wo_copy(p).wait()
            acc = jnp.dot(o_ref[c], w2[0:q_loc, cols[p]], preferred_element_type=F32)
            buf[c, :, :, :, :, cols[p]] = acc.astype(BF16).reshape(2, 2, 2, blk, wide)
            start(0, c, 0, p)

    gu_tile = 256
    gu_tiles = [(f, min(gu_tile, ff_loc - f)) for f in range(0, ff_loc, gu_tile)]

    def dot_t(w_rows, h):
        return lax.dot_general(w_rows, h, (((1,), (1,)), ((), ())), preferred_element_type=F32)

    def p2(services):
        def chunk(c, carry):
            def serve(point):
                for (sc, sp), fns in services.items():
                    if sp == point:
                        @pl.when(c == sc)
                        def _(fns=fns):
                            for fn in fns:
                                fn()

            for j, (f0, fw) in enumerate(gu_tiles):
                serve(j)
                h = buf[c].reshape(rows, d_model)
                g = dot_t(w1[f0:f0 + fw, :], h)
                up = dot_t(w3[f0:f0 + fw, :], h)
                act[:, f0:f0 + fw] = jnp.transpose(g * jax.nn.sigmoid(g) * up).astype(BF16)

            base = len(gu_tiles)

            def down(cs):
                acc = jnp.dot(act[...], w2[:, cs], preferred_element_type=F32)
                buf[c, :, :, :, :, cs] = acc.astype(BF16).reshape(2, 2, 2, blk, half_d)
            for ab in range(2):
                serve(base + ab)
                down(pl.ds(ab * half_d, half_d))
                start(1, c, 0, 2 * ab)
                start(1, c, 0, 2 * ab + 1)
            return carry
        lax.fori_loop(0, n_chunks, chunk, 0)

    p1(0)
    for j in range(n_k):
        for i in range(2):
            w_copy(i, j).start()
    both(s1, 0, 0)
    p1(1)
    p1(2)
    for j in range(n_k):
        w_copy(2, j).start()
    both(s2, 0, 0)
    both(s1, 0, 1)
    x_copy().wait()
    s3(0, 0)
    both(s2, 0, 1)
    both(g2, 0, 0)
    s3(0, 1)
    both(s1, 0, 2)
    both(g3, 0, 0)
    for j in range(n_k):
        for i in range(3):
            w_copy(i, j).wait()
    done(0, 0)

    F = functools.partial
    p2({
        (0, 0): [F(both, g2, 0, 1)],
        (0, 2): [F(both, s2, 0, 2)],
        (0, 5): [F(both, g3, 0, 1)],
        (0, 6): [F(s3, 0, 2)],
        (1, 0): [F(done, 0, 1), F(both, g2, 0, 2)],
        (1, 1): [F(both, s1, 1, 0)],
        (1, 4): [F(both, g3, 0, 2)],
        (1, 6): [F(both, s2, 1, 0)],
        (2, 0): [F(done, 0, 2), F(s3, 1, 0)],
        (2, 1): [F(both, s1, 1, 1)],
        (2, 3): [F(both, g2, 1, 0)],
        (2, 5): [F(both, s2, 1, 1)],
        (2, 7): [F(both, g3, 1, 0)],
    })
    both(s1, 1, 2)
    s3(1, 1)
    both(s2, 1, 2)
    both(g2, 1, 1)
    s3(1, 2)
    both(g3, 1, 1)
    both(g2, 1, 2)
    fin(1, 0)
    fin(1, 1)
    both(g3, 1, 2)
    fin(1, 2)
    for c in range(n_chunks):
        for p in range(n_p):
            y_copy(c, p).wait()


def tail(o, x_seq, w_o, w1, w3, w2, g_attn, g_mlp):
    n_chunks, rows, d_model = x_seq.shape
    q_loc = o.shape[-1]
    ff_loc = w2.shape[0]
    blk = rows // 8
    dims = (n_chunks, rows, d_model, q_loc, ff_loc)
    vmem = pl.BlockSpec(memory_space=pltpu.VMEM)
    hbm = pl.BlockSpec(memory_space=pl.ANY)
    y = pl.pallas_call(
        functools.partial(tail_kernel, dims),
        name='tail',
        out_shape=jax.ShapeDtypeStruct((n_chunks, 2, 2, 2, blk, d_model), BF16),
        in_specs=[vmem, vmem, vmem, hbm, hbm, hbm, hbm, hbm],
        out_specs=hbm,
        scratch_shapes=[
            pltpu.VMEM((n_chunks, 2, 2, 2, blk, d_model), BF16),
            pltpu.VMEM((n_chunks, 2, 2, blk, d_model), BF16),
            pltpu.VMEM((n_chunks, 2, blk, d_model), BF16),
            pltpu.VMEM((n_chunks, blk, d_model), BF16),
            pltpu.VMEM((n_chunks, blk, d_model), BF16),
            pltpu.VMEM((n_chunks, blk, d_model), BF16),
            pltpu.VMEM((rows, ff_loc), BF16),
            pltpu.VMEM((2, d_model), F32),
            pltpu.VMEM((ff_loc, d_model), BF16),
            pltpu.VMEM((ff_loc, d_model), BF16),
            pltpu.VMEM((ff_loc, d_model), BF16),
            pltpu.SemaphoreType.DMA((2, n_chunks, 24)),
            pltpu.SemaphoreType.DMA((2, n_chunks, 24)),
            pltpu.SemaphoreType.DMA((3, 4)),
            pltpu.SemaphoreType.DMA((4,)),
            pltpu.SemaphoreType.DMA,
            pltpu.SemaphoreType.DMA((n_chunks, 4)),
            pltpu.SemaphoreType.REGULAR((2, n_chunks)),
        ],
        compiler_params=pltpu.CompilerParams(collective_id=1, has_side_effects=True, vmem_limit_bytes=67043328),
    )(o, g_attn.reshape(-1, 128), g_mlp.reshape(-1, 128), x_seq.reshape(n_chunks, 8, blk, d_model), w_o, w1.T, w3.T, w2)
    return y.reshape(n_chunks, rows, d_model)


def head_kernel(dims, len_ref, gq_ref, gk_ref, freq_ref, x_hbm, wq_hbm, wk_hbm, wv_hbm, q_out, k_out, v_out,
                x, w, raw, cos_t, sin_t, sums, x_sem, w_sem, send_sem, recv_sem):
    n_steps, rows, d_model, q_loc, hd, n_tp = dims
    heads = q_loc // hd
    width = q_loc + 2 * hd
    tp = lax.axis_index('tp')

    def x_copy(t):
        return pltpu.make_async_copy(x_hbm.at[t], x.at[t], x_sem.at[t])

    n_k = 4
    k_rows = d_model // n_k

    def w_copies(j):
        rs = pl.ds(j * k_rows, k_rows)
        return (pltpu.make_async_copy(wq_hbm.at[rs], w.at[rs, pl.ds(0, q_loc)], w_sem.at[0, j]),
                pltpu.make_async_copy(wk_hbm.at[rs], w.at[rs, pl.ds(q_loc, hd)], w_sem.at[1, j]),
                pltpu.make_async_copy(wv_hbm.at[rs], w.at[rs, pl.ds(q_loc + hd, hd)], w_sem.at[2, j]))

    x_copy(0).start()
    for j in range(n_k):
        for cp in w_copies(j):
            cp.start()
    for t in range(1, n_steps):
        x_copy(t).start()

    barrier = pltpu.get_barrier_semaphore()
    peers = [lax.rem(tp + d, n_tp) for d in range(1, n_tp)]
    for p in peers:
        pl.semaphore_signal(barrier, inc=1, device_id={'tp': p}, device_id_type=pl.DeviceIdType.MESH)

    lens = jnp.transpose(jnp.broadcast_to(len_ref[...].astype(F32), (rows, rows)))
    lane = lax.broadcasted_iota(jnp.int32, (rows, hd), 1)
    sign = jnp.where(lane < hd // 2, -1.0, 1.0).astype(F32)
    for t in range(n_steps):
        ang = (lens + float(t)) * freq_ref[...]
        cos_t[t] = jnp.cos(ang)
        sin_t[t] = jnp.sin(ang) * sign

    sq_lane = lax.broadcasted_iota(jnp.int32, (rows, rows), 1)

    def send(t, d):
        return pltpu.make_async_remote_copy(
            src_ref=sums.at[t, tp], dst_ref=sums.at[t, tp], send_sem=send_sem.at[t, d], recv_sem=recv_sem.at[t, d],
            device_id={'tp': peers[d]}, device_id_type=pl.DeviceIdType.MESH)

    def project(t):
        x_copy(t).wait()
        if t == 0:
            res = jnp.zeros((rows, q_loc + hd), F32)
            for j in range(n_k):
                for cp in w_copies(j)[:2]:
                    cp.wait()
                ks = slice(j * k_rows, (j + 1) * k_rows)
                res = res + jnp.dot(x[t, :, ks], w[ks, 0:q_loc + hd], preferred_element_type=F32)
            res = res.astype(BF16)
        else:
            res = jnp.dot(x[t], w[:, 0:q_loc + hd], preferred_element_type=F32).astype(BF16)
        raw[t] = res
        q = res[:, :q_loc].astype(F32)
        k = res[:, q_loc:q_loc + hd].astype(F32)
        part = jnp.where(sq_lane == 0, jnp.sum(q * q, axis=-1, keepdims=True), jnp.sum(k * k, axis=-1, keepdims=True))
        sums[t, tp] = jnp.transpose(part)[0:8]
        if t == 0:
            pl.semaphore_wait(barrier, n_tp - 1)
        for d in range(n_tp - 1):
            send(t, d).start()

    def rotate_all(t):
        for d in range(n_tp - 1):
            send(t, d).wait()
        tot = sums[t, 0]
        for d in range(1, n_tp):
            tot = tot + sums[t, d]
        full = jnp.transpose(jnp.concatenate([tot, jnp.zeros((rows - 8, rows), F32)], axis=0))
        q_scale = rms_factor(full[:, 0:1], q_loc * n_tp)
        k_scale = rms_factor(full[:, 1:2], hd * n_tp)

        def rotate(col, scale, gain):
            val = raw[t, :, col:col + hd].astype(F32) * scale * gain.astype(F32)
            return (val * cos_t[t] + pltpu.roll(val, hd // 2, 1) * sin_t[t]).astype(BF16).astype(F32)
        for j in range(heads):
            q_out[pl.ds(t * heads + j, rows, stride=16), :] = rotate(j * hd, q_scale, gq_ref[j:j + 1, :])
        k_out[t] = rotate(q_loc, k_scale, gk_ref[...])

    for t in range(n_steps):
        project(t)
    for j in range(n_k):
        w_copies(j)[2].wait()
    for t in range(n_steps):
        v_out[t] = jnp.dot(x[t], w[:, q_loc + hd:width], preferred_element_type=F32).astype(BF16).astype(F32)
    q_out[pl.ds(n_steps * heads, rows, stride=16), :] = jnp.zeros((rows, hd), F32)
    for t in range(n_steps):
        rotate_all(t)


def head(x_seq, cache_len, w_q, w_k, w_v, g_q, g_k, n_tp):
    n_steps, rows, d_model = x_seq.shape
    q_loc, hd = w_q.shape[1], w_k.shape[1]
    width = q_loc + 2 * hd
    half = hd // 2
    inv_freq = np.float32(ROPE_THETA) ** (-(np.arange(half, dtype=np.float32) * np.float32(2.0 / hd)))
    freq = jnp.asarray(np.concatenate([inv_freq, inv_freq]).reshape(1, hd), F32)
    vmem = pl.BlockSpec(memory_space=pltpu.VMEM)
    hbm = pl.BlockSpec(memory_space=pl.ANY)
    return pl.pallas_call(
        functools.partial(head_kernel, (n_steps, rows, d_model, q_loc, hd, n_tp)),
        name='head',
        out_shape=(jax.ShapeDtypeStruct((rows * 16, hd), F32),
                   jax.ShapeDtypeStruct((n_steps, rows, hd), F32),
                   jax.ShapeDtypeStruct((n_steps, rows, hd), F32)),
        in_specs=[vmem] * 4 + [hbm] * 4,
        out_specs=(vmem,) * 3,
        scratch_shapes=[
            pltpu.VMEM((n_steps, rows, d_model), BF16),
            pltpu.VMEM((d_model, width), BF16),
            pltpu.VMEM((n_steps, rows, q_loc + hd), BF16),
            pltpu.VMEM((n_steps, rows, hd), F32),
            pltpu.VMEM((n_steps, rows, hd), F32),
            pltpu.VMEM((n_steps, n_tp, 8, rows), F32),
            pltpu.SemaphoreType.DMA((n_steps,)),
            pltpu.SemaphoreType.DMA((3, 4)),
            pltpu.SemaphoreType.DMA((n_steps, n_tp - 1)),
            pltpu.SemaphoreType.DMA((n_steps, n_tp - 1)),
        ],
        compiler_params=pltpu.CompilerParams(collective_id=0, has_side_effects=True, vmem_limit_bytes=67043328),
    )(cache_len.reshape(1, -1), g_q.reshape(-1, hd), g_k.reshape(1, -1), freq, x_seq, w_q, w_k, w_v)


def attn_kernel(dims, len_ref, q_hbm, kn_hbm, vn_hbm, k_hbm, v_hbm, o_hbm, ko_hbm, vo_hbm,
                kb, vb, q, kn, vn, s_scr, e_scr, l_scr, o_scr, o_buf, n_sem, in_sem, out_sem, o_sem):
    n_steps, nb, heads, hd, seq_max, n_rows = dims
    n_blocks = n_rows // nb
    win = 32
    row_step = lax.broadcasted_iota(jnp.int32, (16, seq_max), 0) // heads
    col = lax.broadcasted_iota(jnp.int32, (16, seq_max), 1)
    ahead = col - row_step
    win_row = lax.broadcasted_iota(jnp.int32, (win, hd), 0)
    small = [pltpu.make_async_copy(src, dst, n_sem.at[i])
             for i, (src, dst) in enumerate(((kn_hbm, kn), (vn_hbm, vn), (q_hbm, q)))]

    def load(i, blk):
        src, dst = ((k_hbm, kb), (v_hbm, vb))[i]
        rs = pl.ds(blk * nb, nb)
        return pltpu.make_async_copy(src.at[rs], dst.at[rs], in_sem.at[i, blk])

    def store(i, blk):
        src, dst = ((kb, ko_hbm), (vb, vo_hbm))[i]
        rs = pl.ds(blk * nb, nb)
        return pltpu.make_async_copy(src.at[rs], dst.at[rs], out_sem.at[i, blk])

    def o_store(blk):
        rs = pl.ds(blk * nb, nb)
        return pltpu.make_async_copy(o_buf.at[:, rs], o_hbm.at[:, rs], o_sem.at[blk])

    small[0].start()
    load(0, 0).start()
    for cp in small[1:]:
        cp.start()
    load(1, 0).start()
    for blk in range(1, n_blocks):
        for i in range(2):
            load(i, blk).start()
    small[0].wait()

    def block(blk, carry):
        first = blk * nb
        for j, (buf, new) in enumerate(((kb, kn), (vb, vn))):
            load(j, blk).wait()
            if j == 1:
                @pl.when(blk == 0)
                def _():
                    for cp in small[1:]:
                        cp.wait()
            new_rows = [new[t, pl.ds(pl.multiple_of(first, nb), nb), :] for t in range(n_steps)]
            for i in range(nb):
                ln = len_ref[first + i]
                base = pl.multiple_of(jnp.minimum((ln // 16) * 16, seq_max - win), 16)
                rel = win_row + (base - ln)
                cut = buf[first + i, pl.ds(base, win), :].astype(F32)
                for t in range(n_steps):
                    cut = jnp.where(rel == t, new_rows[t][i:i + 1, :], cut)
                buf[first + i, pl.ds(base, win), :] = cut.astype(BF16)
            store(j, blk).start()
        for i in range(nb):
            s = lax.dot_general(q[first + i].astype(BF16), kb[first + i], (((1,), (1,)), ((), ())), preferred_element_type=F32) * hd ** -0.5
            s_scr[i * 16:(i + 1) * 16, :] = jnp.where(ahead <= len_ref[first + i], s, -jnp.inf)
        for i in range(0, nb, 2):
            rs = slice(i * 16, (i + 2) * 16)
            s = s_scr[rs, :]
            e = jnp.exp(s - jnp.max(s, axis=-1, keepdims=True))
            l_scr[rs, :] = jnp.broadcast_to(jnp.sum(e, axis=-1, keepdims=True), (32, hd))
            e_scr[rs, :] = e.astype(BF16)
        for i in range(nb):
            rs = slice(i * 16, (i + 1) * 16)
            o_scr[rs, :] = jnp.dot(e_scr[rs, :], vb[first + i], preferred_element_type=F32)
        o_scr[...] = o_scr[...] / l_scr[...]
        for t in range(n_steps):
            for j in range(heads):
                o_buf[t, pl.ds(pl.multiple_of(first, nb), nb), j * hd:(j + 1) * hd] = o_scr[pl.ds(t * heads + j, nb, stride=16), :].astype(BF16)
        o_store(blk).start()
        return carry
    lax.fori_loop(0, n_blocks, block, 0)
    for blk in range(n_blocks):
        for i in range(2):
            store(i, blk).wait()
        o_store(blk).wait()


def attend(q, kn, vn, k_cache, v_cache, cache_len, heads):
    n_rows, _, seq_max, hd = k_cache.shape
    n_steps = kn.shape[0]
    nb = 32
    hbm = pl.BlockSpec(memory_space=pl.ANY)
    cache_shape = jax.ShapeDtypeStruct((n_rows, seq_max, hd), BF16)
    flops = 4 * n_rows * 16 * seq_max * hd
    return pl.pallas_call(
        functools.partial(attn_kernel, (n_steps, nb, heads, hd, seq_max, n_rows)),
        name='attend',
        in_specs=[pl.BlockSpec(memory_space=pltpu.SMEM)] + [hbm] * 5,
        out_specs=(hbm, hbm, hbm),
        scratch_shapes=[
            pltpu.VMEM((n_rows, seq_max, hd), BF16),
            pltpu.VMEM((n_rows, seq_max, hd), BF16),
            pltpu.VMEM((n_rows, 16, hd), F32),
            pltpu.VMEM((n_steps, n_rows, hd), F32),
            pltpu.VMEM((n_steps, n_rows, hd), F32),
            pltpu.VMEM((nb * 16, seq_max), F32),
            pltpu.VMEM((nb * 16, seq_max), BF16),
            pltpu.VMEM((nb * 16, hd), F32),
            pltpu.VMEM((nb * 16, hd), F32),
            pltpu.VMEM((n_steps, n_rows, heads * hd), BF16),
            pltpu.SemaphoreType.DMA((3,)),
            pltpu.SemaphoreType.DMA((2, n_rows // nb)),
            pltpu.SemaphoreType.DMA((2, n_rows // nb)),
            pltpu.SemaphoreType.DMA((n_rows // nb,)),
        ],
        out_shape=(jax.ShapeDtypeStruct((n_steps, n_rows, heads * hd), BF16), cache_shape, cache_shape),
        compiler_params=pltpu.CompilerParams(vmem_limit_bytes=67043328),
        cost_estimate=pl.CostEstimate(flops=flops, bytes_accessed=4 * n_rows * seq_max * hd * 2, transcendentals=n_rows * 16 * seq_max),
    )(cache_len, q.reshape(n_rows, 16, hd), kn, vn, k_cache[:, 0], v_cache[:, 0])


def finish_kernel(n, src, dst, buf, in_sem, out_sem):
    ins = [pltpu.make_async_copy(src.at[i], buf.at[i], in_sem.at[i]) for i in range(n)]
    outs = [pltpu.make_async_copy(buf.at[i], dst.at[i], out_sem.at[i]) for i in range(n)]
    for cp in ins:
        cp.start()
    for a, b in zip(ins, outs):
        a.wait()
        b.start()
    for cp in outs:
        cp.wait()


def finish(y):
    n_steps, rows, d_model = y.shape
    n = 4 * n_steps
    shape = (n, n_steps * rows // n, d_model)
    hbm = pl.BlockSpec(memory_space=pl.ANY)
    out = pl.pallas_call(
        functools.partial(finish_kernel, n),
        name='finish',
        in_specs=[hbm],
        out_specs=hbm,
        scratch_shapes=[pltpu.VMEM(shape, BF16), pltpu.SemaphoreType.DMA((n,)), pltpu.SemaphoreType.DMA((n,))],
        out_shape=jax.ShapeDtypeStruct(shape, BF16),
        compiler_params=pltpu.CompilerParams(vmem_limit_bytes=67043328),
    )(y.reshape(shape))
    return out.reshape(y.shape)


def local_layer(n_tp, x_seq, cache_len, k_cache, v_cache, w_q, w_k, w_v, w_o, w_gate, w_up, w_down, g_q, g_k, g_attn, g_mlp):
    heads = w_q.shape[1] // k_cache.shape[3]
    q, kn, vn = head(x_seq, cache_len, w_q, w_k, w_v, g_q, g_k, n_tp)
    o, k_out, v_out = attend(q, kn, vn, k_cache, v_cache, cache_len, heads)
    y = tail(o, x_seq, w_o, w_gate, w_up, w_down, g_attn, g_mlp)
    return finish(y), k_out[:, None], v_out[:, None]


def solution(mesh):
    tp_size = mesh.shape['tp']
    data_spec = P(None, 'dp', None)
    cache_spec = P('dp', 'tp', None, None)
    col_spec = P(None, 'tp')
    row_spec = P('tp', None)
    arg_specs = (data_spec, P('dp'), cache_spec, cache_spec, col_spec, col_spec, col_spec, row_spec, col_spec, col_spec, row_spec, P('tp'), P('tp'), P(None), P(None))
    out_specs = (data_spec, cache_spec, cache_spec)
    return jax.shard_map(functools.partial(local_layer, tp_size), mesh=mesh, in_specs=arg_specs, out_specs=out_specs, check_vma=False)
```

```python
import functools

import jax
import jax.numpy as jnp
import numpy as np
from jax import lax
from jax.experimental import pallas as pl
from jax.experimental.pallas import tpu as pltpu
from jax.sharding import PartitionSpec as P

ROPE_THETA = 500000.0
NORM_EPS = 1e-6
F32 = jnp.float32
BF16 = jnp.bfloat16


def rms_factor(sq_sum, full_width):
    return lax.rsqrt(sq_sum / full_width + NORM_EPS)


def tail_kernel(dims, o_ref, ga_ref, gm_ref, x_hbm, wo_hbm, w1_hbm, w3_hbm, w2_hbm, y_hbm,
                buf, r0, r1, r2, st, own, act, gains, w1, w3, w2,
                send_sem, recv_sem, w_sem, o_sem, x_sem, y_sem, free_sem):
    n_chunks, rows, d_model, q_loc, ff_loc = dims
    blk = rows // 8
    half_d = d_model // 2
    tp = lax.axis_index('tp')
    core = lax.rem(tp, 2)
    xb = lax.rem(lax.div(tp, 2), 2)
    yb = lax.div(tp, 4)
    sib = tp + 1 - 2 * core
    x_nb = tp + 2 - 4 * xb
    y_nb = tp + 4 - 8 * yb
    oc, ox, oy = 1 - core, 1 - xb, 1 - yb
    n_p = 4
    wide = d_model // n_p
    cols = [pl.ds(p * wide, wide) for p in range(n_p)]
    me = core * 4 + xb * 2 + yb

    n_wo = 4
    wo_tile = d_model // n_wo

    def wo_copy(j):
        cs = pl.ds(j * wo_tile, wo_tile)
        return pltpu.make_async_copy(wo_hbm.at[:, cs], w2.at[pl.ds(0, q_loc), cs], o_sem.at[j])

    def x_copy():
        return pltpu.make_async_copy(x_hbm.at[:, me], own, x_sem)

    n_k = 4
    k_rows = ff_loc // n_k

    def w_copy(i, j):
        src, dst = ((w1_hbm, w1), (w3_hbm, w3), (w2_hbm, w2))[i]
        rs = pl.ds(j * k_rows, k_rows)
        return pltpu.make_async_copy(src.at[rs], dst.at[rs], w_sem.at[i, j])

    for j in range(n_wo):
        wo_copy(j).start()
    x_copy().start()

    barrier = pltpu.get_barrier_semaphore()
    for peer in (sib, x_nb, y_nb):
        pl.semaphore_signal(barrier, inc=1, device_id={'tp': peer}, device_id_type=pl.DeviceIdType.MESH)
    for i, g_ref in enumerate((ga_ref, gm_ref)):
        for j in range(d_model // 128):
            gains[i:i + 1, j * 128:(j + 1) * 128] = g_ref[j:j + 1, :].astype(F32)
    pl.semaphore_wait(barrier, 3)

    def xfer(k, c, ph, p):
        odd = p % 2
        cs = cols[p]
        b = buf.at[c]
        if ph == 0:
            src, dst, peer = b.at[oc, :, :, :, cs], r0.at[c, :, :, :, cs], sib
        elif ph == 1:
            src = b.at[core, :, oy, :, cs] if odd else b.at[core, ox, :, :, cs]
            dst, peer = r1.at[c, :, :, cs], (x_nb, y_nb)[odd]
        elif ph == 2:
            src, dst, peer = st.at[c, :, cs], r2.at[c, :, cs], (y_nb, x_nb)[odd]
        else:
            if ph == 3:
                src, peer = b.at[core, xb, yb, :, cs], (y_nb, x_nb)[odd]
            elif ph == 4:
                src = b.at[core, :, yb, :, cs] if odd else b.at[core, xb, :, :, cs]
                peer = (x_nb, y_nb)[odd]
            else:
                src, peer = b.at[core, :, :, :, cs], sib
            dst = src
        return pltpu.make_async_remote_copy(
            src_ref=src, dst_ref=dst, send_sem=send_sem.at[k, c, ph * n_p + p], recv_sem=recv_sem.at[k, c, ph * n_p + p],
            device_id={'tp': peer}, device_id_type=pl.DeviceIdType.MESH)

    def start(k, c, ph, p):
        xfer(k, c, ph, p).start()

    def s1(k, c, p):
        cs = cols[p]
        x = xfer(k, c, 0, p)
        x.wait_recv()
        if p % 2 == 0:
            buf[c, core, ox, :, :, cs] = buf[c, core, ox, :, :, cs] + r0[c, ox, :, :, cs]
            start(k, c, 1, p)
            buf[c, core, xb, :, :, cs] = buf[c, core, xb, :, :, cs] + r0[c, xb, :, :, cs]
        else:
            for i in range(2):
                buf[c, core, i, oy, :, cs] = buf[c, core, i, oy, :, cs] + r0[c, i, oy, :, cs]
            start(k, c, 1, p)
            for i in range(2):
                buf[c, core, i, yb, :, cs] = buf[c, core, i, yb, :, cs] + r0[c, i, yb, :, cs]
        x.wait_send()
        if p == n_p - 1:
            pl.semaphore_signal(free_sem.at[k, c], inc=1, device_id={'tp': sib}, device_id_type=pl.DeviceIdType.MESH)

    def s2(k, c, p):
        cs = cols[p]
        x = xfer(k, c, 1, p)
        x.wait_recv()
        if p % 2 == 0:
            st[c, :, cs] = buf[c, core, xb, oy, :, cs] + r1[c, oy, :, cs]
            start(k, c, 2, p)
            buf[c, core, xb, yb, :, cs] = buf[c, core, xb, yb, :, cs] + r1[c, yb, :, cs]
        else:
            st[c, :, cs] = buf[c, core, ox, yb, :, cs] + r1[c, ox, :, cs]
            start(k, c, 2, p)
            buf[c, core, xb, yb, :, cs] = buf[c, core, xb, yb, :, cs] + r1[c, xb, :, cs]
        x.wait_send()

    v_tile = 256

    def s3(k, c):
        sq = jnp.zeros((blk, v_tile), F32)
        for j in range(d_model // v_tile):
            if j * v_tile % wide == 0:
                xfer(k, c, 2, j * v_tile // wide).wait_recv()
            cs = pl.ds(j * v_tile, v_tile)
            tot = (buf[c, core, xb, yb, :, cs].astype(F32) + r2[c, :, cs].astype(F32)).astype(BF16)
            buf[c, core, xb, yb, :, cs] = tot
            tot = tot.astype(F32)
            sq = sq + tot * tot
        scale = rms_factor(jnp.sum(sq, axis=-1, keepdims=True), d_model)
        for p in range(n_p):
            for j in range(wide // v_tile):
                cs = pl.ds(p * wide + j * v_tile, v_tile)
                res = (own[c, :, cs].astype(F32) + buf[c, core, xb, yb, :, cs].astype(F32) * scale * gains[k:k + 1, cs]).astype(BF16)
                buf[c, core, xb, yb, :, cs] = res
                if k == 0:
                    own[c, :, cs] = res
            start(k, c, 3, p)
        for p in range(n_p):
            xfer(k, c, 2, p).wait_send()

    def g2(k, c, p):
        xfer(k, c, 3, p).wait_recv()
        start(k, c, 4, p)

    def g3(k, c, p):
        xfer(k, c, 4, p).wait_recv()
        if p == 0:
            pl.semaphore_wait(free_sem.at[k, c], 1)
        start(k, c, 5, p)

    def done(k, c):
        for p in range(n_p):
            xfer(k, c, 5, p).wait_recv()
        for ph in range(3, 6):
            for p in range(n_p):
                xfer(k, c, ph, p).wait_send()

    def y_copy(c, p):
        cs = cols[p]
        return pltpu.make_async_copy(buf.at[c, :, :, :, :, cs], y_hbm.at[c, :, :, :, :, cs], y_sem.at[c, p])

    def fin(k, c):
        for p in range(n_p):
            xfer(k, c, 5, p).wait_recv()
            y_copy(c, p).start()
        for ph in range(3, 6):
            for p in range(n_p):
                xfer(k, c, ph, p).wait_send()

    def both(fn, k, c):
        for p in range(n_p):
            fn(k, c, p)

    def p1(c):
        for p in range(n_p):
            if c == 0:
                wo_copy(p).wait()
            acc = jnp.dot(o_ref[c], w2[0:q_loc, cols[p]], preferred_element_type=F32)
            buf[c, :, :, :, :, cols[p]] = acc.astype(BF16).reshape(2, 2, 2, blk, wide)
            start(0, c, 0, p)

    gu_tile = 256
    gu_tiles = [(f, min(gu_tile, ff_loc - f)) for f in range(0, ff_loc, gu_tile)]

    def dot_t(w_rows, h):
        return lax.dot_general(w_rows, h, (((1,), (1,)), ((), ())), preferred_element_type=F32)

    def p2(services):
        def chunk(c, carry):
            def serve(point):
                for (sc, sp), fns in services.items():
                    if sp == point:
                        @pl.when(c == sc)
                        def _(fns=fns):
                            for fn in fns:
                                fn()

            for j, (f0, fw) in enumerate(gu_tiles):
                serve(j)
                h = buf[c].reshape(rows, d_model)
                g = dot_t(w1[f0:f0 + fw, :], h)
                up = dot_t(w3[f0:f0 + fw, :], h)
                act[:, f0:f0 + fw] = jnp.transpose(g * jax.nn.sigmoid(g) * up).astype(BF16)

            base = len(gu_tiles)

            def down(cs):
                acc = jnp.dot(act[...], w2[:, cs], preferred_element_type=F32)
                buf[c, :, :, :, :, cs] = acc.astype(BF16).reshape(2, 2, 2, blk, half_d)
            for ab in range(2):
                serve(base + ab)
                down(pl.ds(ab * half_d, half_d))
                start(1, c, 0, 2 * ab)
                start(1, c, 0, 2 * ab + 1)
            return carry
        lax.fori_loop(0, n_chunks, chunk, 0)

    p1(0)
    for j in range(n_k):
        for i in range(2):
            w_copy(i, j).start()
    both(s1, 0, 0)
    p1(1)
    p1(2)
    for j in range(n_k):
        w_copy(2, j).start()
    both(s2, 0, 0)
    both(s1, 0, 1)
    x_copy().wait()
    s3(0, 0)
    both(s2, 0, 1)
    both(g2, 0, 0)
    s3(0, 1)
    both(s1, 0, 2)
    both(g3, 0, 0)
    for j in range(n_k):
        for i in range(3):
            w_copy(i, j).wait()
    done(0, 0)

    F = functools.partial
    p2({
        (0, 0): [F(both, g2, 0, 1)],
        (0, 2): [F(both, s2, 0, 2)],
        (0, 5): [F(both, g3, 0, 1)],
        (0, 6): [F(s3, 0, 2)],
        (1, 0): [F(done, 0, 1), F(both, g2, 0, 2)],
        (1, 1): [F(both, s1, 1, 0)],
        (1, 6): [F(both, s2, 1, 0)],
        (2, 0): [F(done, 0, 2), F(s3, 1, 0)],
        (2, 1): [F(both, s1, 1, 1)],
        (2, 3): [F(both, g2, 1, 0)],
        (2, 5): [F(both, s2, 1, 1)],
        (2, 7): [F(both, g3, 1, 0)],
        (2, 8): [F(s3, 1, 1)],
        (1, 5): [F(both, g3, 0, 2)],
    })
    both(s1, 1, 2)
    both(s2, 1, 2)
    both(g2, 1, 1)
    s3(1, 2)
    both(g3, 1, 1)
    both(g2, 1, 2)
    fin(1, 0)
    fin(1, 1)
    both(g3, 1, 2)
    fin(1, 2)
    for c in range(n_chunks):
        for p in range(n_p):
            y_copy(c, p).wait()


def tail(o, x_seq, w_o, w1, w3, w2, g_attn, g_mlp):
    n_chunks, rows, d_model = x_seq.shape
    q_loc = o.shape[-1]
    ff_loc = w2.shape[0]
    blk = rows // 8
    dims = (n_chunks, rows, d_model, q_loc, ff_loc)
    vmem = pl.BlockSpec(memory_space=pltpu.VMEM)
    hbm = pl.BlockSpec(memory_space=pl.ANY)
    y = pl.pallas_call(
        functools.partial(tail_kernel, dims),
        name='tail',
        out_shape=jax.ShapeDtypeStruct((n_chunks, 2, 2, 2, blk, d_model), BF16),
        in_specs=[vmem, vmem, vmem, hbm, hbm, hbm, hbm, hbm],
        out_specs=hbm,
        scratch_shapes=[
            pltpu.VMEM((n_chunks, 2, 2, 2, blk, d_model), BF16),
            pltpu.VMEM((n_chunks, 2, 2, blk, d_model), BF16),
            pltpu.VMEM((n_chunks, 2, blk, d_model), BF16),
            pltpu.VMEM((n_chunks, blk, d_model), BF16),
            pltpu.VMEM((n_chunks, blk, d_model), BF16),
            pltpu.VMEM((n_chunks, blk, d_model), BF16),
            pltpu.VMEM((rows, ff_loc), BF16),
            pltpu.VMEM((2, d_model), F32),
            pltpu.VMEM((ff_loc, d_model), BF16),
            pltpu.VMEM((ff_loc, d_model), BF16),
            pltpu.VMEM((ff_loc, d_model), BF16),
            pltpu.SemaphoreType.DMA((2, n_chunks, 24)),
            pltpu.SemaphoreType.DMA((2, n_chunks, 24)),
            pltpu.SemaphoreType.DMA((3, 4)),
            pltpu.SemaphoreType.DMA((4,)),
            pltpu.SemaphoreType.DMA,
            pltpu.SemaphoreType.DMA((n_chunks, 4)),
            pltpu.SemaphoreType.REGULAR((2, n_chunks)),
        ],
        compiler_params=pltpu.CompilerParams(collective_id=1, has_side_effects=True, vmem_limit_bytes=67043328),
    )(o, g_attn.reshape(-1, 128), g_mlp.reshape(-1, 128), x_seq.reshape(n_chunks, 8, blk, d_model), w_o, w1.T, w3.T, w2)
    return y.reshape(n_chunks, rows, d_model)


def head_kernel(dims, len_ref, gq_ref, gk_ref, freq_ref, x_hbm, wq_hbm, wk_hbm, wv_hbm, q_out, k_out, v_out,
                x, w, raw, cos_t, sin_t, sums, x_sem, w_sem, send_sem, recv_sem):
    n_steps, rows, d_model, q_loc, hd, n_tp = dims
    heads = q_loc // hd
    width = q_loc + 2 * hd
    tp = lax.axis_index('tp')

    def x_copy(t):
        return pltpu.make_async_copy(x_hbm.at[t], x.at[t], x_sem.at[t])

    n_k = 4
    k_rows = d_model // n_k

    def w_copies(j):
        rs = pl.ds(j * k_rows, k_rows)
        return (pltpu.make_async_copy(wq_hbm.at[rs], w.at[rs, pl.ds(0, q_loc)], w_sem.at[0, j]),
                pltpu.make_async_copy(wk_hbm.at[rs], w.at[rs, pl.ds(q_loc, hd)], w_sem.at[1, j]),
                pltpu.make_async_copy(wv_hbm.at[rs], w.at[rs, pl.ds(q_loc + hd, hd)], w_sem.at[2, j]))

    x_copy(0).start()
    for j in range(n_k):
        for cp in w_copies(j):
            cp.start()
    for t in range(1, n_steps):
        x_copy(t).start()

    barrier = pltpu.get_barrier_semaphore()
    peers = [lax.rem(tp + d, n_tp) for d in range(1, n_tp)]
    for p in peers:
        pl.semaphore_signal(barrier, inc=1, device_id={'tp': p}, device_id_type=pl.DeviceIdType.MESH)

    lens = jnp.transpose(jnp.broadcast_to(len_ref[...].astype(F32), (rows, rows)))
    lane = lax.broadcasted_iota(jnp.int32, (rows, hd), 1)
    sign = jnp.where(lane < hd // 2, -1.0, 1.0).astype(F32)
    for t in range(n_steps):
        ang = (lens + float(t)) * freq_ref[...]
        cos_t[t] = jnp.cos(ang)
        sin_t[t] = jnp.sin(ang) * sign

    sq_lane = lax.broadcasted_iota(jnp.int32, (rows, rows), 1)

    def send(t, d):
        return pltpu.make_async_remote_copy(
            src_ref=sums.at[t, tp], dst_ref=sums.at[t, tp], send_sem=send_sem.at[t, d], recv_sem=recv_sem.at[t, d],
            device_id={'tp': peers[d]}, device_id_type=pl.DeviceIdType.MESH)

    def project(t):
        x_copy(t).wait()
        if t == 0:
            res = jnp.zeros((rows, q_loc + hd), F32)
            for j in range(n_k):
                for cp in w_copies(j)[:2]:
                    cp.wait()
                ks = slice(j * k_rows, (j + 1) * k_rows)
                res = res + jnp.dot(x[t, :, ks], w[ks, 0:q_loc + hd], preferred_element_type=F32)
            res = res.astype(BF16)
        else:
            res = jnp.dot(x[t], w[:, 0:q_loc + hd], preferred_element_type=F32).astype(BF16)
        raw[t] = res
        q = res[:, :q_loc].astype(F32)
        k = res[:, q_loc:q_loc + hd].astype(F32)
        part = jnp.where(sq_lane == 0, jnp.sum(q * q, axis=-1, keepdims=True), jnp.sum(k * k, axis=-1, keepdims=True))
        sums[t, tp] = jnp.transpose(part)[0:8]
        if t == 0:
            pl.semaphore_wait(barrier, n_tp - 1)
        for d in range(n_tp - 1):
            send(t, d).start()

    def rotate_all(t):
        for d in range(n_tp - 1):
            send(t, d).wait()
        tot = sums[t, 0]
        for d in range(1, n_tp):
            tot = tot + sums[t, d]
        full = jnp.transpose(jnp.concatenate([tot, jnp.zeros((rows - 8, rows), F32)], axis=0))
        q_scale = rms_factor(full[:, 0:1], q_loc * n_tp)
        k_scale = rms_factor(full[:, 1:2], hd * n_tp)

        def rotate(col, scale, gain):
            val = raw[t, :, col:col + hd].astype(F32) * scale * gain.astype(F32)
            return (val * cos_t[t] + pltpu.roll(val, hd // 2, 1) * sin_t[t]).astype(BF16).astype(F32)
        for j in range(heads):
            q_out[pl.ds(t * heads + j, rows, stride=16), :] = rotate(j * hd, q_scale, gq_ref[j:j + 1, :])
        k_out[t] = rotate(q_loc, k_scale, gk_ref[...])

    for t in range(n_steps):
        project(t)
    for j in range(n_k):
        w_copies(j)[2].wait()
    for t in range(n_steps):
        v_out[t] = jnp.dot(x[t], w[:, q_loc + hd:width], preferred_element_type=F32).astype(BF16).astype(F32)
    q_out[pl.ds(n_steps * heads, rows, stride=16), :] = jnp.zeros((rows, hd), F32)
    for t in range(n_steps):
        rotate_all(t)


def head(x_seq, cache_len, w_q, w_k, w_v, g_q, g_k, n_tp):
    n_steps, rows, d_model = x_seq.shape
    q_loc, hd = w_q.shape[1], w_k.shape[1]
    width = q_loc + 2 * hd
    half = hd // 2
    inv_freq = np.float32(ROPE_THETA) ** (-(np.arange(half, dtype=np.float32) * np.float32(2.0 / hd)))
    freq = jnp.asarray(np.concatenate([inv_freq, inv_freq]).reshape(1, hd), F32)
    vmem = pl.BlockSpec(memory_space=pltpu.VMEM)
    hbm = pl.BlockSpec(memory_space=pl.ANY)
    return pl.pallas_call(
        functools.partial(head_kernel, (n_steps, rows, d_model, q_loc, hd, n_tp)),
        name='head',
        out_shape=(jax.ShapeDtypeStruct((rows * 16, hd), F32),
                   jax.ShapeDtypeStruct((n_steps, rows, hd), F32),
                   jax.ShapeDtypeStruct((n_steps, rows, hd), F32)),
        in_specs=[vmem] * 4 + [hbm] * 4,
        out_specs=(vmem,) * 3,
        scratch_shapes=[
            pltpu.VMEM((n_steps, rows, d_model), BF16),
            pltpu.VMEM((d_model, width), BF16),
            pltpu.VMEM((n_steps, rows, q_loc + hd), BF16),
            pltpu.VMEM((n_steps, rows, hd), F32),
            pltpu.VMEM((n_steps, rows, hd), F32),
            pltpu.VMEM((n_steps, n_tp, 8, rows), F32),
            pltpu.SemaphoreType.DMA((n_steps,)),
            pltpu.SemaphoreType.DMA((3, 4)),
            pltpu.SemaphoreType.DMA((n_steps, n_tp - 1)),
            pltpu.SemaphoreType.DMA((n_steps, n_tp - 1)),
        ],
        compiler_params=pltpu.CompilerParams(collective_id=0, has_side_effects=True, vmem_limit_bytes=67043328),
    )(cache_len.reshape(1, -1), g_q.reshape(-1, hd), g_k.reshape(1, -1), freq, x_seq, w_q, w_k, w_v)


def attn_kernel(dims, len_ref, q_hbm, kn_hbm, vn_hbm, k_hbm, v_hbm, o_hbm, ko_hbm, vo_hbm,
                kb, vb, q, kn, vn, s_scr, e_scr, l_scr, o_scr, o_buf, n_sem, in_sem, out_sem, o_sem):
    n_steps, nb, heads, hd, seq_max, n_rows = dims
    n_blocks = n_rows // nb
    win = 32
    row_step = lax.broadcasted_iota(jnp.int32, (16, seq_max), 0) // heads
    col = lax.broadcasted_iota(jnp.int32, (16, seq_max), 1)
    ahead = col - row_step
    win_row = lax.broadcasted_iota(jnp.int32, (win, hd), 0)
    small = [pltpu.make_async_copy(src, dst, n_sem.at[i])
             for i, (src, dst) in enumerate(((kn_hbm, kn), (vn_hbm, vn), (q_hbm, q)))]

    def load(i, blk):
        src, dst = ((k_hbm, kb), (v_hbm, vb))[i]
        rs = pl.ds(blk * nb, nb)
        return pltpu.make_async_copy(src.at[rs], dst.at[rs], in_sem.at[i, blk])

    def store(i, blk):
        src, dst = ((kb, ko_hbm), (vb, vo_hbm))[i]
        rs = pl.ds(blk * nb, nb)
        return pltpu.make_async_copy(src.at[rs], dst.at[rs], out_sem.at[i, blk])

    def o_store(blk):
        rs = pl.ds(blk * nb, nb)
        return pltpu.make_async_copy(o_buf.at[:, rs], o_hbm.at[:, rs], o_sem.at[blk])

    small[0].start()
    load(0, 0).start()
    for cp in small[1:]:
        cp.start()
    load(1, 0).start()
    for blk in range(1, n_blocks):
        for i in range(2):
            load(i, blk).start()
    small[0].wait()

    def block(blk, carry):
        first = blk * nb
        for j, (buf, new) in enumerate(((kb, kn), (vb, vn))):
            load(j, blk).wait()
            if j == 1:
                @pl.when(blk == 0)
                def _():
                    for cp in small[1:]:
                        cp.wait()
            new_rows = [new[t, pl.ds(pl.multiple_of(first, nb), nb), :] for t in range(n_steps)]
            for i in range(nb):
                ln = len_ref[first + i]
                base = pl.multiple_of(jnp.minimum((ln // 16) * 16, seq_max - win), 16)
                rel = win_row + (base - ln)
                cut = buf[first + i, pl.ds(base, win), :].astype(F32)
                for t in range(n_steps):
                    cut = jnp.where(rel == t, new_rows[t][i:i + 1, :], cut)
                buf[first + i, pl.ds(base, win), :] = cut.astype(BF16)
            store(j, blk).start()
        for i in range(nb):
            s = lax.dot_general(q[first + i].astype(BF16), kb[first + i], (((1,), (1,)), ((), ())), preferred_element_type=F32) * hd ** -0.5
            s_scr[i * 16:(i + 1) * 16, :] = jnp.where(ahead <= len_ref[first + i], s, -jnp.inf)
        for i in range(0, nb, 2):
            rs = slice(i * 16, (i + 2) * 16)
            s = s_scr[rs, :]
            e = jnp.exp(s - jnp.max(s, axis=-1, keepdims=True))
            l_scr[rs, :] = jnp.broadcast_to(jnp.sum(e, axis=-1, keepdims=True), (32, hd))
            e_scr[rs, :] = e.astype(BF16)
        for i in range(nb):
            rs = slice(i * 16, (i + 1) * 16)
            o_scr[rs, :] = jnp.dot(e_scr[rs, :], vb[first + i], preferred_element_type=F32)
        o_scr[...] = o_scr[...] / l_scr[...]
        for t in range(n_steps):
            for j in range(heads):
                o_buf[t, pl.ds(pl.multiple_of(first, nb), nb), j * hd:(j + 1) * hd] = o_scr[pl.ds(t * heads + j, nb, stride=16), :].astype(BF16)
        o_store(blk).start()
        return carry
    lax.fori_loop(0, n_blocks, block, 0)
    for blk in range(n_blocks):
        for i in range(2):
            store(i, blk).wait()
        o_store(blk).wait()


def attend(q, kn, vn, k_cache, v_cache, cache_len, heads):
    n_rows, _, seq_max, hd = k_cache.shape
    n_steps = kn.shape[0]
    nb = 32
    hbm = pl.BlockSpec(memory_space=pl.ANY)
    cache_shape = jax.ShapeDtypeStruct((n_rows, seq_max, hd), BF16)
    flops = 4 * n_rows * 16 * seq_max * hd
    return pl.pallas_call(
        functools.partial(attn_kernel, (n_steps, nb, heads, hd, seq_max, n_rows)),
        name='attend',
        in_specs=[pl.BlockSpec(memory_space=pltpu.SMEM)] + [hbm] * 5,
        out_specs=(hbm, hbm, hbm),
        scratch_shapes=[
            pltpu.VMEM((n_rows, seq_max, hd), BF16),
            pltpu.VMEM((n_rows, seq_max, hd), BF16),
            pltpu.VMEM((n_rows, 16, hd), F32),
            pltpu.VMEM((n_steps, n_rows, hd), F32),
            pltpu.VMEM((n_steps, n_rows, hd), F32),
            pltpu.VMEM((nb * 16, seq_max), F32),
            pltpu.VMEM((nb * 16, seq_max), BF16),
            pltpu.VMEM((nb * 16, hd), F32),
            pltpu.VMEM((nb * 16, hd), F32),
            pltpu.VMEM((n_steps, n_rows, heads * hd), BF16),
            pltpu.SemaphoreType.DMA((3,)),
            pltpu.SemaphoreType.DMA((2, n_rows // nb)),
            pltpu.SemaphoreType.DMA((2, n_rows // nb)),
            pltpu.SemaphoreType.DMA((n_rows // nb,)),
        ],
        out_shape=(jax.ShapeDtypeStruct((n_steps, n_rows, heads * hd), BF16), cache_shape, cache_shape),
        compiler_params=pltpu.CompilerParams(vmem_limit_bytes=67043328),
        cost_estimate=pl.CostEstimate(flops=flops, bytes_accessed=4 * n_rows * seq_max * hd * 2, transcendentals=n_rows * 16 * seq_max),
    )(cache_len, q.reshape(n_rows, 16, hd), kn, vn, k_cache[:, 0], v_cache[:, 0])


def finish_kernel(n, src, dst, buf, in_sem, out_sem):
    ins = [pltpu.make_async_copy(src.at[i], buf.at[i], in_sem.at[i]) for i in range(n)]
    outs = [pltpu.make_async_copy(buf.at[i], dst.at[i], out_sem.at[i]) for i in range(n)]
    for cp in ins:
        cp.start()
    for a, b in zip(ins, outs):
        a.wait()
        b.start()
    for cp in outs:
        cp.wait()


def finish(y):
    n_steps, rows, d_model = y.shape
    n = 4 * n_steps
    shape = (n, n_steps * rows // n, d_model)
    hbm = pl.BlockSpec(memory_space=pl.ANY)
    out = pl.pallas_call(
        functools.partial(finish_kernel, n),
        name='finish',
        in_specs=[hbm],
        out_specs=hbm,
        scratch_shapes=[pltpu.VMEM(shape, BF16), pltpu.SemaphoreType.DMA((n,)), pltpu.SemaphoreType.DMA((n,))],
        out_shape=jax.ShapeDtypeStruct(shape, BF16),
        compiler_params=pltpu.CompilerParams(vmem_limit_bytes=67043328),
    )(y.reshape(shape))
    return out.reshape(y.shape)


def local_layer(n_tp, x_seq, cache_len, k_cache, v_cache, w_q, w_k, w_v, w_o, w_gate, w_up, w_down, g_q, g_k, g_attn, g_mlp):
    heads = w_q.shape[1] // k_cache.shape[3]
    q, kn, vn = head(x_seq, cache_len, w_q, w_k, w_v, g_q, g_k, n_tp)
    o, k_out, v_out = attend(q, kn, vn, k_cache, v_cache, cache_len, heads)
    y = tail(o, x_seq, w_o, w_gate, w_up, w_down, g_attn, g_mlp)
    return finish(y), k_out[:, None], v_out[:, None]


def solution(mesh):
    tp_size = mesh.shape['tp']
    data_spec = P(None, 'dp', None)
    cache_spec = P('dp', 'tp', None, None)
    col_spec = P(None, 'tp')
    row_spec = P('tp', None)
    arg_specs = (data_spec, P('dp'), cache_spec, cache_spec, col_spec, col_spec, col_spec, row_spec, col_spec, col_spec, row_spec, P('tp'), P('tp'), P(None), P(None))
    out_specs = (data_spec, cache_spec, cache_spec)
    return jax.shard_map(functools.partial(local_layer, tp_size), mesh=mesh, in_specs=arg_specs, out_specs=out_specs, check_vma=False)
```
